128 devices in a mesh: dp: 8 (over y_lo, z), ctx: 16 (over x, y_hi, core).
Axes of the slice: x: 4, y: 4 (y_hi: 2, y_lo: 2; y = y_hi * 2 + y_lo), z: 4, core: 2. Of those that a mesh axis runs over, the one named last changes fastest.
Arguments:
- item_ids: int32 [32, 4096], P('dp', 'ctx'), may hold values from 0 to 131071, as said below
- lengths: int32 [32], P('dp'), may hold values from 512 to 4096
- table: bfloat16 [131072, 512], P('dp'), may hold values from -6 to 6
- w_in: bfloat16 [512, 2048], replicated, may hold values from -0.25 to 0.25
- w_out: bfloat16 [512, 512], replicated, may hold values from -0.25 to 0.25
Outputs:
- layer_out: bfloat16 [32, 4096, 512], P('dp', 'ctx')
The draws below stay inside these ranges and needn't reach their ends.
Inputs may be any that keep to these rules, and one draw needn't show every extreme that they name: `item_ids`: the owner of an id is id // 16384. In every user's block of 256 positions of one index of ctx, at most 64 ids have one owner; in each such block one owner, the same for all users at that index of ctx, has exactly 64.
All inputs are finite; a program needn't handle non-finite values.
Results may differ from the reference program's by a relative error of at most 0.0054.
Values may be sent and summed in bfloat16 or wider, within the bound.
No kernel may reach another device: no remote copies, remote signals or barrier semaphores. Data moves between devices by JAX's collectives and lax.ppermute only.
A program may use at most 128 MiB of HBM per device.

```python
import math
import jax
import jax.numpy as jnp
from jax import lax

D = 512
HEADS = 8
BLK = 256
VOC_DEV = 16384
SEQ = 4096
USERS = 32
VOCAB = 131072
CAP = 64


def draw_item_ids(key, part):
    owner_count = VOCAB // VOC_DEV
    block_count = SEQ // BLK
    hottest = jax.random.randint(jax.random.fold_in(key, 1), (block_count,), 0, owner_count).astype(jnp.int32)

    def one_block(user, block, hot_owner):
        block_key = jax.random.fold_in(jax.random.fold_in(key, 2), user * block_count + block)
        key_slots = jax.random.fold_in(block_key, 3)
        key_order = jax.random.fold_in(block_key, 4)
        key_top = jax.random.fold_in(block_key, 5)
        key_rows = jax.random.fold_in(block_key, 6)
        slots = jax.random.permutation(key_slots, (owner_count - 1) * CAP)[:BLK - CAP].astype(jnp.int32)
        others = slots // CAP
        others = others + (others >= hot_owner).astype(jnp.int32)
        owners = jnp.concatenate([jnp.full((CAP,), hot_owner, jnp.int32), others])
        owners = jax.random.permutation(key_order, owners)
        upper = jax.random.randint(key_top, (BLK,), 1, VOC_DEV + 1)
        rows = jax.random.randint(key_rows, (BLK,), 0, upper)
        return (owners * VOC_DEV + rows).astype(jnp.int32)
    users = jnp.arange(USERS, dtype=jnp.int32)
    blocks = jnp.arange(block_count, dtype=jnp.int32)
    per_user = jax.vmap(lambda user: jax.vmap(lambda block, hot_owner: one_block(user, block, hot_owner))(blocks, hottest))
    drawn = per_user(users)
    return drawn.reshape(USERS, SEQ)


def set_ends(result, key, smallest, top_value):
    shape = result.shape
    index_at = [jax.random.randint(jax.random.fold_in(key, axis), (), 0, shape[axis]) for axis in range(len(shape))]
    result = result.at[tuple(index_at)].set(smallest)
    longest = shape.index(max(shape))
    index_at[longest] = (index_at[longest] + 1) % shape[longest]
    return result.at[tuple(index_at)].set(top_value)


def steps_of(stream_key, extent, pieces, low, largest):
    def one(axis_at, shards_of):
        heights = jax.random.uniform(jax.random.fold_in(jax.random.fold_in(stream_key, 6), axis_at), (shards_of,), jnp.float32, low / len(pieces), largest / len(pieces))
        return jnp.repeat(jnp.exp(heights), extent[axis_at] // shards_of).reshape((-1,) + (1,) * (len(extent) - axis_at - 1))

    factor_of = one(*pieces[0])
    for cut in pieces[1:]:
        factor_of = factor_of * one(*cut)
    return factor_of


def normal_values(own_key, dims, width, reach, pieces=(), kind=jnp.bfloat16):
    values = jax.random.normal(own_key, dims, jnp.float32) * width
    if len(pieces) > 0:
        values = steps_of(own_key, dims, pieces, -0.22, 0.18) * values
    return jnp.clip(values, min=-reach, max=reach).astype(kind)


def setup_inputs(seed: int = 0) -> dict:
    key_of = jax.random.split(jax.random.key(seed), 6)
    return {
        "item_ids": draw_item_ids(jax.random.fold_in(key_of[5], 71), 0),
        "lengths": set_ends(jax.random.randint(key_of[1], (USERS,), SEQ // 8, SEQ + 1), jax.random.fold_in(key_of[1], 1), SEQ // 8, SEQ).astype(jnp.int32),
        "table": normal_values(key_of[2], (VOCAB, D), 1.0, 6.0, ((0, 8),)),
        "w_in": normal_values(key_of[3], (D, 4 * D), D ** -0.5, 0.25),
        "w_out": normal_values(key_of[4], (D, D), D ** -0.5, 0.25),
    }


def layer_norm(values):
    center = values - lax.optimization_barrier(jnp.mean(values, axis=-1, keepdims=True))
    spread = lax.optimization_barrier(jnp.mean(center * center, axis=-1, keepdims=True))
    return center * lax.rsqrt(spread + 1e-05)

def reference(item_ids, lengths, table, w_in, w_out):
    embedded = jnp.take(table, item_ids, axis=0)
    normed = layer_norm(embedded.astype(jnp.float32)).astype(jnp.bfloat16)
    projected = jax.nn.silu(jnp.dot(normed.reshape(-1, D), w_in, preferred_element_type=jnp.float32))
    projected = projected.astype(jnp.bfloat16).reshape(USERS, SEQ, 4 * D)
    gate_rows = projected[..., :D]
    value_rows = projected[..., D:2 * D]
    query_rows = projected[..., 2 * D:3 * D]
    key_rows = projected[..., 3 * D:]
    head_size = D // HEADS
    query_block = math.gcd(SEQ, 512)

    def one_user(packed):
        user_queries, user_keys, user_values, length_one = packed
        outputs = []
        for block_index in range(SEQ // query_block):
            row_low = block_index * query_block
            row_high = row_low + query_block
            query_heads = user_queries[row_low:row_high].astype(jnp.float32).reshape(query_block, HEADS, head_size)
            key_heads = user_keys[:row_high].astype(jnp.float32).reshape(row_high, HEADS, head_size)
            value_heads = user_values[:row_high].astype(jnp.float32).reshape(row_high, HEADS, head_size)
            scores = jnp.einsum('qhd,khd->hqk', query_heads, key_heads) * (1.0 / math.sqrt(head_size))
            query_pos = row_low + jnp.arange(query_block, dtype=jnp.int32)
            key_pos = jnp.arange(row_high, dtype=jnp.int32)
            visible = (key_pos[None, :] <= query_pos[:, None]) & (key_pos[None, :] < length_one)
            weights = jnp.where(visible[None], jax.nn.silu(scores), 0.0).astype(jnp.bfloat16)
            attended = jnp.einsum('hqk,khd->qhd', weights.astype(jnp.float32), value_heads)
            outputs.append(attended.reshape(query_block, D))
        return jnp.concatenate(outputs, axis=0)
    attended = lax.map(one_user, (query_rows, key_rows, value_rows, lengths))
    gated = (layer_norm(attended) * gate_rows.astype(jnp.float32)).astype(jnp.bfloat16)
    mixed = jnp.dot(gated.reshape(-1, D), w_out, preferred_element_type=jnp.float32).reshape(USERS, SEQ, D)
    return (embedded.astype(jnp.float32) + mixed).astype(jnp.bfloat16)
```

```python
import jax, jax.numpy as jnp, functools
from jax import lax
from jax.experimental import pallas as pl
from jax.experimental.pallas import tpu as pltpu
BF=jnp.bfloat16; F32=jnp.float32
BLK=256; D=512

def half_silu(h):
    return h + h*jnp.tanh(h)

def nt(a,b):
    return lax.dot_general(a,b,(((1,),(1,)),((),())),preferred_element_type=F32)
def nn(a,b):
    return jnp.dot(a,b,preferred_element_type=F32)

def kv_kernel(nb, sc_ref, x_ref, wk_ref, wvT_ref, wqT_ref, wgT_ref, k_ref, vT_ref, qT_ref, gT_ref, xq_ref, n_scr, nq_scr):
    def body(i,_):
        place = sc_ref[3+i]
        x = x_ref[pl.ds(pl.multiple_of(i*BLK,BLK),BLK),:].astype(F32)
        mean = jnp.mean(x,axis=1,keepdims=True)
        c = x-mean
        var = jnp.mean(c*c,axis=1,keepdims=True)
        n = (c*lax.rsqrt(var+1e-5)).astype(BF)
        n_scr[...] = n
        row = pl.multiple_of(place*BLK,BLK)
        k_ref[pl.ds(row,BLK),:] = half_silu(nn(n,wk_ref[...])).astype(BF)
        v = half_silu(nt(wvT_ref[...],n))
        pos = sc_ref[2]+place*BLK+lax.broadcasted_iota(jnp.int32,(1,BLK),1)
        vT_ref[:,pl.ds(row,BLK)] = jnp.where(pos<sc_ref[0],v,0.0).astype(BF)
        qo = pl.multiple_of(sc_ref[1],64)
        qrow = pl.multiple_of(place*64,64)
        nq_scr[pl.ds(qrow,64),:] = n_scr[pl.ds(qo,64),:]
        xq_ref[pl.ds(qrow,64),:] = x_ref[pl.ds(pl.multiple_of(i*BLK+qo,64),64),:]
        return 0
    lax.fori_loop(0,nb,body,0)
    nq = nq_scr[...]
    qT_ref[...] = half_silu(nt(wqT_ref[...],nq)).astype(BF)*BF(1/16)
    gT_ref[...] = half_silu(nt(wgT_ref[...],nq)).astype(BF)

def kv_call(nb, sc, x, wk, wvT, wqT, wgT):
    nq=nb*64
    vm=pl.BlockSpec(memory_space=pltpu.VMEM)
    return pl.pallas_call(functools.partial(kv_kernel,nb),
        out_shape=[jax.ShapeDtypeStruct((nb*BLK,D),BF),jax.ShapeDtypeStruct((D,nb*BLK),BF),
                   jax.ShapeDtypeStruct((D,nq),BF),jax.ShapeDtypeStruct((D,nq),BF),jax.ShapeDtypeStruct((nq,D),BF)],
        in_specs=[pl.BlockSpec(memory_space=pltpu.SMEM)]+[vm]*5,
        out_specs=[vm]*5,
        scratch_shapes=[pltpu.VMEM((BLK,D),BF),pltpu.VMEM((nq,D),BF)],
        compiler_params=pltpu.CompilerParams(vmem_limit_bytes=56*1024*1024),
        name="kv",
    )(sc,x,wk,wvT,wqT,wgT)

def attn_kernel(nprev, G, sc_ref, *refs):
    nch=nprev+1
    ks=refs[:nch]; vs=refs[nch:2*nch]
    qT_ref,gT_ref,xq_ref,wo_ref,out_ref,o_scr = refs[2*nch:]
    nb=8
    def head_pair(p,_):
        lane=pl.multiple_of(p*128,128)
        rid=lax.broadcasted_iota(jnp.int32,(128,256),0)
        for t in range(nb//4):
            qT=qT_ref[pl.ds(lane,128),256*t:256*t+256]
            zero=jnp.zeros_like(qT)
            qs=(jnp.where(rid<64,qT,zero),jnp.where(rid<64,zero,qT))
            accs=[None,None]
            for ch in range(nch):
                last = ch==nch-1
                nk = 4*(t+1) if last else nb
                for g in range(0,nk,G):
                    k=ks[ch][g*BLK:(g+G)*BLK,pl.ds(lane,128)]
                    for hh in range(2):
                        s=nn(k,qs[hh])
                        w=s+s*jnp.tanh(s)
                        if last and g+G>4*t:
                            r=lax.broadcasted_iota(jnp.int32,(G*BLK,256),0)+(g-4*t)*BLK
                            cc=lax.broadcasted_iota(jnp.int32,(1,256),1)
                            thr=(cc//64)*256+(cc%64)+sc_ref[1]
                            w=jnp.where(r<=thr,w,0.0)
                        o=nn(vs[ch][pl.ds(pl.multiple_of(lane+64*hh,64),64),g*BLK:(g+G)*BLK],w.astype(BF))
                        accs[hh]=o if accs[hh] is None else accs[hh]+o
            for hh in range(2):
                o_scr[pl.ds(pl.multiple_of(lane+64*hh,64),64),256*t:256*t+256]=accs[hh]
        return 0
    lax.fori_loop(0,4,head_pair,0)
    for t in range(nb//4):
        cs=slice(256*t,256*t+256)
        o=o_scr[:,cs]
        mean=jnp.mean(o,axis=0,keepdims=True)
        c=o-mean
        var=jnp.mean(c*c,axis=0,keepdims=True)
        gated=((c*lax.rsqrt(var+1e-5))*gT_ref[:,cs].astype(F32)).astype(BF)
        mixed=lax.dot_general(gated,wo_ref[...],(((0,),(0,)),((),())),preferred_element_type=F32)
        out_ref[cs,:]=(xq_ref[cs,:].astype(F32)+mixed).astype(BF)

def attn_call(nprev, G, sc, ks, vs, qT, gT, xq, wo):
    vm=pl.BlockSpec(memory_space=pltpu.VMEM)
    n=2*(nprev+1)+4
    return pl.pallas_call(functools.partial(attn_kernel,nprev,G),
        out_shape=jax.ShapeDtypeStruct((512,D),BF),
        in_specs=[pl.BlockSpec(memory_space=pltpu.SMEM)]+[vm]*n,
        out_specs=vm,
        scratch_shapes=[pltpu.VMEM((D,512),F32)],
        compiler_params=pltpu.CompilerParams(vmem_limit_bytes=56*1024*1024),
        name=f"attn{nprev}",
    )(sc,*ks,*vs,qT,gT,xq,wo)


from jax.sharding import Mesh
from jax.sharding import PartitionSpec as P

CTX = ("xh", "xl", "yh", "co")
FLIP = [(0, 1), (1, 0)]


def per_device(item_ids, lengths, table, w_in, w_out):
    owned = table.shape[0]
    me = lax.axis_index("dp")
    xh, xl, yh, co = (lax.axis_index(a) for a in CTX)
    owners = lax.axis_size("dp")
    half = (w_in * 0.5).astype(BF)
    wgT, wvT, wqT = (half[:, D * i : D * (i + 1)].T for i in range(3))
    wk = half[:, 3 * D :]

    send = jnp.broadcast_to(item_ids[None], (owners, 4, BLK)).reshape(owners * 4, BLK)
    wanted = lax.all_to_all(send, ("dp", "xh", "yh"), 0, 0, tiled=True).reshape(owners, 4, BLK)
    mine = lax.dynamic_index_in_dim(wanted, me, 0, keepdims=False)
    length = lax.dynamic_index_in_dim(lengths, 2 * xh + yh, 0, keepdims=False)
    upto = jnp.triu(jnp.ones((2 * BLK, 2 * BLK), BF))

    def ranks(member):
        return nn(member.astype(BF), upto).astype(jnp.int32) - 1

    cap = 2 * 64
    places = []
    for xx, cc in ((xl, co), (1 - xl, co), (xl, 1 - co), (1 - xl, 1 - co)):
        places += [4 * xx + cc, 4 * xx + cc + 2]

    def fetch(c):
        ids = wanted[:, 2 * c : 2 * c + 2].reshape(owners, 2 * BLK)
        local = ids - me * owned
        here = (local >= 0) & (local < owned)
        rank = jnp.where(here, ranks(here), -1)
        slot = lax.broadcasted_iota(jnp.int32, (owners, cap, 2 * BLK), 1)
        rows = jnp.sum(jnp.where(rank[:, None, :] == slot, local[:, None, :], 0), axis=2)
        picked = jnp.take(table, rows.reshape(-1), axis=0, mode="clip").reshape(owners, cap, D)
        got = lax.all_to_all(picked, "dp", 0, 0, tiled=True).reshape(owners * cap, D)
        own_ids = mine[2 * c : 2 * c + 2].reshape(2 * BLK)
        owner = own_ids // owned
        member = owner[None, :] == lax.broadcasted_iota(jnp.int32, (owners, 2 * BLK), 0)
        at = jnp.sum(jnp.where(member, ranks(member), 0), axis=0) + owner * cap
        pick = (at[:, None] == lax.broadcasted_iota(jnp.int32, (2 * BLK, owners * cap), 1)).astype(BF)
        return nn(pick, got).astype(BF)

    def exchange(own):
        far = lax.ppermute(own, "xl", FLIP)
        near = lax.ppermute(own, "co", FLIP)
        diag = lax.ppermute(far, "co", FLIP)
        return jnp.concatenate([own, far, near, diag], axis=0)

    ks, vs, outs = [], [], []
    for c in range(2):
        x = exchange(fetch(c))
        sc = jnp.stack([length, 64 * (2 * xl + co), jnp.int32(8 * BLK * c)] + places).astype(jnp.int32)
        k, v, q, g, xq = kv_call(8, sc, x, wk, wvT, wqT, wgT)
        ks.append(k)
        vs.append(v)
        outs.append(attn_call(c, 4, sc, ks, vs, q, g, xq, w_out))
    out = jnp.concatenate(outs, axis=0).reshape(16, 64, D)
    back = lax.all_to_all(out, CTX, 0, 0, tiled=True)
    back = back.reshape(2, 2, 2, 2, 64, D).transpose(0, 2, 1, 3, 4, 5)
    return back.reshape(4, BLK, D)


def solution(mesh):
    finer = Mesh(mesh.devices.reshape(mesh.shape["dp"], 2, 2, 2, 2), ("dp",) + CTX)
    return jax.shard_map(
        per_device,
        mesh=finer,
        in_specs=(P("dp", CTX), P("dp"), P("dp", None), P(), P()),
        out_specs=P("dp", CTX, None),
        check_vma=False,
    )
```

```python
import functools

import jax
import jax.numpy as jnp
from jax import lax
from jax.experimental import pallas as pl
from jax.experimental.pallas import tpu as pltpu

BF = jnp.bfloat16
F32 = jnp.float32
BLK = 256
D = 512
GRP = 1024
PART = 64
CAP = 128
VM = pl.BlockSpec(memory_space=pltpu.VMEM)
SM = pl.BlockSpec(memory_space=pltpu.SMEM)
ANY = pl.BlockSpec(memory_space=pl.ANY)
PARAMS = pltpu.CompilerParams(vmem_limit_bytes=56 * 1024 * 1024)
BUNCH = 32


def twice_silu(h):
    return h + h * jnp.tanh(h)


def nt(a, b):
    return lax.dot_general(a, b, (((1,), (1,)), ((), ())), preferred_element_type=F32)


def nn(a, b):
    return jnp.dot(a, b, preferred_element_type=F32)


def gather_kernel(owners, rows_ref, count_ref, low_ref, table_ref, out_ref, buf, sems):
    bunches = CAP // BUNCH

    def real(o, b):
        return b * BUNCH < count_ref[o]

    def copy(o, b, i):
        at = o * CAP + b * BUNCH + i
        return pltpu.make_async_copy(
            table_ref.at[lax.shift_right_logical(rows_ref[o, b * BUNCH + i], 3)],
            buf.at[at],
            sems.at[o * bunches + b],
        )

    def start(k, _):
        o = k // bunches
        b = k % bunches

        @pl.when(real(o, b))
        def _():
            for i in range(BUNCH):
                copy(o, b, i).start()

        return 0

    lax.fori_loop(0, owners * bunches, start, 0)
    width = BUNCH * 8
    lane = lax.broadcasted_iota(jnp.int32, (BUNCH, width), 1)
    base = 8 * lax.broadcasted_iota(jnp.int32, (BUNCH, 1), 0)
    for o in range(owners):
        for b in range(bunches):
            dst = slice(o * CAP + b * BUNCH, o * CAP + (b + 1) * BUNCH)

            @pl.when(real(o, b))
            def _():
                pltpu.make_async_copy(buf.at[dst], buf.at[dst], sems.at[o * bunches + b]).wait()
                want = base + low_ref[b * BUNCH : (b + 1) * BUNCH, o : o + 1]
                pick = (lane == want).astype(F32).astype(BF)
                got = buf[dst].reshape(width, D)
                out_ref[dst, :] = nn(pick, got).astype(BF)

            @pl.when(jnp.logical_not(real(o, b)))
            def _():
                out_ref[dst, :] = jnp.zeros((BUNCH, D), BF)


def gather_call(rows, count, low, table):
    owners = rows.shape[0]
    return pl.pallas_call(
        functools.partial(gather_kernel, owners),
        out_shape=jax.ShapeDtypeStruct((owners * CAP, D), BF),
        in_specs=[SM, SM, VM, ANY],
        out_specs=VM,
        scratch_shapes=[
            pltpu.VMEM((owners * CAP, 8, D), BF),
            pltpu.SemaphoreType.DMA((owners * CAP // BUNCH,)),
        ],
        compiler_params=PARAMS,
        name="gather",
    )(rows, count, low, table.reshape(-1, 8, D))


def kv_kernel(
    first, group_at, sc_ref, p1_ref, p2_ref, wk_ref, wv_ref, wq_ref, wg_ref, k_ref, v_ref, q_ref, g_ref, xq_ref, n_scr, nq_scr
):
    co = sc_ref[2]
    base = first + GRP * sc_ref[group_at]
    qo = pl.multiple_of(sc_ref[1], PART)
    for s, ref in enumerate((p1_ref, p2_ref)):
        x = ref[...].astype(F32)
        c = x - jnp.mean(x, axis=1, keepdims=True)
        var = jnp.mean(c * c, axis=1, keepdims=True)
        n_scr[s] = (c * lax.rsqrt(var + 1e-5)).astype(BF)
    for s, ref in enumerate((p1_ref, p2_ref)):
        edge = co if s == 0 else 1 - co
        n = n_scr[s]
        k = twice_silu(0.5 * nn(n, wk_ref[...])).astype(BF)
        v = twice_silu(0.5 * nt(wv_ref[...], n))
        for j in range(2):
            at = pl.multiple_of((edge + 2 * j) * BLK, BLK)
            k_ref[pl.ds(at, BLK), :] = k[j * BLK : (j + 1) * BLK]
            pos = base + at + lax.broadcasted_iota(jnp.int32, (1, BLK), 1)
            v_ref[:, pl.ds(at, BLK)] = jnp.where(pos < sc_ref[0], v[:, j * BLK : (j + 1) * BLK], 0.0).astype(BF)
            to = pl.multiple_of((edge + 2 * j) * PART, PART)
            nq_scr[pl.ds(to, PART), :] = n_scr[s, pl.ds(j * BLK + qo, PART), :]
            xq_ref[pl.ds(to, PART), :] = ref[pl.ds(j * BLK + qo, PART), :]
    nq = nq_scr[...]
    q_ref[...] = twice_silu(0.5 * nt(wq_ref[...], nq)).astype(BF) * BF(1 / 16)
    g_ref[...] = twice_silu(0.5 * nt(wg_ref[...], nq)).astype(BF)


def kv_call(first, group_at, sc, p1, p2, w_in, w_turned):
    def part(i):
        return pl.BlockSpec((D, D), lambda _: (i, 0))

    def whole(shape):
        return pl.BlockSpec(shape, lambda _: (0,) * len(shape))

    quarter = GRP // 4
    shapes = [(GRP, D), (D, GRP), (D, quarter), (D, quarter), (quarter, D)]
    return pl.pallas_call(
        functools.partial(kv_kernel, first, group_at),
        grid=(1,),
        out_shape=[jax.ShapeDtypeStruct(s, BF) for s in shapes],
        in_specs=[SM, whole((D, D)), whole((D, D)), pl.BlockSpec((D, D), lambda _: (0, 3)), part(1), part(2), part(0)],
        out_specs=[whole(s) for s in shapes],
        scratch_shapes=[pltpu.VMEM((2, D, D), BF), pltpu.VMEM((quarter, D), BF)],
        compiler_params=PARAMS,
        name="kv",
    )(sc, p1, p2, w_in, w_turned, w_turned, w_turned)


def attn_kernel(chunk, sc_ref, *refs):
    halves = 2 * (chunk + 1)
    k_in, v_in = refs[:halves], refs[halves : 2 * halves]
    q_in, g_in, x_in = (refs[2 * halves + 2 * i : 2 * halves + 2 * i + 2] for i in range(3))
    w_ref = refs[2 * halves + 6]
    out_ref, k_scr, v_scr, q_scr, g_scr, x_scr, o_scr, r_scr, sems, out_sem = refs[-10:]
    copies = []
    for i in range(halves):
        grp = 2 * (i // 2) + sc_ref[3 + i % 2]
        pairs = [(k_in[i], k_scr, grp), (v_in[i], v_scr, grp)]
        if i >= halves - 2:
            side = sc_ref[3 + i % 2]
            pairs += [(a[i % 2], s, side) for a, s in ((q_in, q_scr), (g_in, g_scr), (x_in, x_scr))]
        for src, dst, to in pairs:
            copies.append(pltpu.make_async_copy(src, dst.at[to], sems.at[len(copies)]))
    for c in copies:
        c.start()
    for c in copies:
        c.wait()
    rid = lax.broadcasted_iota(jnp.int32, (128, 256), 0)
    col = lax.broadcasted_iota(jnp.int32, (1, 512), 1) & 255
    last_key = (col // PART) * BLK + (col % PART) + sc_ref[1]
    key = lax.broadcasted_iota(jnp.int32, (BLK, 512), 0)

    def head_pair(p, _):
        lane = pl.multiple_of(p * 128, 128)
        steps = [(t, g, i) for t in range(2) for g in range(2 * chunk + t + 1) for i in range(4)]
        queries = []
        for t in range(2):
            q = q_scr[t, pl.ds(lane, 128), :]
            zero = jnp.zeros_like(q)
            queries.append(jnp.concatenate([jnp.where(rid < 64, q, zero), jnp.where(rid < 64, zero, q)], axis=1))

        def scores(step):
            t, g, i = step
            return nn(k_scr[g, i * BLK : (i + 1) * BLK, pl.ds(lane, 128)], queries[t])

        def weights(step, s):
            t, g, i = step
            w = s + s * jnp.tanh(s)
            if g == 2 * chunk + t:
                w = jnp.where(key + i * BLK <= last_key, w, 0.0)
            return w.astype(BF)

        sums = [None, None]

        def gather_values(step, w):
            t, g, i = step
            o = nn(v_scr[g, pl.ds(lane, 128), i * BLK : (i + 1) * BLK], w)
            o = (o[:64, :256], o[64:, 256:])
            sums[t] = o if sums[t] is None else (sums[t][0] + o[0], sums[t][1] + o[1])

        s = scores(steps[0])
        before = None
        for n, step in enumerate(steps):
            ahead = scores(steps[n + 1]) if n + 1 < len(steps) else None
            w = weights(step, s)
            if before is not None:
                gather_values(steps[n - 1], before)
            before, s = w, ahead
        gather_values(steps[-1], before)
        for t in range(2):
            for hh in range(2):
                o_scr[t, pl.ds(pl.multiple_of(lane + 64 * hh, 64), 64), :] = sums[t][hh]
        return 0

    lax.fori_loop(0, 4, head_pair, 0)
    for t in range(2):
        o = o_scr[t]
        c = o - jnp.mean(o, axis=0, keepdims=True)
        var = jnp.mean(c * c, axis=0, keepdims=True)
        gated = ((c * lax.rsqrt(var + 1e-5)) * g_scr[t].astype(F32)).astype(BF)
        mixed = lax.dot_general(gated, w_ref[...], (((0,), (0,)), ((), ())), preferred_element_type=F32)
        r_scr[t * 256 : (t + 1) * 256, :] = (x_scr[t].astype(F32) + mixed).astype(BF)
    done = pltpu.make_async_copy(r_scr, out_ref.at[pl.ds(chunk * 512, 512)], out_sem)
    done.start()
    done.wait()


def attn_call(chunk, sc, ks, vs, qs, gs, xs, w_out, previous):
    halves = 2 * (chunk + 1)
    inputs = [sc, *ks, *vs, *qs, *gs, *xs, w_out]
    specs = [SM] + [ANY] * (2 * halves + 6) + [VM]
    alias = {}
    if previous is not None:
        alias = {len(inputs): 0}
        inputs.append(previous)
        specs.append(ANY)
    return pl.pallas_call(
        functools.partial(attn_kernel, chunk),
        out_shape=jax.ShapeDtypeStruct((1024, D), BF),
        in_specs=specs,
        out_specs=ANY,
        input_output_aliases=alias,
        scratch_shapes=[
            pltpu.VMEM((halves, GRP, D), BF),
            pltpu.VMEM((halves, D, GRP), BF),
            pltpu.VMEM((2, D, 256), BF),
            pltpu.VMEM((2, D, 256), BF),
            pltpu.VMEM((2, 256, D), BF),
            pltpu.VMEM((2, D, 256), F32),
            pltpu.VMEM((512, D), BF),
            pltpu.SemaphoreType.DMA((2 * halves + 6,)),
            pltpu.SemaphoreType.DMA,
        ],
        compiler_params=PARAMS,
        name="attend" + str(chunk),
    )(*inputs)


from jax.sharding import Mesh
from jax.sharding import PartitionSpec as P

CTX = ("xh", "xl", "yh", "co")
FLIP = [(0, 1), (1, 0)]


def per_device(item_ids, lengths, table, w_in, w_out):
    owned = table.shape[0]
    me = lax.axis_index("dp")
    xh, xl, yh, co = (lax.axis_index(a) for a in CTX)
    owners = lax.axis_size("dp")
    w_turned = w_in.T

    send = jnp.broadcast_to(item_ids[None], (owners, 4, BLK)).reshape(owners * 4, BLK)
    wanted = lax.all_to_all(send, ("dp", "xh", "yh"), 0, 0, tiled=True).reshape(owners, 4, BLK)
    mine = lax.dynamic_index_in_dim(wanted, me, 0, keepdims=False)
    user = 2 * xh + yh
    length = jnp.sum(jnp.where(lax.iota(jnp.int32, 4) == user, lengths, 0))
    upto = jnp.triu(jnp.ones((2 * BLK, 2 * BLK), BF))
    slots = lax.iota(jnp.int32, 8)
    sc = jnp.zeros((8,), jnp.int32)
    for i, value in enumerate((length, PART * (2 * xl + co), co, xl, 1 - xl)):
        sc = jnp.where(slots == i, value, sc)

    def ranks(member):
        return nn(member.astype(BF), upto).astype(jnp.int32) - 1

    def fetch(c):
        ids = wanted[:, 2 * c : 2 * c + 2].reshape(owners, 2 * BLK)
        local = ids - me * owned
        here = (local >= 0) & (local < owned)
        rank = jnp.where(here, ranks(here), -1)
        slot = lax.broadcasted_iota(jnp.int32, (owners, CAP, 2 * BLK), 1)
        rows = jnp.sum(jnp.where(rank[:, None, :] == slot, local[:, None, :], 0), axis=2)
        count = jnp.sum(here.astype(jnp.int32), axis=1)
        picked = gather_call(rows, count, (rows & 7).T, table).reshape(owners, CAP, D)
        return lax.all_to_all(picked, "dp", 0, 0, tiled=True).reshape(owners * CAP, D)

    def place(c, got):
        own_ids = mine[2 * c : 2 * c + 2].reshape(2 * BLK)
        owner = own_ids // owned
        member = owner[None, :] == lax.broadcasted_iota(jnp.int32, (owners, 2 * BLK), 0)
        at = jnp.sum(jnp.where(member, ranks(member), 0), axis=0) + owner * CAP
        pick = (at[:, None] == lax.broadcasted_iota(jnp.int32, (2 * BLK, owners * CAP), 1)).astype(BF)
        return nn(pick, got).astype(BF)

    ks, vs, out = [], [], None
    for c in range(2):
        own = place(c, fetch(c))
        far = lax.ppermute(own, "xl", FLIP)
        near = lax.ppermute(own, "co", FLIP)
        diag = lax.ppermute(far, "co", FLIP)
        first = 2 * GRP * c
        k0, v0, q0, g0, x0 = kv_call(first, 3, sc, own, near, w_in, w_turned)
        k1, v1, q1, g1, x1 = kv_call(first, 4, sc, far, diag, w_in, w_turned)
        ks += [k0, k1]
        vs += [v0, v1]
        out = attn_call(c, sc, ks, vs, (q0, q1), (g0, g1), (x0, x1), w_out, out)
    back = lax.all_to_all(out.reshape(16, PART, D), CTX, 0, 0, tiled=True)
    back = back.reshape(2, 2, 2, 2, PART, D).transpose(0, 2, 1, 3, 4, 5)
    return back.reshape(4, BLK, D)


def solution(mesh):
    finer = Mesh(mesh.devices.reshape(mesh.shape["dp"], 2, 2, 2, 2), ("dp",) + CTX)
    return jax.shard_map(
        per_device,
        mesh=finer,
        in_specs=(P("dp", CTX), P("dp"), P("dp", None), P(), P()),
        out_specs=P("dp", CTX, None),
        check_vma=False,
    )
```

```python
import functools

import jax
import jax.numpy as jnp
from jax import lax
from jax.experimental import pallas as pl
from jax.experimental.pallas import tpu as pltpu

BF = jnp.bfloat16
F32 = jnp.float32
BLK = 256
D = 512
GRP = 1024
PART = 64
CAP = 128
VM = pl.BlockSpec(memory_space=pltpu.VMEM)
SM = pl.BlockSpec(memory_space=pltpu.SMEM)
ANY = pl.BlockSpec(memory_space=pl.ANY)


def cost(us):
    return pl.CostEstimate(flops=int(us * FLOPS_PER_US), bytes_accessed=0, transcendentals=0)


FLOPS_PER_US = 4_000_000
PARAMS = pltpu.CompilerParams(vmem_limit_bytes=56 * 1024 * 1024)
BUNCH = 32


def twice_silu(h):
    return h + h * jnp.tanh(h)


def tn(a, b):
    return lax.dot_general(a, b, (((0,), (1,)), ((), ())), preferred_element_type=F32)


def nn(a, b):
    return jnp.dot(a, b, preferred_element_type=F32)


def gather_kernel(owners, rows_ref, count_ref, low_ref, table_ref, out_ref, buf, sems):
    bunches = CAP // BUNCH

    def real(o, b):
        return b * BUNCH < count_ref[o]

    def copy(o, b, i):
        at = o * CAP + b * BUNCH + i
        return pltpu.make_async_copy(
            table_ref.at[lax.shift_right_logical(rows_ref[o, b * BUNCH + i], 3)],
            buf.at[at],
            sems.at[o * bunches + b],
        )

    def start(k, _):
        o = k // bunches
        b = k % bunches

        @pl.when(real(o, b))
        def _():
            for i in range(BUNCH):
                copy(o, b, i).start()

        return 0

    lax.fori_loop(0, owners * bunches, start, 0)
    width = BUNCH * 8
    lane = lax.broadcasted_iota(jnp.int32, (BUNCH, width), 1)
    base = 8 * lax.broadcasted_iota(jnp.int32, (BUNCH, 1), 0)
    for o in range(owners):
        for b in range(bunches):
            dst = slice(o * CAP + b * BUNCH, o * CAP + (b + 1) * BUNCH)

            @pl.when(real(o, b))
            def _():
                pltpu.make_async_copy(buf.at[dst], buf.at[dst], sems.at[o * bunches + b]).wait()
                want = base + low_ref[b * BUNCH : (b + 1) * BUNCH, o : o + 1]
                pick = (lane == want).astype(F32).astype(BF)
                got = buf[dst].reshape(width, D)
                out_ref[dst, :] = nn(pick, got).astype(BF)

            @pl.when(jnp.logical_not(real(o, b)))
            def _():
                out_ref[dst, :] = jnp.zeros((BUNCH, D), BF)


def gather_call(rows, count, low, table):
    owners = rows.shape[0]
    return pl.pallas_call(
        functools.partial(gather_kernel, owners),
        out_shape=jax.ShapeDtypeStruct((owners * CAP, D), BF),
        in_specs=[SM, SM, VM, ANY],
        out_specs=VM,
        scratch_shapes=[
            pltpu.VMEM((owners * CAP, 8, D), BF),
            pltpu.SemaphoreType.DMA((owners * CAP // BUNCH,)),
        ],
        compiler_params=PARAMS,
        cost_estimate=cost(8),
        name="gather",
    )(rows, count, low, table.reshape(-1, 8, D))


def kv_kernel(
    first, group_at, sc_ref, p1_ref, p2_ref, wk_ref, wv_ref, wq_ref, wg_ref, k_ref, v_ref, q_ref, g_ref, xq_ref, n_scr, nq_scr
):
    co = sc_ref[2]
    base = first + GRP * sc_ref[group_at]
    qo = pl.multiple_of(sc_ref[1], PART)
    for s, ref in enumerate((p1_ref, p2_ref)):
        x = ref[...].astype(F32)
        c = x - jnp.mean(x, axis=1, keepdims=True)
        var = jnp.mean(c * c, axis=1, keepdims=True)
        n_scr[s] = (c * lax.rsqrt(var + 1e-5)).astype(BF)
    for s, ref in enumerate((p1_ref, p2_ref)):
        edge = co if s == 0 else 1 - co
        n = n_scr[s]
        k = twice_silu(0.5 * nn(n, wk_ref[...])).astype(BF)
        v = twice_silu(0.5 * tn(wv_ref[...], n))
        for j in range(2):
            at = pl.multiple_of((edge + 2 * j) * BLK, BLK)
            k_ref[pl.ds(at, BLK), :] = k[j * BLK : (j + 1) * BLK]
            pos = base + at + lax.broadcasted_iota(jnp.int32, (1, BLK), 1)
            v_ref[:, pl.ds(at, BLK)] = jnp.where(pos < sc_ref[0], v[:, j * BLK : (j + 1) * BLK], 0.0).astype(BF)
            to = pl.multiple_of((edge + 2 * j) * PART, PART)
            nq_scr[pl.ds(to, PART), :] = n_scr[s, pl.ds(j * BLK + qo, PART), :]
            xq_ref[pl.ds(to, PART), :] = ref[pl.ds(j * BLK + qo, PART), :]
    nq = nq_scr[...]
    q_ref[...] = twice_silu(0.5 * tn(wq_ref[...], nq)).astype(BF) * BF(1 / 16)
    g_ref[...] = twice_silu(0.5 * tn(wg_ref[...], nq)).astype(BF)


def kv_call(first, group_at, sc, p1, p2, w_in):
    def part(i):
        return pl.BlockSpec((D, D), lambda _: (0, i))

    def whole(shape):
        return pl.BlockSpec(shape, lambda _: (0,) * len(shape))

    quarter = GRP // 4
    shapes = [(GRP, D), (D, GRP), (D, quarter), (D, quarter), (quarter, D)]
    return pl.pallas_call(
        functools.partial(kv_kernel, first, group_at),
        grid=(1,),
        out_shape=[jax.ShapeDtypeStruct(s, BF) for s in shapes],
        in_specs=[SM, whole((D, D)), whole((D, D)), part(3), part(1), part(2), part(0)],
        out_specs=[whole(s) for s in shapes],
        scratch_shapes=[pltpu.VMEM((2, D, D), BF), pltpu.VMEM((quarter, D), BF)],
        compiler_params=PARAMS,
        cost_estimate=cost(5.5),
        name="kv",
    )(sc, p1, p2, w_in, w_in, w_in, w_in)


def attn_kernel(chunk, sc_ref, *refs):
    halves = 2 * (chunk + 1)
    k_in, v_in = refs[:halves], refs[halves : 2 * halves]
    q_in, g_in, x_in = (refs[2 * halves + 2 * i : 2 * halves + 2 * i + 2] for i in range(3))
    w_ref = refs[2 * halves + 6]
    out_ref, k_scr, v_scr, q_scr, g_scr, x_scr, o_scr, r_scr, sems, out_sem = refs[-10:]
    copies = []
    for i in range(halves):
        grp = 2 * (i // 2) + sc_ref[3 + i % 2]
        pairs = [(k_in[i], k_scr, grp), (v_in[i], v_scr, grp)]
        if i >= halves - 2:
            side = sc_ref[3 + i % 2]
            pairs += [(a[i % 2], s, side) for a, s in ((q_in, q_scr), (g_in, g_scr), (x_in, x_scr))]
        for src, dst, to in pairs:
            copies.append(pltpu.make_async_copy(src, dst.at[to], sems.at[len(copies)]))
    for c in copies:
        c.start()
    for c in copies:
        c.wait()
    rid = lax.broadcasted_iota(jnp.int32, (128, 256), 0)
    col = lax.broadcasted_iota(jnp.int32, (1, 512), 1) & 255
    last_key = (col // PART) * BLK + (col % PART) + sc_ref[1]
    key = lax.broadcasted_iota(jnp.int32, (BLK, 512), 0)

    def head_pair(p, _):
        lane = pl.multiple_of(p * 128, 128)
        steps = [(t, g, i) for t in range(2) for g in range(2 * chunk + t + 1) for i in range(4)]
        queries = []
        for t in range(2):
            q = q_scr[t, pl.ds(lane, 128), :]
            zero = jnp.zeros_like(q)
            queries.append(jnp.concatenate([jnp.where(rid < 64, q, zero), jnp.where(rid < 64, zero, q)], axis=1))

        def scores(step):
            t, g, i = step
            return nn(k_scr[g, i * BLK : (i + 1) * BLK, pl.ds(lane, 128)], queries[t])

        def weights(step, s):
            t, g, i = step
            w = s + s * jnp.tanh(s)
            if g == 2 * chunk + t:
                w = jnp.where(key + i * BLK <= last_key, w, 0.0)
            return w.astype(BF)

        sums = [None, None]

        def gather_values(step, w):
            t, g, i = step
            o = nn(v_scr[g, pl.ds(lane, 128), i * BLK : (i + 1) * BLK], w)
            o = (o[:64, :256], o[64:, 256:])
            sums[t] = o if sums[t] is None else (sums[t][0] + o[0], sums[t][1] + o[1])

        s = scores(steps[0])
        before = None
        for n, step in enumerate(steps):
            ahead = scores(steps[n + 1]) if n + 1 < len(steps) else None
            w = weights(step, s)
            if before is not None:
                gather_values(steps[n - 1], before)
            before, s = w, ahead
        gather_values(steps[-1], before)
        for t in range(2):
            for hh in range(2):
                o_scr[t, pl.ds(pl.multiple_of(lane + 64 * hh, 64), 64), :] = sums[t][hh]
        return 0

    lax.fori_loop(0, 4, head_pair, 0)
    for t in range(2):
        o = o_scr[t]
        c = o - jnp.mean(o, axis=0, keepdims=True)
        var = jnp.mean(c * c, axis=0, keepdims=True)
        gated = ((c * lax.rsqrt(var + 1e-5)) * g_scr[t].astype(F32)).astype(BF)
        mixed = lax.dot_general(gated, w_ref[...], (((0,), (0,)), ((), ())), preferred_element_type=F32)
        r_scr[t * 256 : (t + 1) * 256, :] = (x_scr[t].astype(F32) + mixed).astype(BF)
    done = pltpu.make_async_copy(r_scr, out_ref.at[pl.ds(chunk * 512, 512)], out_sem)
    done.start()
    done.wait()


def attn_call(chunk, sc, ks, vs, qs, gs, xs, w_out, previous):
    halves = 2 * (chunk + 1)
    inputs = [sc, *ks, *vs, *qs, *gs, *xs, w_out]
    specs = [SM] + [ANY] * (2 * halves + 6) + [VM]
    alias = {}
    if previous is not None:
        alias = {len(inputs): 0}
        inputs.append(previous)
        specs.append(ANY)
    return pl.pallas_call(
        functools.partial(attn_kernel, chunk),
        out_shape=jax.ShapeDtypeStruct((1024, D), BF),
        in_specs=specs,
        out_specs=ANY,
        input_output_aliases=alias,
        scratch_shapes=[
            pltpu.VMEM((halves, GRP, D), BF),
            pltpu.VMEM((halves, D, GRP), BF),
            pltpu.VMEM((2, D, 256), BF),
            pltpu.VMEM((2, D, 256), BF),
            pltpu.VMEM((2, 256, D), BF),
            pltpu.VMEM((2, D, 256), F32),
            pltpu.VMEM((512, D), BF),
            pltpu.SemaphoreType.DMA((2 * halves + 6,)),
            pltpu.SemaphoreType.DMA,
        ],
        compiler_params=PARAMS,
        cost_estimate=cost(12 + 8 * chunk),
    )(*inputs)


from jax.sharding import Mesh
from jax.sharding import PartitionSpec as P

CTX = ("xh", "xl", "yh", "co")
FLIP = [(0, 1), (1, 0)]


def layer(item_ids, lengths, table, w_in, w_out):
    owned = table.shape[0]
    me = lax.axis_index("dp")
    xh, xl, yh, co = (lax.axis_index(a) for a in CTX)
    owners = lax.axis_size("dp")

    send = jnp.broadcast_to(item_ids[None], (owners, 4, BLK)).reshape(owners * 4, BLK)
    wanted = lax.all_to_all(send, ("dp", "xh", "yh"), 0, 0, tiled=True).reshape(owners, 4, BLK)
    mine = lax.dynamic_index_in_dim(wanted, me, 0, keepdims=False)
    user = 2 * xh + yh
    length = jnp.sum(jnp.where(lax.iota(jnp.int32, 4) == user, lengths, 0))
    upto = jnp.triu(jnp.ones((2 * BLK, 2 * BLK), BF))
    slots = lax.iota(jnp.int32, 8)
    sc = jnp.zeros((8,), jnp.int32)
    for i, value in enumerate((length, PART * (2 * xl + co), co, xl, 1 - xl)):
        sc = jnp.where(slots == i, value, sc)

    def ranks(member):
        return nn(member.astype(BF), upto).astype(jnp.int32) - 1

    def fetch(c):
        ids = wanted[:, 2 * c : 2 * c + 2].reshape(owners, 2 * BLK)
        local = ids - me * owned
        here = (local >= 0) & (local < owned)
        rank = jnp.where(here, ranks(here), -1)
        slot = lax.broadcasted_iota(jnp.int32, (owners, CAP, 2 * BLK), 1)
        rows = jnp.sum(jnp.where(rank[:, None, :] == slot, local[:, None, :], 0), axis=2)
        count = jnp.sum(here.astype(jnp.int32), axis=1)
        picked = gather_call(rows, count, (rows & 7).T, table).reshape(owners, CAP, D)
        return lax.all_to_all(picked, "dp", 0, 0, tiled=True).reshape(owners * CAP, D)

    def place(c, got):
        own_ids = mine[2 * c : 2 * c + 2].reshape(2 * BLK)
        owner = own_ids // owned
        member = owner[None, :] == lax.broadcasted_iota(jnp.int32, (owners, 2 * BLK), 0)
        at = jnp.sum(jnp.where(member, ranks(member), 0), axis=0) + owner * CAP
        pick = (at[:, None] == lax.broadcasted_iota(jnp.int32, (2 * BLK, owners * CAP), 1)).astype(BF)
        return nn(pick, got).astype(BF)

    ks, vs, out = [], [], None
    for c in range(2):
        got = fetch(c)
        own = place(c, got)
        far = lax.ppermute(own, "xl", FLIP)
        near = lax.ppermute(own, "co", FLIP)
        diag = lax.ppermute(far, "co", FLIP)
        first = 2 * GRP * c
        k0, v0, q0, g0, x0 = kv_call(first, 3, sc, own, near, w_in)
        k1, v1, q1, g1, x1 = kv_call(first, 4, sc, far, diag, w_in)
        ks += [k0, k1]
        vs += [v0, v1]
        out = attn_call(c, sc, ks, vs, (q0, q1), (g0, g1), (x0, x1), w_out, out)
    back = lax.all_to_all(out.reshape(16, PART, D), CTX, 0, 0, tiled=True)
    back = back.reshape(2, 2, 2, 2, PART, D).transpose(0, 2, 1, 3, 4, 5)
    return back.reshape(4, BLK, D)


def solution(mesh):
    finer = Mesh(mesh.devices.reshape(mesh.shape["dp"], 2, 2, 2, 2), ("dp",) + CTX)
    return jax.shard_map(
        layer,
        mesh=finer,
        in_specs=(P("dp", CTX), P("dp"), P("dp", None), P(), P()),
        out_specs=P("dp", CTX, None),
        check_vma=False,
    )
```

```python
import functools

import jax
import jax.numpy as jnp
from jax import lax
from jax.experimental import pallas as pl
from jax.experimental.pallas import tpu as pltpu

BF = jnp.bfloat16
F32 = jnp.float32
BLK = 256
D = 512
GRP = 1024
PART = 64
CAP = 128
ROW8 = 8
BUNCH = 32
VM = pl.BlockSpec(memory_space=pltpu.VMEM)
SM = pl.BlockSpec(memory_space=pltpu.SMEM)
ANY = pl.BlockSpec(memory_space=pl.ANY)
PARAMS = pltpu.CompilerParams(vmem_limit_bytes=16 * 1024 * 1024)


def cost(us):
    return pl.CostEstimate(flops=int(us * 4_000_000), bytes_accessed=0, transcendentals=0)


def in_vmem(x):
    return pltpu.with_memory_space_constraint(x, pltpu.VMEM)


def twice_silu(h):
    return h + h * jnp.tanh(h)


def tn(a, b):
    return lax.dot_general(a, b, (((0,), (1,)), ((), ())), preferred_element_type=F32)


def nn(a, b):
    return jnp.dot(a, b, preferred_element_type=F32)


def gather_kernel(owners, rows_ref, count_ref, ids_ref, table_ref, out_ref, buf, sems):
    def eights(o):
        return (count_ref[o] + ROW8 - 1) // ROW8

    for o in range(owners):

        def start(j, _, o=o):
            for i in range(ROW8):
                s = j * ROW8 + i
                pltpu.make_async_copy(
                    table_ref.at[lax.shift_right_logical(rows_ref[o, s], 3)], buf.at[o * CAP + s], sems.at[o]
                ).start()
            return 0

        def clear(j, _, o=o):
            buf[pl.ds(o * CAP + j * ROW8, ROW8)] = jnp.zeros((ROW8, 8, D), BF)
            return 0

        lax.fori_loop(0, eights(o), start, 0)
        full = BUNCH // ROW8
        lax.fori_loop(eights(o), (eights(o) + full - 1) // full * full, clear, 0)
    low = (ids_ref[...] & 7).astype(F32).T
    width = BUNCH * 8
    lane = lax.broadcasted_iota(jnp.int32, (BUNCH, width), 1).astype(F32)
    slot = lax.broadcasted_iota(jnp.int32, (BUNCH, 1), 0)
    for o in range(owners):
        eight = buf.at[pl.ds(o * CAP, ROW8)]

        def wait(j, _, o=o, eight=eight):
            pltpu.make_async_copy(eight, eight, sems.at[o]).wait()
            return 0

        lax.fori_loop(0, eights(o), wait, 0)
        for b in range(CAP // BUNCH):
            dst = slice(o * CAP + b * BUNCH, o * CAP + (b + 1) * BUNCH)
            want = (8 * slot).astype(F32) + low[b * BUNCH : (b + 1) * BUNCH, o : o + 1]
            pick = (lane == want).astype(F32).astype(BF)
            got = nn(pick, buf[dst].reshape(width, D))
            out_ref[dst, :] = jnp.where(slot + b * BUNCH < count_ref[o], got, 0.0).astype(BF)


def gather_call(rows, count, groups):
    owners = rows.shape[0]
    return pl.pallas_call(
        functools.partial(gather_kernel, owners),
        out_shape=jax.ShapeDtypeStruct((owners * CAP, D), BF),
        in_specs=[SM, SM, VM, pl.BlockSpec(memory_space=pltpu.HBM)],
        out_specs=VM,
        scratch_shapes=[pltpu.VMEM((owners * CAP, 8, D), BF), pltpu.SemaphoreType.DMA((owners,))],
        compiler_params=pltpu.CompilerParams(vmem_limit_bytes=56 * 1024 * 1024),
        cost_estimate=cost(7),
        name="gather",
    )(rows, count, rows, groups)


def project(first, side, sc_ref, pieces, w_ref, k_ref, v_ref, q_ref, g_ref, x_ref, n_scr, nq_scr):
    co = sc_ref[2]
    base = first + GRP * sc_ref[3 + side]
    qo = pl.multiple_of(sc_ref[1], PART)
    wg, wv, wq, wk = (slice(D * i, D * (i + 1)) for i in range(4))
    for s, ref in enumerate(pieces):
        x = ref[...].astype(F32)
        c = x - jnp.mean(x, axis=1, keepdims=True)
        var = jnp.mean(c * c, axis=1, keepdims=True)
        n_scr[s] = (c * lax.rsqrt(var + 1e-5)).astype(BF)
    for s, ref in enumerate(pieces):
        edge = co if s == 0 else 1 - co
        n = n_scr[s]
        k = twice_silu(0.5 * nn(n, w_ref[:, wk])).astype(BF)
        v = twice_silu(0.5 * tn(w_ref[:, wv], n))
        for j in range(2):
            at = pl.multiple_of((edge + 2 * j) * BLK, BLK)
            k_ref[pl.ds(at, BLK), :] = k[j * BLK : (j + 1) * BLK]
            pos = base + at + lax.broadcasted_iota(jnp.int32, (1, BLK), 1)
            v_ref[:, pl.ds(at, BLK)] = jnp.where(pos < sc_ref[0], v[:, j * BLK : (j + 1) * BLK], 0.0).astype(BF)
            to = pl.multiple_of((edge + 2 * j) * PART, PART)
            nq_scr[pl.ds(to, PART), :] = n_scr[s, pl.ds(j * BLK + qo, PART), :]
            x_ref[pl.ds(to, PART), :] = ref[pl.ds(j * BLK + qo, PART), :]
    nq = nq_scr[...]
    q_ref[...] = twice_silu(0.5 * tn(w_ref[:, wq], nq)).astype(BF) * BF(1 / 16)
    g_ref[...] = twice_silu(0.5 * tn(w_ref[:, wg], nq)).astype(BF)


def attend(sc_ref, tiles, together):
    rid = lax.broadcasted_iota(jnp.int32, (128, 256), 0)
    col = lax.broadcasted_iota(jnp.int32, (1, 512), 1) & 255
    last_key = (col // PART) * BLK + (col % PART) + sc_ref[1]
    key = lax.broadcasted_iota(jnp.int32, (BLK, 512), 0)

    def heads(pp, _):
        steps = [
            (u, t, m, i)
            for u in range(together)
            for t in range(len(tiles))
            for m in range(len(tiles[t][2]))
            for i in range(GRP // BLK)
        ]
        queries = {}
        sums = {}

        def lanes(u):
            return pl.multiple_of((pp * together + u) * 128, 128)

        def scores(step):
            u, t, m, i = step
            if (u, t) not in queries:
                q = tiles[t][0][pl.ds(lanes(u), 128), :]
                zero = jnp.zeros_like(q)
                queries[u, t] = jnp.concatenate([jnp.where(rid < 64, q, zero), jnp.where(rid < 64, zero, q)], axis=1)
            return nn(tiles[t][2][m][0][i * BLK : (i + 1) * BLK, pl.ds(lanes(u), 128)], queries[u, t])

        def weights(step, s):
            _, t, m, i = step
            w = s + s * jnp.tanh(s)
            if tiles[t][2][m][2]:
                w = jnp.where(key + i * BLK <= last_key, w, 0.0)
            return w.astype(BF)

        def add_values(step, w):
            u, t, m, i = step
            o = nn(tiles[t][2][m][1][pl.ds(lanes(u), 128), i * BLK : (i + 1) * BLK], w)
            o = (o[:64, :256], o[64:, 256:])
            old = sums.get((u, t))
            sums[u, t] = o if old is None else (old[0] + o[0], old[1] + o[1])

        s = scores(steps[0])
        before = None
        for n, step in enumerate(steps):
            ahead = scores(steps[n + 1]) if n + 1 < len(steps) else None
            w = weights(step, s)
            if before is not None:
                add_values(steps[n - 1], before)
            before, s = w, ahead
        add_values(steps[-1], before)
        for (u, t), pair in sums.items():
            for hh in range(2):
                tiles[t][1][pl.ds(pl.multiple_of(lanes(u) + 64 * hh, 64), 64), :] = pair[hh]
        return 0

    lax.fori_loop(0, 4 // together, heads, 0)


def near_kernel(chunk, sc_ref, *refs):
    past = refs[: 4 * chunk]
    p1, p2, w_ref, k_ref, v_ref, q_ref, g_ref, x_ref, o_ref, n_scr, nq_scr = refs[4 * chunk :]
    project(2 * GRP * chunk, 0, sc_ref, (p1, p2), w_ref, k_ref, v_ref, q_ref, g_ref, x_ref, n_scr, nq_scr)
    seen = [(past[2 * i], past[2 * i + 1], False) for i in range(2 * chunk)]
    attend(sc_ref, [(q_ref, o_ref, seen + [(k_ref, v_ref, True)])], 2)


def far_kernel(chunk, sc_ref, *refs):
    past = refs[: 4 * chunk]
    p1, p2, w_ref, wo_ref, kn, vn, qn, gn, xn, on = refs[4 * chunk : 4 * chunk + 10]
    rest = refs[4 * chunk + 10 :]
    if chunk:
        first_ref, rest = rest[0], rest[1:]
        out_ref, rest = rest[0], rest[1:]
        kf, vf = rest[-2:]
    else:
        out_ref, kf, vf = rest[:3]
        rest = rest[3:]
    n_scr, nq_scr, qf, gf, xf, of, qx, kx, vx, ox = rest[:10]
    project(2 * GRP * chunk, 1, sc_ref, (p1, p2), w_ref, kf, vf, qf, gf, xf, n_scr, nq_scr)
    low = sc_ref[3] == 0

    @pl.when(low)
    def _():
        qx[...], kx[...], vx[...] = qf[...], kn[...], vn[...]

    @pl.when(jnp.logical_not(low))
    def _():
        qx[...], kx[...], vx[...] = qn[...], kf[...], vf[...]

    seen = [(past[2 * i], past[2 * i + 1], False) for i in range(2 * chunk)]
    attend(sc_ref, [(qf, of, seen + [(kf, vf, True)]), (qx, ox, [(kx, vx, False)])], 2 - chunk)
    if chunk:
        out_ref[:512, :] = first_ref[...]
    for side, (o_ref, g_ref, x_ref) in enumerate(((on, gn, xn), (of, gf, xf))):
        o = o_ref[...] + jnp.where(sc_ref[3 + side] == 1, ox[...], 0.0)
        c = o - jnp.mean(o, axis=0, keepdims=True)
        var = jnp.mean(c * c, axis=0, keepdims=True)
        gated = ((c * lax.rsqrt(var + 1e-5)) * g_ref[...].astype(F32)).astype(BF)
        mixed = lax.dot_general(gated, wo_ref[...], (((0,), (0,)), ((), ())), preferred_element_type=F32)
        at = pl.multiple_of(512 * chunk + 256 * sc_ref[3 + side], 256)
        out_ref[pl.ds(at, 256), :] = (x_ref[...].astype(F32) + mixed).astype(BF)


SIZES = [(GRP, D), (D, GRP), (D, 256), (D, 256), (256, D)]


def near_call(chunk, sc, past, own, near, w_in):
    inputs = [*past, own, near, w_in]
    outs = pl.pallas_call(
        functools.partial(near_kernel, chunk),
        out_shape=[pltpu.VMEM(s, BF) for s in SIZES] + [pltpu.VMEM((D, 256), F32)],
        in_specs=[SM] + [VM] * len(inputs),
        out_specs=[VM] * 6,
        scratch_shapes=[pltpu.VMEM((2, D, D), BF), pltpu.VMEM((256, D), BF)],
        compiler_params=PARAMS,
        cost_estimate=cost(6 + 6 * chunk),
    )(sc, *inputs)
    return outs


def far_call(chunk, sc, past, far, diag, w_in, w_out, kept, first):
    inputs = [*past, far, diag, w_in, w_out, *kept]
    scratch = [
        pltpu.VMEM((2, D, D), BF),
        pltpu.VMEM((256, D), BF),
        pltpu.VMEM((D, 256), BF),
        pltpu.VMEM((D, 256), BF),
        pltpu.VMEM((256, D), BF),
        pltpu.VMEM((D, 256), F32),
        pltpu.VMEM((D, 256), BF),
        pltpu.VMEM((GRP, D), BF),
        pltpu.VMEM((D, GRP), BF),
        pltpu.VMEM((D, 256), F32),
    ]
    held = [pltpu.VMEM(s, BF) for s in SIZES[:2]]
    if chunk:
        inputs.append(first)
        shapes, scratch = [jax.ShapeDtypeStruct((1024, D), BF)], scratch + held
    else:
        shapes = [pltpu.VMEM((512, D), BF)] + held
    return pl.pallas_call(
        functools.partial(far_kernel, chunk),
        out_shape=shapes,
        in_specs=[SM] + [VM] * len(inputs),
        out_specs=[VM] * len(shapes),
        scratch_shapes=scratch,
        compiler_params=PARAMS,
        cost_estimate=cost(9 + 5 * chunk),
    )(sc, *inputs)


from jax.sharding import Mesh
from jax.sharding import PartitionSpec as P

CTX = ("xh", "xl", "yh", "co")
FLIP = [(0, 1), (1, 0)]


def layer(item_ids, lengths, table, w_in, w_out):
    owned = table.shape[0]
    me = lax.axis_index("dp")
    xh, xl, yh, co = (lax.axis_index(a) for a in CTX)
    owners = lax.axis_size("dp")
    w_in, w_out = in_vmem(w_in), in_vmem(w_out)
    groups = table.reshape(-1, 8, D)

    send = jnp.broadcast_to(item_ids[None], (owners, 4, BLK)).reshape(owners * 4, BLK)
    wanted = lax.all_to_all(send, ("dp", "xh", "yh"), 0, 0, tiled=True).reshape(owners, 4, BLK)
    mine = lax.dynamic_index_in_dim(wanted, me, 0, keepdims=False)
    user = 2 * xh + yh
    length = jnp.sum(jnp.where(lax.iota(jnp.int32, 4) == user, lengths, 0))
    upto = jnp.triu(jnp.ones((2 * BLK, 2 * BLK), BF))
    slots = lax.iota(jnp.int32, 8)
    sc = jnp.zeros((8,), jnp.int32)
    for i, value in enumerate((length, PART * (2 * xl + co), co, xl, 1 - xl)):
        sc = jnp.where(slots == i, value, sc)

    def ranks(member):
        return nn(member.astype(BF), upto).astype(jnp.int32) - 1

    def fetch(c):
        ids = wanted[:, 2 * c : 2 * c + 2].reshape(owners, 2 * BLK)
        local = ids - me * owned
        here = (local >= 0) & (local < owned)
        rank = jnp.where(here, ranks(here), -1)
        slot = lax.broadcasted_iota(jnp.int32, (owners, CAP, 2 * BLK), 1)
        rows = jnp.sum(jnp.where(rank[:, None, :] == slot, local[:, None, :], 0), axis=2)
        count = jnp.sum(here.astype(jnp.int32), axis=1)
        picked = gather_call(rows, count, groups).reshape(owners, CAP, D)
        return lax.all_to_all(picked, "dp", 0, 0, tiled=True).reshape(owners * CAP, D)

    def place(c, got):
        own_ids = mine[2 * c : 2 * c + 2].reshape(2 * BLK)
        owner = own_ids // owned
        member = owner[None, :] == lax.broadcasted_iota(jnp.int32, (owners, 2 * BLK), 0)
        at = jnp.sum(jnp.where(member, ranks(member), 0), axis=0) + owner * CAP
        pick = (at[:, None] == lax.broadcasted_iota(jnp.int32, (2 * BLK, owners * CAP), 1)).astype(BF)
        return nn(pick, got).astype(BF)

    past, first = [], None
    for c in range(2):
        got = fetch(c)
        own = place(c, got)
        far = lax.ppermute(own, "xl", FLIP)
        near = lax.ppermute(own, "co", FLIP)
        diag = lax.ppermute(far, "co", FLIP)
        pieces = [in_vmem(a) for a in (own, near, far, diag)]
        kept = near_call(c, sc, past, *pieces[:2], w_in)
        kept = [in_vmem(a) for a in kept]
        done = far_call(c, sc, past, *pieces[2:], w_in, w_out, kept, first)
        if c == 0:
            first, k1, v1 = (in_vmem(a) for a in done)
            past = [*kept[:2], k1, v1]
    back = lax.all_to_all(done[0].reshape(16, PART, D), CTX, 0, 0, tiled=True)
    back = back.reshape(2, 2, 2, 2, PART, D).transpose(0, 2, 1, 3, 4, 5)
    return back.reshape(4, BLK, D)


def solution(mesh):
    finer = Mesh(mesh.devices.reshape(mesh.shape["dp"], 2, 2, 2, 2), ("dp",) + CTX)
    return jax.shard_map(
        layer,
        mesh=finer,
        in_specs=(P("dp", CTX), P("dp"), P("dp", None), P(), P()),
        out_specs=P("dp", CTX, None),
        check_vma=False,
    )
```

```python
import functools

import jax
import jax.numpy as jnp
from jax import lax
from jax.experimental import pallas as pl
from jax.experimental.pallas import tpu as pltpu

BF = jnp.bfloat16
F32 = jnp.float32
BLK = 256
D = 512
GRP = 1024
PART = 64
CAP = 128
ROW8 = 8
BUNCH = 32
VM = pl.BlockSpec(memory_space=pltpu.VMEM)
SM = pl.BlockSpec(memory_space=pltpu.SMEM)
ANY = pl.BlockSpec(memory_space=pl.ANY)
PARAMS = pltpu.CompilerParams(vmem_limit_bytes=16 * 1024 * 1024)


def cost(us):
    return pl.CostEstimate(flops=int(us * 4_000_000), bytes_accessed=0, transcendentals=0)


def in_vmem(x):
    return pltpu.with_memory_space_constraint(x, pltpu.VMEM)


def twice_silu(h):
    return h + h * jnp.tanh(h)


def tn(a, b):
    return lax.dot_general(a, b, (((0,), (1,)), ((), ())), preferred_element_type=F32)


def nn(a, b):
    return jnp.dot(a, b, preferred_element_type=F32)


def gather_kernel(owners, rows_ref, count_ref, ids_ref, table_ref, out_ref, buf, sems):
    def eights(o):
        return (count_ref[o] + ROW8 - 1) // ROW8

    for o in range(owners):

        def start(j, _, o=o):
            for i in range(ROW8):
                s = j * ROW8 + i
                pltpu.make_async_copy(
                    table_ref.at[lax.shift_right_logical(rows_ref[o, s], 3)], buf.at[o * CAP + s], sems.at[o]
                ).start()
            return 0

        def clear(j, _, o=o):
            buf[pl.ds(o * CAP + j * ROW8, ROW8)] = jnp.zeros((ROW8, 8, D), BF)
            return 0

        lax.fori_loop(0, eights(o), start, 0)
        full = BUNCH // ROW8
        lax.fori_loop(eights(o), (eights(o) + full - 1) // full * full, clear, 0)
    low = (ids_ref[...] & 7).astype(F32).T
    width = BUNCH * 8
    lane = lax.broadcasted_iota(jnp.int32, (BUNCH, width), 1).astype(F32)
    slot = lax.broadcasted_iota(jnp.int32, (BUNCH, 1), 0)
    for o in range(owners):
        eight = buf.at[pl.ds(o * CAP, ROW8)]

        def wait(j, _, o=o, eight=eight):
            pltpu.make_async_copy(eight, eight, sems.at[o]).wait()
            return 0

        lax.fori_loop(0, eights(o), wait, 0)
        for b in range(CAP // BUNCH):
            dst = slice(o * CAP + b * BUNCH, o * CAP + (b + 1) * BUNCH)
            want = (8 * slot).astype(F32) + low[b * BUNCH : (b + 1) * BUNCH, o : o + 1]
            pick = (lane == want).astype(F32).astype(BF)
            got = nn(pick, buf[dst].reshape(width, D))
            out_ref[dst, :] = jnp.where(slot + b * BUNCH < count_ref[o], got, 0.0).astype(BF)


def gather_call(rows, count, groups):
    owners = rows.shape[0]
    return pl.pallas_call(
        functools.partial(gather_kernel, owners),
        out_shape=jax.ShapeDtypeStruct((owners * CAP, D), BF),
        in_specs=[SM, SM, VM, pl.BlockSpec(memory_space=pltpu.HBM)],
        out_specs=VM,
        scratch_shapes=[pltpu.VMEM((owners * CAP, 8, D), BF), pltpu.SemaphoreType.DMA((owners,))],
        compiler_params=pltpu.CompilerParams(vmem_limit_bytes=56 * 1024 * 1024),
        cost_estimate=cost(7),
        name="gather",
    )(rows, count, rows, groups)


def place_kernel(at_ref, got_ref, own_ref):
    rows, slots = own_ref.shape[0], got_ref.shape[0]
    at = jnp.broadcast_to(at_ref[...].astype(F32), (8, rows)).T[:, :1]
    slot = lax.broadcasted_iota(jnp.int32, (rows, slots), 1).astype(F32)
    own_ref[...] = nn((slot == at).astype(F32).astype(BF), got_ref[...]).astype(BF)


def place_call(at, got):
    return pl.pallas_call(
        place_kernel,
        out_shape=pltpu.VMEM((at.shape[1], D), BF),
        in_specs=[VM, VM],
        out_specs=VM,
        compiler_params=PARAMS,
        cost_estimate=cost(1.5),
        name="place",
    )(at, got)


def project(first, side, sc_ref, pieces, w_ref, k_ref, v_ref, q_ref, g_ref, x_ref, n_scr, nq_scr):
    co = sc_ref[2]
    base = first + GRP * sc_ref[3 + side]
    qo = pl.multiple_of(sc_ref[1], PART)
    wg, wv, wq, wk = (slice(D * i, D * (i + 1)) for i in range(4))
    for s, ref in enumerate(pieces):
        x = ref[...].astype(F32)
        c = x - jnp.mean(x, axis=1, keepdims=True)
        var = jnp.mean(c * c, axis=1, keepdims=True)
        n_scr[s] = (c * lax.rsqrt(var + 1e-5)).astype(BF)
    for s, ref in enumerate(pieces):
        edge = co if s == 0 else 1 - co
        n = n_scr[s]
        k = twice_silu(0.5 * nn(n, w_ref[:, wk])).astype(BF)
        v = twice_silu(0.5 * tn(w_ref[:, wv], n))
        for j in range(2):
            at = pl.multiple_of((edge + 2 * j) * BLK, BLK)
            k_ref[pl.ds(at, BLK), :] = k[j * BLK : (j + 1) * BLK]
            pos = base + at + lax.broadcasted_iota(jnp.int32, (1, BLK), 1)
            v_ref[:, pl.ds(at, BLK)] = jnp.where(pos < sc_ref[0], v[:, j * BLK : (j + 1) * BLK], 0.0).astype(BF)
            to = pl.multiple_of((edge + 2 * j) * PART, PART)
            nq_scr[pl.ds(to, PART), :] = n_scr[s, pl.ds(j * BLK + qo, PART), :]
            x_ref[pl.ds(to, PART), :] = ref[pl.ds(j * BLK + qo, PART), :]
    nq = nq_scr[...]
    q_ref[...] = twice_silu(0.5 * tn(w_ref[:, wq], nq)).astype(BF) * BF(1 / 16)
    g_ref[...] = twice_silu(0.5 * tn(w_ref[:, wg], nq)).astype(BF)


def attend(sc_ref, tiles, together):
    rid = lax.broadcasted_iota(jnp.int32, (128, 256), 0)
    col = lax.broadcasted_iota(jnp.int32, (1, 512), 1) & 255
    last_key = (col // PART) * BLK + (col % PART) + sc_ref[1]
    key = lax.broadcasted_iota(jnp.int32, (BLK, 512), 0)

    def heads(pp, _):
        steps = [
            (u, t, m, i)
            for u in range(together)
            for t in range(len(tiles))
            for m in range(len(tiles[t][2]))
            for i in range(GRP // BLK)
        ]
        queries = {}
        sums = {}

        def lanes(u):
            return pl.multiple_of((pp * together + u) * 128, 128)

        def scores(step):
            u, t, m, i = step
            if (u, t) not in queries:
                q = tiles[t][0][pl.ds(lanes(u), 128), :]
                zero = jnp.zeros_like(q)
                queries[u, t] = jnp.concatenate([jnp.where(rid < 64, q, zero), jnp.where(rid < 64, zero, q)], axis=1)
            return nn(tiles[t][2][m][0][i * BLK : (i + 1) * BLK, pl.ds(lanes(u), 128)], queries[u, t])

        def weights(step, s):
            _, t, m, i = step
            w = s + s * jnp.tanh(s)
            if tiles[t][2][m][2]:
                w = jnp.where(key + i * BLK <= last_key, w, 0.0)
            return w.astype(BF)

        def add_values(step, w):
            u, t, m, i = step
            o = [
                nn(
                    tiles[t][2][m][1][pl.ds(pl.multiple_of(lanes(u) + 64 * hh, 64), 64), i * BLK : (i + 1) * BLK],
                    w[:, 256 * hh : 256 * (hh + 1)],
                )
                for hh in range(2)
            ]
            old = sums.get((u, t))
            sums[u, t] = o if old is None else (old[0] + o[0], old[1] + o[1])

        s = scores(steps[0])
        before = None
        for n, step in enumerate(steps):
            ahead = scores(steps[n + 1]) if n + 1 < len(steps) else None
            w = weights(step, s)
            if before is not None:
                add_values(steps[n - 1], before)
            before, s = w, ahead
        add_values(steps[-1], before)
        for (u, t), pair in sums.items():
            for hh in range(2):
                tiles[t][1][pl.ds(pl.multiple_of(lanes(u) + 64 * hh, 64), 64), :] = pair[hh]
        return 0

    lax.fori_loop(0, 4 // together, heads, 0)


def near_kernel(chunk, sc_ref, *refs):
    past = refs[: 4 * chunk]
    p1, p2, w_ref, k_ref, v_ref, q_ref, g_ref, x_ref, o_ref, n_scr, nq_scr = refs[4 * chunk :]
    project(2 * GRP * chunk, 0, sc_ref, (p1, p2), w_ref, k_ref, v_ref, q_ref, g_ref, x_ref, n_scr, nq_scr)
    seen = [(past[2 * i], past[2 * i + 1], False) for i in range(2 * chunk)]
    attend(sc_ref, [(q_ref, o_ref, seen + [(k_ref, v_ref, True)])], 2)


def far_kernel(chunk, sc_ref, *refs):
    past = refs[: 4 * chunk]
    p1, p2, w_ref, wo_ref, kn, vn, qn, gn, xn, on = refs[4 * chunk : 4 * chunk + 10]
    rest = refs[4 * chunk + 10 :]
    if chunk:
        first_ref, rest = rest[0], rest[1:]
        out_ref, rest = rest[0], rest[1:]
        kf, vf = rest[-2:]
    else:
        out_ref, kf, vf = rest[:3]
        rest = rest[3:]
    n_scr, nq_scr, qf, gf, xf, of, qx, kx, vx, ox = rest[:10]
    project(2 * GRP * chunk, 1, sc_ref, (p1, p2), w_ref, kf, vf, qf, gf, xf, n_scr, nq_scr)
    low = sc_ref[3] == 0

    @pl.when(low)
    def _():
        qx[...], kx[...], vx[...] = qf[...], kn[...], vn[...]

    @pl.when(jnp.logical_not(low))
    def _():
        qx[...], kx[...], vx[...] = qn[...], kf[...], vf[...]

    seen = [(past[2 * i], past[2 * i + 1], False) for i in range(2 * chunk)]
    attend(sc_ref, [(qf, of, seen + [(kf, vf, True)]), (qx, ox, [(kx, vx, False)])], 2)
    if chunk:
        out_ref[:512, :] = first_ref[...]
    for side, (o_ref, g_ref, x_ref) in enumerate(((on, gn, xn), (of, gf, xf))):
        o = o_ref[...] + jnp.where(sc_ref[3 + side] == 1, ox[...], 0.0)
        c = o - jnp.mean(o, axis=0, keepdims=True)
        var = jnp.mean(c * c, axis=0, keepdims=True)
        gated = ((c * lax.rsqrt(var + 1e-5)) * g_ref[...].astype(F32)).astype(BF)
        mixed = lax.dot_general(gated, wo_ref[...], (((0,), (0,)), ((), ())), preferred_element_type=F32)
        out = (x_ref[...].astype(F32) + mixed).astype(BF)
        for j in range(2):
            at = pl.multiple_of(512 * chunk + 256 * j + 128 * sc_ref[3 + side], 128)
            out_ref[pl.ds(at, 128), :] = out[128 * j : 128 * (j + 1)]


SIZES = [(GRP, D), (D, GRP), (D, 256), (D, 256), (256, D)]


def near_call(chunk, sc, past, own, near, w_in):
    inputs = [*past, own, near, w_in]
    outs = pl.pallas_call(
        functools.partial(near_kernel, chunk),
        out_shape=[pltpu.VMEM(s, BF) for s in SIZES] + [pltpu.VMEM((D, 256), F32)],
        in_specs=[SM] + [VM] * len(inputs),
        out_specs=[VM] * 6,
        scratch_shapes=[pltpu.VMEM((2, D, D), BF), pltpu.VMEM((256, D), BF)],
        compiler_params=PARAMS,
        cost_estimate=cost(6 + 6 * chunk),
    )(sc, *inputs)
    return outs


def far_call(chunk, sc, past, far, diag, w_in, w_out, kept, first):
    inputs = [*past, far, diag, w_in, w_out, *kept]
    scratch = [
        pltpu.VMEM((2, D, D), BF),
        pltpu.VMEM((256, D), BF),
        pltpu.VMEM((D, 256), BF),
        pltpu.VMEM((D, 256), BF),
        pltpu.VMEM((256, D), BF),
        pltpu.VMEM((D, 256), F32),
        pltpu.VMEM((D, 256), BF),
        pltpu.VMEM((GRP, D), BF),
        pltpu.VMEM((D, GRP), BF),
        pltpu.VMEM((D, 256), F32),
    ]
    held = [pltpu.VMEM(s, BF) for s in SIZES[:2]]
    if chunk:
        inputs.append(first)
        shapes, scratch = [jax.ShapeDtypeStruct((1024, D), BF)], scratch + held
    else:
        shapes = [pltpu.VMEM((512, D), BF)] + held
    return pl.pallas_call(
        functools.partial(far_kernel, chunk),
        out_shape=shapes,
        in_specs=[SM] + [VM] * len(inputs),
        out_specs=[VM] * len(shapes),
        scratch_shapes=scratch,
        compiler_params=PARAMS,
        cost_estimate=cost(9 + 5 * chunk),
    )(sc, *inputs)


from jax.sharding import Mesh
from jax.sharding import PartitionSpec as P

CTX = ("xh", "xl", "yh", "co")
FLIP = [(0, 1), (1, 0)]


def layer(item_ids, lengths, table, w_in, w_out):
    owned = table.shape[0]
    me = lax.axis_index("dp")
    xh, xl, yh, co = (lax.axis_index(a) for a in CTX)
    owners = lax.axis_size("dp")
    w_in, w_out = in_vmem(w_in), in_vmem(w_out)
    groups = table.reshape(-1, 8, D)

    send = jnp.broadcast_to(item_ids[None, :, None], (owners, 4, 1, BLK)).reshape(owners * 4, 1, BLK)
    wanted = lax.all_to_all(send, ("dp", "xh", "yh"), 0, 0, tiled=True).reshape(owners, 4, BLK)
    mine = lax.dynamic_index_in_dim(wanted, me, 0, keepdims=False)
    user = 2 * xh + yh
    length = jnp.sum(jnp.where(lax.iota(jnp.int32, 4) == user, lengths, 0))
    upto = jnp.triu(jnp.ones((2 * BLK, 2 * BLK), BF))
    slots = lax.iota(jnp.int32, 8)
    sc = jnp.zeros((8,), jnp.int32)
    for i, value in enumerate((length, PART * (2 * xl + co), co, xl, 1 - xl)):
        sc = jnp.where(slots == i, value, sc)

    def ranks(member):
        return nn(member.astype(BF), upto).astype(jnp.int32) - 1

    def fetch(c):
        ids = wanted[:, 2 * c : 2 * c + 2].reshape(owners, 2 * BLK)
        local = ids - me * owned
        here = (local >= 0) & (local < owned)
        rank = jnp.where(here, ranks(here), -1)
        slot = lax.broadcasted_iota(jnp.int32, (owners, CAP, 2 * BLK), 1)
        rows = jnp.sum(jnp.where(rank[:, None, :] == slot, local[:, None, :], 0), axis=2)
        count = jnp.sum(here.astype(jnp.int32), axis=1)
        picked = gather_call(rows, count, groups).reshape(owners, CAP, D)
        return lax.all_to_all(picked, "dp", 0, 0, tiled=True).reshape(owners * CAP, D)

    def place(c, got):
        own_ids = mine[2 * c : 2 * c + 2].reshape(2 * BLK)
        owner = own_ids // owned
        member = owner[None, :] == lax.broadcasted_iota(jnp.int32, (owners, 2 * BLK), 0)
        at = jnp.sum(jnp.where(member, ranks(member), 0), axis=0) + owner * CAP
        return in_vmem(place_call(at[None], got))

    past, first = [], None
    for c in range(2):
        got = fetch(c)
        own = place(c, got)
        far = lax.ppermute(own, "xl", FLIP)
        near = lax.ppermute(own, "co", FLIP)
        diag = lax.ppermute(far, "co", FLIP)
        pieces = [in_vmem(a) for a in (own, near, far, diag)]
        kept = near_call(c, sc, past, *pieces[:2], w_in)
        kept = [in_vmem(a) for a in kept]
        done = far_call(c, sc, past, *pieces[2:], w_in, w_out, kept, first)
        if c == 0:
            first, k1, v1 = (in_vmem(a) for a in done)
            past = [*kept[:2], k1, v1]
    back = lax.all_to_all(done[0].reshape(16, PART, D), ("xh", "yh", "xl", "co"), 0, 0, tiled=True)
    return back.reshape(4, BLK, D)


def solution(mesh):
    finer = Mesh(mesh.devices.reshape(mesh.shape["dp"], 2, 2, 2, 2), ("dp",) + CTX)
    return jax.shard_map(
        layer,
        mesh=finer,
        in_specs=(P("dp", CTX), P("dp"), P("dp", None), P(), P()),
        out_specs=P("dp", CTX, None),
        check_vma=False,
    )
```

```python
import functools

import jax
import jax.numpy as jnp
from jax import lax
from jax.experimental import pallas as pl
from jax.experimental.pallas import tpu as pltpu

BF = jnp.bfloat16
F32 = jnp.float32
BLK = 256
D = 512
GRP = 1024
PART = 64
CAP = 128
ROW8 = 8
BUNCH = 32
VM = pl.BlockSpec(memory_space=pltpu.VMEM)
SM = pl.BlockSpec(memory_space=pltpu.SMEM)
ANY = pl.BlockSpec(memory_space=pl.ANY)
PARAMS = pltpu.CompilerParams(vmem_limit_bytes=16 * 1024 * 1024)


def cost(us):
    return pl.CostEstimate(flops=int(us * 4_000_000), bytes_accessed=0, transcendentals=0)


def in_vmem(x):
    return pltpu.with_memory_space_constraint(x, pltpu.VMEM)


def twice_silu(h):
    return h + h * jnp.tanh(h)


def tn(a, b):
    return lax.dot_general(a, b, (((0,), (1,)), ((), ())), preferred_element_type=F32)


def nn(a, b):
    return jnp.dot(a, b, preferred_element_type=F32)


def gather_kernel(owners, outs, rows_ref, count_ref, ids_ref, table_ref, *refs):
    out_refs, (buf, sems) = refs[:outs], refs[outs:]
    me = lax.axis_index("dp") if outs > 1 else 0

    def who(k):
        return jnp.bitwise_xor(me, k) if outs > 1 else k

    def eights(k):
        return (count_ref[who(k)] + ROW8 - 1) // ROW8

    for k in range(owners):
        o = who(k)

        def start(j, _, k=k, o=o):
            for i in range(ROW8):
                s = j * ROW8 + i
                pltpu.make_async_copy(
                    table_ref.at[lax.shift_right_logical(rows_ref[o, s], 3)], buf.at[k * CAP + s], sems.at[k]
                ).start()
            return 0

        def clear(j, _, k=k):
            buf[pl.ds(k * CAP + j * ROW8, ROW8)] = jnp.zeros((ROW8, 8, D), BF)
            return 0

        lax.fori_loop(0, eights(k), start, 0)
        full = BUNCH // ROW8
        lax.fori_loop(eights(k), (eights(k) + full - 1) // full * full, clear, 0)
    width = BUNCH * 8
    lane = lax.broadcasted_iota(jnp.int32, (BUNCH, width), 1).astype(F32)
    slot = lax.broadcasted_iota(jnp.int32, (BUNCH, 1), 0)
    for k in range(owners):
        o = who(k)
        eight = buf.at[pl.ds(k * CAP, ROW8)]
        low = jnp.broadcast_to((ids_ref[pl.ds(o, 1), :] & 7).astype(F32), (8, CAP)).T[:, :1]

        def wait(j, _, k=k, eight=eight):
            pltpu.make_async_copy(eight, eight, sems.at[k]).wait()
            return 0

        lax.fori_loop(0, eights(k), wait, 0)
        for b in range(CAP // BUNCH):
            want = (8 * slot).astype(F32) + low[b * BUNCH : (b + 1) * BUNCH]
            pick = (lane == want).astype(F32).astype(BF)
            at = k * CAP + b * BUNCH
            got = nn(pick, buf[at : at + BUNCH].reshape(width, D))
            got = jnp.where(slot + b * BUNCH < count_ref[o], got, 0.0).astype(BF)
            if outs > 1:
                out_refs[k][b * BUNCH : (b + 1) * BUNCH, :] = got
            else:
                out_refs[0][at : at + BUNCH, :] = got


def gather_call(rows, count, groups, outs):
    owners = rows.shape[0]
    shape = jax.ShapeDtypeStruct((owners // outs * CAP, D), BF)
    return pl.pallas_call(
        functools.partial(gather_kernel, owners, outs),
        out_shape=[shape] * outs,
        in_specs=[SM, SM, VM, pl.BlockSpec(memory_space=pltpu.HBM)],
        out_specs=[VM] * outs,
        scratch_shapes=[pltpu.VMEM((owners * CAP, 8, D), BF), pltpu.SemaphoreType.DMA((owners,))],
        compiler_params=pltpu.CompilerParams(vmem_limit_bytes=56 * 1024 * 1024),
        cost_estimate=cost(7),
    )(rows, count, rows, groups)


def place_kernel(at_ref, *refs):
    pieces, own_ref = refs[:-1], refs[-1]
    rows = own_ref.shape[0]
    at = jnp.broadcast_to(at_ref[...].astype(F32), (8, rows)).T[:, :1]
    lane = lax.broadcasted_iota(jnp.int32, (rows, 2 * CAP), 1).astype(F32)
    own = None
    for j in range(len(pieces) // 2):
        got = jnp.concatenate([pieces[2 * j][...], pieces[2 * j + 1][...]], axis=0)
        part = nn((lane + 2.0 * CAP * j == at).astype(F32).astype(BF), got)
        own = part if own is None else own + part
    own_ref[...] = own.astype(BF)


def place_call(at, pieces):
    return pl.pallas_call(
        place_kernel,
        out_shape=pltpu.VMEM((at.shape[1], D), BF),
        in_specs=[VM] * (1 + len(pieces)),
        out_specs=VM,
        compiler_params=PARAMS,
        cost_estimate=cost(1.5),
        name="place",
    )(at, *pieces)


def project(first, side, sc_ref, pieces, w_ref, k_ref, v_ref, q_ref, g_ref, x_ref, n_scr, nq_scr):
    co = sc_ref[2]
    base = first + GRP * sc_ref[3 + side]
    qo = pl.multiple_of(sc_ref[1], PART)
    wg, wv, wq, wk = (slice(D * i, D * (i + 1)) for i in range(4))
    for s, ref in enumerate(pieces):
        x = ref[...].astype(F32)
        c = x - jnp.mean(x, axis=1, keepdims=True)
        var = jnp.mean(c * c, axis=1, keepdims=True)
        n_scr[s] = (c * lax.rsqrt(var + 1e-5)).astype(BF)
    for s, ref in enumerate(pieces):
        edge = co if s == 0 else 1 - co
        n = n_scr[s]
        k = twice_silu(0.5 * nn(n, w_ref[:, wk])).astype(BF)
        v = twice_silu(0.5 * tn(w_ref[:, wv], n))
        for j in range(2):
            at = pl.multiple_of((edge + 2 * j) * BLK, BLK)
            k_ref[pl.ds(at, BLK), :] = k[j * BLK : (j + 1) * BLK]
            pos = base + at + lax.broadcasted_iota(jnp.int32, (1, BLK), 1)
            v_ref[:, pl.ds(at, BLK)] = jnp.where(pos < sc_ref[0], v[:, j * BLK : (j + 1) * BLK], 0.0).astype(BF)
            to = pl.multiple_of((edge + 2 * j) * PART, PART)
            nq_scr[pl.ds(to, PART), :] = n_scr[s, pl.ds(j * BLK + qo, PART), :]
            x_ref[pl.ds(to, PART), :] = ref[pl.ds(j * BLK + qo, PART), :]
    nq = nq_scr[...]
    q_ref[...] = twice_silu(0.5 * tn(w_ref[:, wq], nq)).astype(BF) * BF(1 / 16)
    g_ref[...] = twice_silu(0.5 * tn(w_ref[:, wg], nq)).astype(BF)


def attend(sc_ref, tiles, together):
    rid = lax.broadcasted_iota(jnp.int32, (128, 256), 0)
    col = lax.broadcasted_iota(jnp.int32, (1, 512), 1) & 255
    last_key = (col // PART) * BLK + (col % PART) + sc_ref[1]
    key = lax.broadcasted_iota(jnp.int32, (BLK, 512), 0)

    def heads(pp, _):
        steps = [
            (u, t, m, i)
            for u in range(together)
            for t in range(len(tiles))
            for m in range(len(tiles[t][2]))
            for i in range(GRP // BLK)
        ]
        queries = {}
        sums = {}

        def lanes(u):
            return pl.multiple_of((pp * together + u) * 128, 128)

        def scores(step):
            u, t, m, i = step
            if (u, t) not in queries:
                q = tiles[t][0][pl.ds(lanes(u), 128), :]
                zero = jnp.zeros_like(q)
                queries[u, t] = jnp.concatenate([jnp.where(rid < 64, q, zero), jnp.where(rid < 64, zero, q)], axis=1)
            return nn(tiles[t][2][m][0][i * BLK : (i + 1) * BLK, pl.ds(lanes(u), 128)], queries[u, t])

        def weights(step, s):
            _, t, m, i = step
            w = s + s * jnp.tanh(s)
            if tiles[t][2][m][2]:
                w = jnp.where(key + i * BLK <= last_key, w, 0.0)
            return w.astype(BF)

        def add_values(step, w):
            u, t, m, i = step
            o = [
                nn(
                    tiles[t][2][m][1][pl.ds(pl.multiple_of(lanes(u) + 64 * hh, 64), 64), i * BLK : (i + 1) * BLK],
                    w[:, 256 * hh : 256 * (hh + 1)],
                )
                for hh in range(2)
            ]
            old = sums.get((u, t))
            sums[u, t] = o if old is None else (old[0] + o[0], old[1] + o[1])

        s = scores(steps[0])
        before = None
        for n, step in enumerate(steps):
            ahead = scores(steps[n + 1]) if n + 1 < len(steps) else None
            w = weights(step, s)
            if before is not None:
                add_values(steps[n - 1], before)
            before, s = w, ahead
        add_values(steps[-1], before)
        for (u, t), pair in sums.items():
            for hh in range(2):
                tiles[t][1][pl.ds(pl.multiple_of(lanes(u) + 64 * hh, 64), 64), :] = pair[hh]
        return 0

    lax.fori_loop(0, 4 // together, heads, 0)


def near_kernel(chunk, sc_ref, *refs):
    past = refs[: 4 * chunk]
    p1, p2, w_ref, k_ref, v_ref, q_ref, g_ref, x_ref, o_ref, n_scr, nq_scr = refs[4 * chunk :]
    project(2 * GRP * chunk, 0, sc_ref, (p1, p2), w_ref, k_ref, v_ref, q_ref, g_ref, x_ref, n_scr, nq_scr)
    seen = [(past[2 * i], past[2 * i + 1], False) for i in range(2 * chunk)]
    attend(sc_ref, [(q_ref, o_ref, seen + [(k_ref, v_ref, True)])], 2)


def far_kernel(chunk, sc_ref, *refs):
    past = refs[: 4 * chunk]
    p1, p2, w_ref, wo_ref, kn, vn, qn, gn, xn, on = refs[4 * chunk : 4 * chunk + 10]
    rest = refs[4 * chunk + 10 :]
    if chunk:
        first_ref, rest = rest[0], rest[1:]
        out_ref, rest = rest[0], rest[1:]
        kf, vf = rest[-2:]
    else:
        out_ref, kf, vf = rest[:3]
        rest = rest[3:]
    n_scr, nq_scr, qf, gf, xf, of, qx, kx, vx, ox = rest[:10]
    project(2 * GRP * chunk, 1, sc_ref, (p1, p2), w_ref, kf, vf, qf, gf, xf, n_scr, nq_scr)
    low = sc_ref[3] == 0

    @pl.when(low)
    def _():
        qx[...], kx[...], vx[...] = qf[...], kn[...], vn[...]

    @pl.when(jnp.logical_not(low))
    def _():
        qx[...], kx[...], vx[...] = qn[...], kf[...], vf[...]

    seen = [(past[2 * i], past[2 * i + 1], False) for i in range(2 * chunk)]
    attend(sc_ref, [(qf, of, seen + [(kf, vf, True)]), (qx, ox, [(kx, vx, False)])], 2)
    if chunk:
        out_ref[:512, :] = first_ref[...]
    for side, (o_ref, g_ref, x_ref) in enumerate(((on, gn, xn), (of, gf, xf))):
        o = o_ref[...] + jnp.where(sc_ref[3 + side] == 1, ox[...], 0.0)
        c = o - jnp.mean(o, axis=0, keepdims=True)
        var = jnp.mean(c * c, axis=0, keepdims=True)
        gated = ((c * lax.rsqrt(var + 1e-5)) * g_ref[...].astype(F32)).astype(BF)
        mixed = lax.dot_general(gated, wo_ref[...], (((0,), (0,)), ((), ())), preferred_element_type=F32)
        out = (x_ref[...].astype(F32) + mixed).astype(BF)
        for j in range(2):
            at = pl.multiple_of(512 * chunk + 256 * j + 128 * sc_ref[3 + side], 128)
            out_ref[pl.ds(at, 128), :] = out[128 * j : 128 * (j + 1)]


SIZES = [(GRP, D), (D, GRP), (D, 256), (D, 256), (256, D)]


def near_call(chunk, sc, past, own, near, w_in):
    inputs = [*past, own, near, w_in]
    outs = pl.pallas_call(
        functools.partial(near_kernel, chunk),
        out_shape=[pltpu.VMEM(s, BF) for s in SIZES] + [pltpu.VMEM((D, 256), F32)],
        in_specs=[SM] + [VM] * len(inputs),
        out_specs=[VM] * 6,
        scratch_shapes=[pltpu.VMEM((2, D, D), BF), pltpu.VMEM((256, D), BF)],
        compiler_params=PARAMS,
        cost_estimate=cost(6 + 6 * chunk),
    )(sc, *inputs)
    return outs


def far_call(chunk, sc, past, far, diag, w_in, w_out, kept, first):
    inputs = [*past, far, diag, w_in, w_out, *kept]
    scratch = [
        pltpu.VMEM((2, D, D), BF),
        pltpu.VMEM((256, D), BF),
        pltpu.VMEM((D, 256), BF),
        pltpu.VMEM((D, 256), BF),
        pltpu.VMEM((256, D), BF),
        pltpu.VMEM((D, 256), F32),
        pltpu.VMEM((D, 256), BF),
        pltpu.VMEM((GRP, D), BF),
        pltpu.VMEM((D, GRP), BF),
        pltpu.VMEM((D, 256), F32),
    ]
    held = [pltpu.VMEM(s, BF) for s in SIZES[:2]]
    if chunk:
        inputs.append(first)
        shapes, scratch = [jax.ShapeDtypeStruct((1024, D), BF)], scratch + held
    else:
        shapes = [pltpu.VMEM((512, D), BF)] + held
    return pl.pallas_call(
        functools.partial(far_kernel, chunk),
        out_shape=shapes,
        in_specs=[SM] + [VM] * len(inputs),
        out_specs=[VM] * len(shapes),
        scratch_shapes=scratch,
        compiler_params=PARAMS,
        cost_estimate=cost(9 + 5 * chunk),
    )(sc, *inputs)


from jax.sharding import Mesh
from jax.sharding import PartitionSpec as P

CTX = ("xh", "xl", "yh", "co")
FLIP = [(0, 1), (1, 0)]
EARLY, LATE = (7, 6, 5), (4, 2, 3, 1)


def layer(item_ids, lengths, table, w_in, w_out):
    owned = table.shape[0]
    me = lax.axis_index("dp")
    xh, xl, yh, co = (lax.axis_index(a) for a in CTX)
    owners = lax.axis_size("dp")
    w_in, w_out = in_vmem(w_in), in_vmem(w_out)
    groups = table.reshape(-1, 8, D)

    send = jnp.broadcast_to(item_ids[None, :, None], (owners, 4, 1, BLK)).reshape(owners * 4, 1, BLK)
    wanted = lax.all_to_all(send, ("dp", "xh", "yh"), 0, 0, tiled=True).reshape(owners, 4, BLK)
    mine = lax.dynamic_index_in_dim(wanted, me, 0, keepdims=False)
    user = 2 * xh + yh
    length = jnp.sum(jnp.where(lax.iota(jnp.int32, 4) == user, lengths, 0))
    upto = jnp.triu(jnp.ones((2 * BLK, 2 * BLK), BF))
    slots = lax.iota(jnp.int32, 8)
    sc = jnp.zeros((8,), jnp.int32)
    for i, value in enumerate((length, PART * (2 * xl + co), co, xl, 1 - xl)):
        sc = jnp.where(slots == i, value, sc)

    def ranks(member):
        return nn(member.astype(BF), upto).astype(jnp.int32) - 1

    def fetch(c):
        ids = wanted[:, 2 * c : 2 * c + 2].reshape(owners, 2 * BLK)
        local = ids - me * owned
        here = (local >= 0) & (local < owned)
        rank = jnp.where(here, ranks(here), -1)
        slot = lax.broadcasted_iota(jnp.int32, (owners, CAP, 2 * BLK), 1)
        rows = jnp.sum(jnp.where(rank[:, None, :] == slot, local[:, None, :], 0), axis=2)
        count = jnp.sum(here.astype(jnp.int32), axis=1)
        if c == 0:
            picked = gather_call(rows, count, groups, 1)[0].reshape(owners, CAP, D)
            return lax.all_to_all(picked, "dp", 0, 0, tiled=True).reshape(owners * CAP, D)
        picked = gather_call(rows, count, groups, owners)
        return picked

    def swap(picked, k):
        return lax.ppermute(picked[k], "dp", [(i, i ^ k) for i in range(owners)])

    def places(c):
        own_ids = mine[2 * c : 2 * c + 2].reshape(2 * BLK)
        owner = own_ids // owned
        member = owner[None, :] == lax.broadcasted_iota(jnp.int32, (owners, 2 * BLK), 0)
        rank = jnp.sum(jnp.where(member, ranks(member), 0), axis=0)
        return rank + (owner if c == 0 else owner ^ me) * CAP

    def place(c, got):
        at = places(c)
        if c:
            return in_vmem(place_call(at[None], got))
        pick = (at[:, None] == lax.broadcasted_iota(jnp.int32, (2 * BLK, owners * CAP), 1)).astype(BF)
        return nn(pick, got).astype(BF)

    past, first = [], None
    for c in range(2):
        got = fetch(c)
        if c:
            early = [swap(got, k) for k in EARLY]
            late = [swap(got, k) for k in LATE]
            received = dict(zip(EARLY + LATE, early + late))
            got = [got[0]] + [received[k] for k in range(1, owners)]
            got = [in_vmem(a) for a in got]
        own = place(c, got)
        far = lax.ppermute(own, "xl", FLIP)
        near = lax.ppermute(own, "co", FLIP)
        diag = lax.ppermute(far, "co", FLIP)
        pieces = [in_vmem(a) for a in (own, near, far, diag)]
        kept = near_call(c, sc, past, *pieces[:2], w_in)
        kept = [in_vmem(a) for a in kept]
        done = far_call(c, sc, past, *pieces[2:], w_in, w_out, kept, first)
        if c == 0:
            first, k1, v1 = (in_vmem(a) for a in done)
            past = [*kept[:2], k1, v1]
    back = lax.all_to_all(done[0].reshape(16, PART, D), ("xh", "yh", "xl", "co"), 0, 0, tiled=True)
    return back.reshape(4, BLK, D)


def solution(mesh):
    finer = Mesh(mesh.devices.reshape(mesh.shape["dp"], 2, 2, 2, 2), ("dp",) + CTX)
    return jax.shard_map(
        layer,
        mesh=finer,
        in_specs=(P("dp", CTX), P("dp"), P("dp", None), P(), P()),
        out_specs=P("dp", CTX, None),
        check_vma=False,
    )
```

```python
import functools

import jax
import jax.numpy as jnp
from jax import lax
from jax.experimental import pallas as pl
from jax.experimental.pallas import tpu as pltpu

BF = jnp.bfloat16
F32 = jnp.float32
BLK = 256
D = 512
GRP = 1024
PART = 64
CAP = 128
ROW8 = 8
BUNCH = 32
VM = pl.BlockSpec(memory_space=pltpu.VMEM)
SM = pl.BlockSpec(memory_space=pltpu.SMEM)
ANY = pl.BlockSpec(memory_space=pl.ANY)
PARAMS = pltpu.CompilerParams(vmem_limit_bytes=16 * 1024 * 1024)


def cost(us):
    return pl.CostEstimate(flops=int(us * 4_000_000), bytes_accessed=0, transcendentals=0)


def in_vmem(x):
    return pltpu.with_memory_space_constraint(x, pltpu.VMEM)


def twice_silu(h):
    return h + h * jnp.tanh(h)


def tn(a, b):
    return lax.dot_general(a, b, (((0,), (1,)), ((), ())), preferred_element_type=F32)


def nn(a, b):
    return jnp.dot(a, b, preferred_element_type=F32)


def gather_kernel(owners, outs, rows_ref, count_ref, ids_ref, table_ref, *refs):
    out_refs, (buf, sems) = refs[:outs], refs[outs:]
    me = lax.axis_index("dp") if outs > 1 else 0

    def who(k):
        return jnp.bitwise_xor(me, k) if outs > 1 else k

    def eights(k):
        return (count_ref[who(k)] + ROW8 - 1) // ROW8

    for k in range(owners):
        o = who(k)

        def start(j, _, k=k, o=o):
            for i in range(ROW8):
                s = j * ROW8 + i
                pltpu.make_async_copy(
                    table_ref.at[lax.shift_right_logical(rows_ref[o, s], 3)], buf.at[k * CAP + s], sems.at[k]
                ).start()
            return 0

        def clear(j, _, k=k):
            buf[pl.ds(k * CAP + j * ROW8, ROW8)] = jnp.zeros((ROW8, 8, D), BF)
            return 0

        lax.fori_loop(0, eights(k), start, 0)
        full = BUNCH // ROW8
        lax.fori_loop(eights(k), (eights(k) + full - 1) // full * full, clear, 0)
    width = BUNCH * 8
    lane = lax.broadcasted_iota(jnp.int32, (BUNCH, width), 1).astype(F32)
    slot = lax.broadcasted_iota(jnp.int32, (BUNCH, 1), 0)
    for k in range(owners):
        eight = buf.at[pl.ds(k * CAP, ROW8)]

        def wait(j, _, k=k, eight=eight):
            pltpu.make_async_copy(eight, eight, sems.at[k]).wait()
            return 0

        lax.fori_loop(0, eights(k), wait, 0)
    low8 = (ids_ref[...] & 7).astype(F32).T
    for k in range(owners):
        o = who(k)
        if outs > 1:
            low = jnp.broadcast_to((ids_ref[pl.ds(o, 1), :] & 7).astype(F32), (8, CAP)).T[:, :1]
        else:
            low = low8[:, k : k + 1]
        for b in range(CAP // BUNCH):
            want = (8 * slot).astype(F32) + low[b * BUNCH : (b + 1) * BUNCH]
            pick = (lane == want).astype(F32).astype(BF)
            at = k * CAP + b * BUNCH
            got = nn(pick, buf[at : at + BUNCH].reshape(width, D))
            got = jnp.where(slot + b * BUNCH < count_ref[o], got, 0.0).astype(BF)
            if outs > 1:
                out_refs[k][b * BUNCH : (b + 1) * BUNCH, :] = got
            else:
                out_refs[0][at : at + BUNCH, :] = got


def gather_call(rows, count, groups, outs):
    owners = rows.shape[0]
    shape = jax.ShapeDtypeStruct((owners // outs * CAP, D), BF)
    return pl.pallas_call(
        functools.partial(gather_kernel, owners, outs),
        out_shape=[shape] * outs,
        in_specs=[SM, SM, VM, pl.BlockSpec(memory_space=pltpu.HBM)],
        out_specs=[VM] * outs,
        scratch_shapes=[pltpu.VMEM((owners * CAP, 8, D), BF), pltpu.SemaphoreType.DMA((owners,))],
        compiler_params=pltpu.CompilerParams(vmem_limit_bytes=56 * 1024 * 1024),
        cost_estimate=cost(7),
    )(rows, count, rows, groups)


def project(first, side, sc_ref, pieces, w_ref, k_ref, v_ref, q_ref, g_ref, x_ref, n_scr, nq_scr):
    co = sc_ref[2]
    base = first + GRP * sc_ref[3 + side]
    qo = pl.multiple_of(sc_ref[1], PART)
    wg, wv, wq, wk = (slice(D * i, D * (i + 1)) for i in range(4))
    for s, ref in enumerate(pieces):
        x = ref[...].astype(F32)
        c = x - jnp.mean(x, axis=1, keepdims=True)
        var = jnp.mean(c * c, axis=1, keepdims=True)
        n_scr[s] = (c * lax.rsqrt(var + 1e-5)).astype(BF)
    for s, ref in enumerate(pieces):
        edge = co if s == 0 else 1 - co
        n = n_scr[s]
        k = twice_silu(0.5 * nn(n, w_ref[:, wk])).astype(BF)
        v = twice_silu(0.5 * tn(w_ref[:, wv], n))
        for j in range(2):
            at = pl.multiple_of((edge + 2 * j) * BLK, BLK)
            k_ref[pl.ds(at, BLK), :] = k[j * BLK : (j + 1) * BLK]
            pos = base + at + lax.broadcasted_iota(jnp.int32, (1, BLK), 1)
            v_ref[:, pl.ds(at, BLK)] = jnp.where(pos < sc_ref[0], v[:, j * BLK : (j + 1) * BLK], 0.0).astype(BF)
            to = pl.multiple_of((edge + 2 * j) * PART, PART)
            nq_scr[pl.ds(to, PART), :] = n_scr[s, pl.ds(j * BLK + qo, PART), :]
            x_ref[pl.ds(to, PART), :] = ref[pl.ds(j * BLK + qo, PART), :]
    nq = nq_scr[...]
    q_ref[...] = twice_silu(0.5 * tn(w_ref[:, wq], nq)).astype(BF) * BF(1 / 16)
    g_ref[...] = twice_silu(0.5 * tn(w_ref[:, wg], nq)).astype(BF)


def attend(sc_ref, tiles, together):
    rid = lax.broadcasted_iota(jnp.int32, (128, 256), 0)
    col = lax.broadcasted_iota(jnp.int32, (1, 512), 1) & 255
    last_key = (col // PART) * BLK + (col % PART) + sc_ref[1]
    key = lax.broadcasted_iota(jnp.int32, (BLK, 512), 0)

    def heads(pp, _):
        steps = [
            (u, t, m, i)
            for u in range(together)
            for t in range(len(tiles))
            for m in range(len(tiles[t][2]))
            for i in range(GRP // BLK)
        ]
        queries = {}
        sums = {}

        def lanes(u):
            return pl.multiple_of((pp * together + u) * 128, 128)

        def scores(step):
            u, t, m, i = step
            if (u, t) not in queries:
                q = tiles[t][0][pl.ds(lanes(u), 128), :]
                zero = jnp.zeros_like(q)
                queries[u, t] = jnp.concatenate([jnp.where(rid < 64, q, zero), jnp.where(rid < 64, zero, q)], axis=1)
            return nn(tiles[t][2][m][0][i * BLK : (i + 1) * BLK, pl.ds(lanes(u), 128)], queries[u, t])

        def weights(step, s):
            _, t, m, i = step
            w = s + s * jnp.tanh(s)
            if tiles[t][2][m][2]:
                w = jnp.where(key + i * BLK <= last_key, w, 0.0)
            return w.astype(BF)

        def add_values(step, w):
            u, t, m, i = step
            o = [
                nn(
                    tiles[t][2][m][1][pl.ds(pl.multiple_of(lanes(u) + 64 * hh, 64), 64), i * BLK : (i + 1) * BLK],
                    w[:, 256 * hh : 256 * (hh + 1)],
                )
                for hh in range(2)
            ]
            old = sums.get((u, t))
            sums[u, t] = o if old is None else (old[0] + o[0], old[1] + o[1])

        s = scores(steps[0])
        before = None
        for n, step in enumerate(steps):
            ahead = scores(steps[n + 1]) if n + 1 < len(steps) else None
            w = weights(step, s)
            if before is not None:
                add_values(steps[n - 1], before)
            before, s = w, ahead
        add_values(steps[-1], before)
        for (u, t), pair in sums.items():
            for hh in range(2):
                tiles[t][1][pl.ds(pl.multiple_of(lanes(u) + 64 * hh, 64), 64), :] = pair[hh]
        return 0

    lax.fori_loop(0, 4 // together, heads, 0)


def near0_kernel(sc_ref, p1, p2, w_ref, *refs):
    outs, held, (n_scr, nq_scr, sems) = refs[:6], refs[6:12], refs[12:]
    k, v, q, g, x, o = held
    copies = [pltpu.make_async_copy(src, dst, sems.at[i]) for i, (src, dst) in enumerate(zip(held, outs))]
    project(0, 0, sc_ref, (p1, p2), w_ref, k, v, q, g, x, n_scr, nq_scr)
    for c in copies[:5]:
        c.start()
    attend(sc_ref, [(q, o, [(k, v, True)])], 2)
    copies[5].start()
    for c in copies:
        c.wait()


def near1_kernel(sc_ref, p1, p2, w_ref, k_ref, v_ref, q_ref, g_ref, x_ref, o_ref, n_scr, nq_scr):
    project(2 * GRP, 0, sc_ref, (p1, p2), w_ref, k_ref, v_ref, q_ref, g_ref, x_ref, n_scr, nq_scr)
    attend(sc_ref, [(q_ref, o_ref, [(k_ref, v_ref, True)])], 2)


def past_kernel(sc_ref, k0, v0, k1, v1, q_ref, before_ref, o_ref):
    attend(sc_ref, [(q_ref, o_ref, [(k0, v0, False), (k1, v1, False)])], 2)
    o_ref[...] = o_ref[...] + before_ref[...]


def finish(chunk, sc_ref, wo_ref, ox, sides, out_ref):
    for side, (o_ref, g_ref, x_ref) in enumerate(sides):
        o = o_ref[...] + jnp.where(sc_ref[3 + side] == 1, ox[...], 0.0)
        c = o - jnp.mean(o, axis=0, keepdims=True)
        var = jnp.mean(c * c, axis=0, keepdims=True)
        gated = ((c * lax.rsqrt(var + 1e-5)) * g_ref[...].astype(F32)).astype(BF)
        mixed = lax.dot_general(gated, wo_ref[...], (((0,), (0,)), ((), ())), preferred_element_type=F32)
        out = (x_ref[...].astype(F32) + mixed).astype(BF)
        for j in range(2):
            at = pl.multiple_of(512 * chunk + 256 * j + 128 * sc_ref[3 + side], 128)
            out_ref[pl.ds(at, 128), :] = out[128 * j : 128 * (j + 1)]


def far_core(chunk, sc_ref, past, p1, p2, w_ref, wo_ref, kept, arrive, out_ref, kf, vf, scratch):
    n_scr, nq_scr, qf, gf, xf, of, qx, kx, vx, ox = scratch
    kn, vn, qn, gn, xn, on = kept
    project(2 * GRP * chunk, 1, sc_ref, (p1, p2), w_ref, kf, vf, qf, gf, xf, n_scr, nq_scr)
    for c in arrive:
        c.wait()
    low = sc_ref[3] == 0

    @pl.when(low)
    def _():
        qx[...], kx[...], vx[...] = qf[...], kn[...], vn[...]

    @pl.when(jnp.logical_not(low))
    def _():
        qx[...], kx[...], vx[...] = qn[...], kf[...], vf[...]

    seen = [(past[2 * i], past[2 * i + 1], False) for i in range(2 * chunk)]
    attend(sc_ref, [(qf, of, seen + [(kf, vf, True)]), (qx, ox, [(kx, vx, False)])], 2)
    finish(chunk, sc_ref, wo_ref, ox, ((on, gn, xn), (of, gf, xf)), out_ref)


def far0_kernel(sc_ref, p1, p2, w_ref, wo_ref, *refs):
    sent, (out_ref, kn, vn, kf, vf), rest = refs[:6], refs[6:11], refs[11:]
    kept = (kn, vn, *rest[:4])
    sems = rest[-1]
    arrive = [pltpu.make_async_copy(src, dst, sems.at[i]) for i, (src, dst) in enumerate(zip(sent, kept))]
    for c in arrive:
        c.start()
    far_core(0, sc_ref, (), p1, p2, w_ref, wo_ref, kept, arrive, out_ref, kf, vf, rest[4:-1])


def far1_kernel(sc_ref, *refs):
    past, (p1, p2, w_ref, wo_ref), kept = refs[:4], refs[4:8], refs[8:14]
    first_ref, out_ref = refs[14:16]
    scratch, (kf, vf) = refs[16:26], refs[26:]
    far_core(1, sc_ref, past, p1, p2, w_ref, wo_ref, kept, (), out_ref, kf, vf, scratch)
    out_ref[:512, :] = first_ref[...]


SIZES = [(GRP, D), (D, GRP), (D, 256), (D, 256), (256, D)]
HBM = pl.BlockSpec(memory_space=pltpu.HBM)
SUMS = pltpu.VMEM((D, 256), F32)
PROJECT = [pltpu.VMEM((2, D, D), BF), pltpu.VMEM((256, D), BF)]


def held(some=slice(None)):
    return [pltpu.VMEM(s, BF) for s in SIZES[some]]


def call(kernel, us, inputs, in_specs, out_shape, out_specs, scratch):
    return pl.pallas_call(
        kernel,
        out_shape=out_shape,
        in_specs=[SM] + in_specs,
        out_specs=out_specs,
        scratch_shapes=scratch,
        compiler_params=PARAMS,
        cost_estimate=cost(us),
    )(*inputs)


def near0_call(sc, own, near, w_in):
    shapes = [pltpu.HBM(s, BF) for s in SIZES] + [pltpu.HBM((D, 256), F32)]
    scratch = held() + [SUMS] + PROJECT + [pltpu.SemaphoreType.DMA((6,))]
    return call(near0_kernel, 6, (sc, own, near, w_in), [VM] * 3, shapes, [HBM] * 6, scratch)


def near1_call(sc, own, near, w_in):
    return call(near1_kernel, 5, (sc, own, near, w_in), [VM] * 3, held() + [SUMS], [VM] * 6, PROJECT)


def past_call(sc, past, q, before):
    return call(past_kernel, 5, (sc, *past, q, before), [VM] * 6, SUMS, VM, [])


FAR = PROJECT + held(slice(2, 5)) + [SUMS, pltpu.VMEM((D, 256), BF)] + held(slice(0, 2)) + [SUMS]


def far0_call(sc, far, diag, w_in, w_out, sent):
    shapes = [pltpu.VMEM((512, D), BF)] + held(slice(0, 2)) * 2
    scratch = held(slice(2, 5)) + [SUMS] + FAR + [pltpu.SemaphoreType.DMA((6,))]
    inputs = (sc, far, diag, w_in, w_out, *sent)
    return call(far0_kernel, 9, inputs, [VM] * 4 + [HBM] * 6, shapes, [VM] * 5, scratch)


def far1_call(sc, past, far, diag, w_in, w_out, kept, first):
    inputs = (sc, *past, far, diag, w_in, w_out, *kept, first)
    shape = jax.ShapeDtypeStruct((1024, D), BF)
    return call(far1_kernel, 11, inputs, [VM] * 15, shape, VM, FAR + held(slice(0, 2)))


from jax.sharding import Mesh
from jax.sharding import PartitionSpec as P

CTX = ("xh", "xl", "yh", "co")
FLIP = [(0, 1), (1, 0)]


def layer(item_ids, lengths, table, w_in, w_out):
    owned = table.shape[0]
    me = lax.axis_index("dp")
    xh, xl, yh, co = (lax.axis_index(a) for a in CTX)
    owners = lax.axis_size("dp")
    w_in, w_out = in_vmem(w_in), in_vmem(w_out)
    groups = table.reshape(-1, 8, D)

    send = jnp.broadcast_to(item_ids[None, :, None], (owners, 4, 1, BLK)).reshape(owners * 4, 1, BLK)
    wanted = lax.all_to_all(send, ("dp", "xh", "yh"), 0, 0, tiled=True).reshape(owners, 4, BLK)
    mine = lax.dynamic_index_in_dim(wanted, me, 0, keepdims=False)
    user = 2 * xh + yh
    length = jnp.sum(jnp.where(lax.iota(jnp.int32, 4) == user, lengths, 0))
    upto = jnp.triu(jnp.ones((2 * BLK, 2 * BLK), BF))
    slots = lax.iota(jnp.int32, 8)
    sc = jnp.zeros((8,), jnp.int32)
    for i, value in enumerate((length, PART * (2 * xl + co), co, xl, 1 - xl)):
        sc = jnp.where(slots == i, value, sc)

    def ranks(member):
        return nn(member.astype(BF), upto).astype(jnp.int32) - 1

    def fetch(c):
        ids = wanted[:, 2 * c : 2 * c + 2].reshape(owners, 2 * BLK)
        local = ids - me * owned
        here = (local >= 0) & (local < owned)
        rank = jnp.where(here, ranks(here), -1)
        slot = lax.broadcasted_iota(jnp.int32, (owners, CAP, 2 * BLK), 1)
        rows = jnp.sum(jnp.where(rank[:, None, :] == slot, local[:, None, :], 0), axis=2)
        count = jnp.sum(here.astype(jnp.int32), axis=1)
        picked = gather_call(rows, count, groups, 1)[0].reshape(owners, CAP, D)
        return lax.all_to_all(picked, "dp", 0, 0, tiled=True).reshape(owners * CAP, D)

    def place(c, got):
        own_ids = mine[2 * c : 2 * c + 2].reshape(2 * BLK)
        owner = own_ids // owned
        member = owner[None, :] == lax.broadcasted_iota(jnp.int32, (owners, 2 * BLK), 0)
        at = jnp.sum(jnp.where(member, ranks(member), 0), axis=0) + owner * CAP
        pick = (at[:, None] == lax.broadcasted_iota(jnp.int32, (2 * BLK, owners * CAP), 1)).astype(BF)
        return nn(pick, got).astype(BF)

    def vmem_all(arrays):
        return [in_vmem(a) for a in arrays]

    for c in range(2):
        got = fetch(c)
        own = place(c, got)
        far = lax.ppermute(own, "xl", FLIP)
        near = lax.ppermute(own, "co", FLIP)
        diag = lax.ppermute(far, "co", FLIP)
        own, near, far, diag = vmem_all((own, near, far, diag))
        if c == 0:
            sent = near0_call(sc, own, near, w_in)
            sent = [pltpu.with_memory_space_constraint(a, pltpu.HBM) for a in sent]
            done = far0_call(sc, far, diag, w_in, w_out, sent)
            first, *past = vmem_all(done)
        else:
            kept = near1_call(sc, own, near, w_in)
            kept = vmem_all(kept)
            total = past_call(sc, past, kept[2], kept[5])
            kept[5] = in_vmem(total)
            out = far1_call(sc, past, far, diag, w_in, w_out, kept, first)
    back = lax.all_to_all(out.reshape(16, PART, D), ("xh", "yh", "xl", "co"), 0, 0, tiled=True)
    return pltpu.with_memory_space_constraint(back.reshape(4, BLK, D), pltpu.HBM)


def solution(mesh):
    finer = Mesh(mesh.devices.reshape(mesh.shape["dp"], 2, 2, 2, 2), ("dp",) + CTX)
    return jax.shard_map(
        layer,
        mesh=finer,
        in_specs=(P("dp", CTX), P("dp"), P("dp", None), P(), P()),
        out_specs=P("dp", CTX, None),
        check_vma=False,
    )
```

```python
import functools

import jax
import jax.numpy as jnp
from jax import lax
from jax.experimental import pallas as pl
from jax.experimental.pallas import tpu as pltpu

BF = jnp.bfloat16
F32 = jnp.float32
BLK = 256
D = 512
GRP = 1024
PART = 64
CAP = 128
ROW8 = 8
BUNCH = 32
VM = pl.BlockSpec(memory_space=pltpu.VMEM)
SM = pl.BlockSpec(memory_space=pltpu.SMEM)
HBM = pl.BlockSpec(memory_space=pltpu.HBM)
PARAMS = pltpu.CompilerParams(vmem_limit_bytes=16 * 1024 * 1024)


def cost(us):
    return pl.CostEstimate(flops=int(us * 4_000_000), bytes_accessed=0, transcendentals=0)


def in_vmem(x):
    return pltpu.with_memory_space_constraint(x, pltpu.VMEM)


def twice_silu(h):
    return h + h * jnp.tanh(h)


def tn(a, b):
    return lax.dot_general(a, b, (((0,), (1,)), ((), ())), preferred_element_type=F32)


def nn(a, b):
    return jnp.dot(a, b, preferred_element_type=F32)


def gather_kernel(owners, outs, rows_ref, count_ref, ids_ref, table_ref, *refs):
    out_refs, (buf, sems) = refs[:outs], refs[outs:]
    me = lax.axis_index("dp") if outs > 1 else 0

    def who(k):
        return jnp.bitwise_xor(me, k) if outs > 1 else k

    def eights(k):
        return (count_ref[who(k)] + ROW8 - 1) // ROW8

    for k in range(owners):
        o = who(k)

        def start(j, _, k=k, o=o):
            for i in range(ROW8):
                s = j * ROW8 + i
                pltpu.make_async_copy(
                    table_ref.at[lax.shift_right_logical(rows_ref[o, s], 3)], buf.at[k * CAP + s], sems.at[k]
                ).start()
            return 0

        def clear(j, _, k=k):
            buf[pl.ds(k * CAP + j * ROW8, ROW8)] = jnp.zeros((ROW8, 8, D), BF)
            return 0

        lax.fori_loop(0, eights(k), start, 0)
        full = BUNCH // ROW8
        lax.fori_loop(eights(k), (eights(k) + full - 1) // full * full, clear, 0)
    width = BUNCH * 8
    lane = lax.broadcasted_iota(jnp.int32, (BUNCH, width), 1).astype(F32)
    slot = lax.broadcasted_iota(jnp.int32, (BUNCH, 1), 0)
    for k in range(owners):
        eight = buf.at[pl.ds(k * CAP, ROW8)]

        def wait(j, _, k=k, eight=eight):
            pltpu.make_async_copy(eight, eight, sems.at[k]).wait()
            return 0

        lax.fori_loop(0, eights(k), wait, 0)
    low8 = (ids_ref[...] & 7).astype(F32).T
    for k in range(owners):
        o = who(k)
        if outs > 1:
            low = jnp.broadcast_to((ids_ref[pl.ds(o, 1), :] & 7).astype(F32), (8, CAP)).T[:, :1]
        else:
            low = low8[:, k : k + 1]
        for b in range(CAP // BUNCH):
            want = (8 * slot).astype(F32) + low[b * BUNCH : (b + 1) * BUNCH]
            pick = (lane == want).astype(F32).astype(BF)
            at = k * CAP + b * BUNCH
            got = nn(pick, buf[at : at + BUNCH].reshape(width, D))
            got = jnp.where(slot + b * BUNCH < count_ref[o], got, 0.0).astype(BF)
            if outs > 1:
                out_refs[k][b * BUNCH : (b + 1) * BUNCH, :] = got
            else:
                out_refs[0][at : at + BUNCH, :] = got


def gather_call(rows, count, groups, outs):
    owners = rows.shape[0]
    shape = jax.ShapeDtypeStruct((owners // outs * CAP, D), BF)
    return pl.pallas_call(
        functools.partial(gather_kernel, owners, outs),
        out_shape=[shape] * outs,
        in_specs=[SM, SM, VM, HBM],
        out_specs=[VM] * outs,
        scratch_shapes=[pltpu.VMEM((owners * CAP, 8, D), BF), pltpu.SemaphoreType.DMA((owners,))],
        compiler_params=pltpu.CompilerParams(vmem_limit_bytes=56 * 1024 * 1024),
        cost_estimate=cost(7),
    )(rows, count, rows, groups)


def place_kernel(at_ref, got_ref, own_ref, buf, sems):
    rows = own_ref.shape[0]
    parts = [pl.ds(2 * CAP * j, 2 * CAP) for j in range(4)]
    copies = [pltpu.make_async_copy(got_ref.at[p], buf.at[p], sems.at[j]) for j, p in enumerate(parts)]
    for c in copies:
        c.start()
    at = jnp.broadcast_to(at_ref[...].astype(F32), (8, rows)).T[:, :1]
    lane = lax.broadcasted_iota(jnp.int32, (rows, 2 * CAP), 1).astype(F32)
    own = None
    for j, c in enumerate(copies):
        pick = (lane + 2.0 * CAP * j == at).astype(F32).astype(BF)
        c.wait()
        part = nn(pick, buf[2 * CAP * j : 2 * CAP * (j + 1), :])
        own = part if own is None else own + part
    own_ref[...] = own.astype(BF)


def place_call(at, got):
    return pl.pallas_call(
        place_kernel,
        out_shape=pltpu.VMEM((at.shape[1], D), BF),
        in_specs=[VM, HBM],
        out_specs=VM,
        scratch_shapes=[pltpu.VMEM(got.shape, BF), pltpu.SemaphoreType.DMA((4,))],
        compiler_params=PARAMS,
        cost_estimate=cost(1.5),
        name="place",
    )(at, got)


def project(first, side, sc_ref, pieces, w_ref, k_ref, v_ref, q_ref, g_ref, x_ref, n_scr, nq_scr):
    co = sc_ref[2]
    base = first + GRP * sc_ref[3 + side]
    qo = pl.multiple_of(sc_ref[1], PART)
    wg, wv, wq, wk = (slice(D * i, D * (i + 1)) for i in range(4))
    for s, ref in enumerate(pieces):
        x = ref[...].astype(F32)
        c = x - jnp.mean(x, axis=1, keepdims=True)
        var = jnp.mean(c * c, axis=1, keepdims=True)
        n_scr[s] = (c * lax.rsqrt(var + 1e-5)).astype(BF)
    for s, ref in enumerate(pieces):
        edge = co if s == 0 else 1 - co
        n = n_scr[s]
        k = twice_silu(0.5 * nn(n, w_ref[:, wk])).astype(BF)
        v = twice_silu(0.5 * tn(w_ref[:, wv], n))
        for j in range(2):
            at = pl.multiple_of((edge + 2 * j) * BLK, BLK)
            k_ref[pl.ds(at, BLK), :] = k[j * BLK : (j + 1) * BLK]
            pos = base + at + lax.broadcasted_iota(jnp.int32, (1, BLK), 1)
            v_ref[:, pl.ds(at, BLK)] = jnp.where(pos < sc_ref[0], v[:, j * BLK : (j + 1) * BLK], 0.0).astype(BF)
            to = pl.multiple_of((edge + 2 * j) * PART, PART)
            nq_scr[pl.ds(to, PART), :] = n_scr[s, pl.ds(j * BLK + qo, PART), :]
            x_ref[pl.ds(to, PART), :] = ref[pl.ds(j * BLK + qo, PART), :]
    nq = nq_scr[...]
    q_ref[...] = twice_silu(0.5 * tn(w_ref[:, wq], nq)).astype(BF) * BF(1 / 16)
    g_ref[...] = twice_silu(0.5 * tn(w_ref[:, wg], nq)).astype(BF)


def attend(sc_ref, tiles, together):
    rid = lax.broadcasted_iota(jnp.int32, (128, 256), 0)
    col = lax.broadcasted_iota(jnp.int32, (1, 512), 1) & 255
    last_key = (col // PART) * BLK + (col % PART) + sc_ref[1]
    key = lax.broadcasted_iota(jnp.int32, (BLK, 512), 0)

    def heads(pp, _):
        steps = [
            (u, t, m, i)
            for u in range(together)
            for t in range(len(tiles))
            for m in range(len(tiles[t][2]))
            for i in range(GRP // BLK)
        ]
        queries = {}
        sums = {}

        def lanes(u):
            return pl.multiple_of((pp * together + u) * 128, 128)

        def scores(step):
            u, t, m, i = step
            if (u, t) not in queries:
                q = tiles[t][0][pl.ds(lanes(u), 128), :]
                zero = jnp.zeros_like(q)
                queries[u, t] = jnp.concatenate([jnp.where(rid < 64, q, zero), jnp.where(rid < 64, zero, q)], axis=1)
            return nn(tiles[t][2][m][0][i * BLK : (i + 1) * BLK, pl.ds(lanes(u), 128)], queries[u, t])

        def weights(step, s):
            _, t, m, i = step
            w = s + s * jnp.tanh(s)
            if tiles[t][2][m][2]:
                w = jnp.where(key + i * BLK <= last_key, w, 0.0)
            return w.astype(BF)

        def add_values(step, w):
            u, t, m, i = step
            o = [
                nn(
                    tiles[t][2][m][1][pl.ds(pl.multiple_of(lanes(u) + 64 * hh, 64), 64), i * BLK : (i + 1) * BLK],
                    w[:, 256 * hh : 256 * (hh + 1)],
                )
                for hh in range(2)
            ]
            old = sums.get((u, t))
            sums[u, t] = o if old is None else (old[0] + o[0], old[1] + o[1])

        s = scores(steps[0])
        before = None
        for n, step in enumerate(steps):
            ahead = scores(steps[n + 1]) if n + 1 < len(steps) else None
            w = weights(step, s)
            if before is not None:
                add_values(steps[n - 1], before)
            before, s = w, ahead
        add_values(steps[-1], before)
        for (u, t), pair in sums.items():
            for hh in range(2):
                tiles[t][1][pl.ds(pl.multiple_of(lanes(u) + 64 * hh, 64), 64), :] = pair[hh]
        return 0

    lax.fori_loop(0, 4 // together, heads, 0)


def near0_kernel(sc_ref, p1, p2, w_ref, *refs):
    outs, held, (n_scr, nq_scr, sems) = refs[:6], refs[6:12], refs[12:]
    k, v, q, g, x, o = held
    copies = [pltpu.make_async_copy(src, dst, sems.at[i]) for i, (src, dst) in enumerate(zip(held, outs))]
    project(0, 0, sc_ref, (p1, p2), w_ref, k, v, q, g, x, n_scr, nq_scr)
    for c in copies[:5]:
        c.start()
    attend(sc_ref, [(q, o, [(k, v, True)])], 2)
    copies[5].start()
    for c in copies:
        c.wait()


def near1_kernel(sc_ref, p1, p2, w_ref, k_ref, v_ref, q_ref, g_ref, x_ref, o_ref, n_scr, nq_scr):
    project(2 * GRP, 0, sc_ref, (p1, p2), w_ref, k_ref, v_ref, q_ref, g_ref, x_ref, n_scr, nq_scr)
    attend(sc_ref, [(q_ref, o_ref, [(k_ref, v_ref, True)])], 2)


def past_kernel(sc_ref, k0, v0, k1, v1, q_ref, before_ref, o_ref):
    attend(sc_ref, [(q_ref, o_ref, [(k0, v0, False), (k1, v1, False)])], 2)
    o_ref[...] = o_ref[...] + before_ref[...]


def finish(chunk, sc_ref, wo_ref, ox, sides, out_ref):
    for side, (o_ref, g_ref, x_ref) in enumerate(sides):
        o = o_ref[...] + jnp.where(sc_ref[3 + side] == 1, ox[...], 0.0)
        c = o - jnp.mean(o, axis=0, keepdims=True)
        var = jnp.mean(c * c, axis=0, keepdims=True)
        gated = ((c * lax.rsqrt(var + 1e-5)) * g_ref[...].astype(F32)).astype(BF)
        mixed = lax.dot_general(gated, wo_ref[...], (((0,), (0,)), ((), ())), preferred_element_type=F32)
        out = (x_ref[...].astype(F32) + mixed).astype(BF)
        for j in range(2):
            at = pl.multiple_of(512 * chunk + 256 * j + 128 * sc_ref[3 + side], 128)
            out_ref[pl.ds(at, 128), :] = out[128 * j : 128 * (j + 1)]


def far_core(chunk, sc_ref, past, p1, p2, w_ref, wo_ref, kept, arrive, out_ref, kf, vf, scratch):
    n_scr, nq_scr, qf, gf, xf, of, qx, kx, vx, ox = scratch
    kn, vn, qn, gn, xn, on = kept
    project(2 * GRP * chunk, 1, sc_ref, (p1, p2), w_ref, kf, vf, qf, gf, xf, n_scr, nq_scr)
    for c in arrive:
        c.wait()
    low = sc_ref[3] == 0

    @pl.when(low)
    def _():
        qx[...], kx[...], vx[...] = qf[...], kn[...], vn[...]

    @pl.when(jnp.logical_not(low))
    def _():
        qx[...], kx[...], vx[...] = qn[...], kf[...], vf[...]

    seen = [(past[2 * i], past[2 * i + 1], False) for i in range(2 * chunk)]
    attend(sc_ref, [(qf, of, seen + [(kf, vf, True)]), (qx, ox, [(kx, vx, False)])], 2)
    finish(chunk, sc_ref, wo_ref, ox, ((on, gn, xn), (of, gf, xf)), out_ref)


def far0_kernel(sc_ref, p1, p2, w_ref, wo_ref, *refs):
    sent, (out_ref, kn, vn, kf, vf), rest = refs[:6], refs[6:11], refs[11:]
    kept = (kn, vn, *rest[:4])
    sems = rest[-1]
    arrive = [pltpu.make_async_copy(src, dst, sems.at[i]) for i, (src, dst) in enumerate(zip(sent, kept))]
    for c in arrive:
        c.start()
    far_core(0, sc_ref, (), p1, p2, w_ref, wo_ref, kept, arrive, out_ref, kf, vf, rest[4:-1])


def far1_kernel(sc_ref, *refs):
    past, (p1, p2, w_ref, wo_ref), kept = refs[:4], refs[4:8], refs[8:14]
    first_ref, out_ref = refs[14:16]
    scratch, (kf, vf) = refs[16:26], refs[26:]
    far_core(1, sc_ref, past, p1, p2, w_ref, wo_ref, kept, (), out_ref, kf, vf, scratch)
    out_ref[:512, :] = first_ref[...]


SIZES = [(GRP, D), (D, GRP), (D, 256), (D, 256), (256, D)]
SUMS = pltpu.VMEM((D, 256), F32)
PROJECT = [pltpu.VMEM((2, D, D), BF), pltpu.VMEM((256, D), BF)]


def held(some=slice(None)):
    return [pltpu.VMEM(s, BF) for s in SIZES[some]]


def call(kernel, us, inputs, in_specs, out_shape, out_specs, scratch):
    return pl.pallas_call(
        kernel,
        out_shape=out_shape,
        in_specs=[SM] + in_specs,
        out_specs=out_specs,
        scratch_shapes=scratch,
        compiler_params=PARAMS,
        cost_estimate=cost(us),
    )(*inputs)


def near0_call(sc, own, near, w_in):
    shapes = [pltpu.HBM(s, BF) for s in SIZES] + [pltpu.HBM((D, 256), F32)]
    scratch = held() + [SUMS] + PROJECT + [pltpu.SemaphoreType.DMA((6,))]
    return call(near0_kernel, 6, (sc, own, near, w_in), [VM] * 3, shapes, [HBM] * 6, scratch)


def near1_call(sc, own, near, w_in):
    return call(near1_kernel, 5, (sc, own, near, w_in), [VM] * 3, held() + [SUMS], [VM] * 6, PROJECT)


def past_call(sc, past, q, before):
    return call(past_kernel, 5, (sc, *past, q, before), [VM] * 6, SUMS, VM, [])


FAR = PROJECT + held(slice(2, 5)) + [SUMS, pltpu.VMEM((D, 256), BF)] + held(slice(0, 2)) + [SUMS]


def far0_call(sc, far, diag, w_in, w_out, sent):
    shapes = [pltpu.VMEM((512, D), BF)] + held(slice(0, 2)) * 2
    scratch = held(slice(2, 5)) + [SUMS] + FAR + [pltpu.SemaphoreType.DMA((6,))]
    inputs = (sc, far, diag, w_in, w_out, *sent)
    return call(far0_kernel, 9, inputs, [VM] * 4 + [HBM] * 6, shapes, [VM] * 5, scratch)


def far1_call(sc, past, far, diag, w_in, w_out, kept, first):
    inputs = (sc, *past, far, diag, w_in, w_out, *kept, first)
    shape = jax.ShapeDtypeStruct((1024, D), BF)
    return call(far1_kernel, 11, inputs, [VM] * 15, shape, VM, FAR + held(slice(0, 2)))


from jax.sharding import Mesh
from jax.sharding import PartitionSpec as P

CTX = ("xh", "xl", "yh", "co")
FLIP = [(0, 1), (1, 0)]


def layer(item_ids, lengths, table, w_in, w_out):
    owned = table.shape[0]
    me = lax.axis_index("dp")
    xh, xl, yh, co = (lax.axis_index(a) for a in CTX)
    owners = lax.axis_size("dp")
    w_in, w_out = in_vmem(w_in), in_vmem(w_out)
    groups = table.reshape(-1, 8, D)

    send = jnp.broadcast_to(item_ids[None, :, None], (owners, 4, 1, BLK)).reshape(owners * 4, 1, BLK)
    wanted = lax.all_to_all(send, ("dp", "xh", "yh"), 0, 0, tiled=True).reshape(owners, 4, BLK)
    mine = lax.dynamic_index_in_dim(wanted, me, 0, keepdims=False)
    user = 2 * xh + yh
    length = jnp.sum(jnp.where(lax.iota(jnp.int32, 4) == user, lengths, 0))
    upto = jnp.triu(jnp.ones((2 * BLK, 2 * BLK), BF))
    slots = lax.iota(jnp.int32, 8)
    sc = jnp.zeros((8,), jnp.int32)
    for i, value in enumerate((length, PART * (2 * xl + co), co, xl, 1 - xl)):
        sc = jnp.where(slots == i, value, sc)

    def ranks(member):
        return nn(member.astype(BF), upto).astype(jnp.int32) - 1

    def fetch(c):
        ids = wanted[:, 2 * c : 2 * c + 2].reshape(owners, 2 * BLK)
        local = ids - me * owned
        here = (local >= 0) & (local < owned)
        rank = jnp.where(here, ranks(here), -1)
        slot = lax.broadcasted_iota(jnp.int32, (owners, CAP, 2 * BLK), 1)
        rows = jnp.sum(jnp.where(rank[:, None, :] == slot, local[:, None, :], 0), axis=2)
        count = jnp.sum(here.astype(jnp.int32), axis=1)
        picked = gather_call(rows, count, groups, 1)[0].reshape(owners, CAP, D)
        return lax.all_to_all(picked, "dp", 0, 0, tiled=True).reshape(owners * CAP, D)

    def place(c, got):
        own_ids = mine[2 * c : 2 * c + 2].reshape(2 * BLK)
        owner = own_ids // owned
        member = owner[None, :] == lax.broadcasted_iota(jnp.int32, (owners, 2 * BLK), 0)
        at = jnp.sum(jnp.where(member, ranks(member), 0), axis=0) + owner * CAP
        return place_call(at[None], pltpu.with_memory_space_constraint(got, pltpu.HBM))

    def vmem_all(arrays):
        return [in_vmem(a) for a in arrays]

    for c in range(2):
        got = fetch(c)
        own = place(c, got)
        far = lax.ppermute(own, "xl", FLIP)
        near = lax.ppermute(own, "co", FLIP)
        diag = lax.ppermute(far, "co", FLIP)
        own, near, far, diag = vmem_all((own, near, far, diag))
        if c == 0:
            sent = near0_call(sc, own, near, w_in)
            sent = [pltpu.with_memory_space_constraint(a, pltpu.HBM) for a in sent]
            done = far0_call(sc, far, diag, w_in, w_out, sent)
            first, *past = vmem_all(done)
        else:
            kept = near1_call(sc, own, near, w_in)
            kept = vmem_all(kept)
            total = past_call(sc, past, kept[2], kept[5])
            kept[5] = in_vmem(total)
            out = far1_call(sc, past, far, diag, w_in, w_out, kept, first)
    back = lax.all_to_all(out.reshape(16, PART, D), ("xh", "yh", "xl", "co"), 0, 0, tiled=True)
    return back.reshape(4, BLK, D)


def solution(mesh):
    finer = Mesh(mesh.devices.reshape(mesh.shape["dp"], 2, 2, 2, 2), ("dp",) + CTX)
    return jax.shard_map(
        layer,
        mesh=finer,
        in_specs=(P("dp", CTX), P("dp"), P("dp", None), P(), P()),
        out_specs=P("dp", CTX, None),
        check_vma=False,
    )
```

```python
import functools

import jax
import jax.numpy as jnp
from jax import lax
from jax.experimental import pallas as pl
from jax.experimental.pallas import tpu as pltpu

BF = jnp.bfloat16
F32 = jnp.float32
BLK = 256
D = 512
GRP = 1024
PART = 64
CAP = 128
ROW8 = 8
BUNCH = 32
VM = pl.BlockSpec(memory_space=pltpu.VMEM)
SM = pl.BlockSpec(memory_space=pltpu.SMEM)
HBM = pl.BlockSpec(memory_space=pltpu.HBM)
PARAMS = pltpu.CompilerParams(vmem_limit_bytes=16 * 1024 * 1024)


def cost(us):
    return pl.CostEstimate(flops=int(us * 4_000_000), bytes_accessed=0, transcendentals=0)


def in_vmem(x):
    return pltpu.with_memory_space_constraint(x, pltpu.VMEM)


def twice_silu(h):
    return h + h * jnp.tanh(h)


def tn(a, b):
    return lax.dot_general(a, b, (((0,), (1,)), ((), ())), preferred_element_type=F32)


def nn(a, b):
    return jnp.dot(a, b, preferred_element_type=F32)


def gather_kernel(owners, outs, rows_ref, count_ref, ids_ref, table_ref, *refs):
    out_refs, (buf, sems) = refs[:outs], refs[outs:]
    me = lax.axis_index("dp") if outs > 1 else 0

    def who(k):
        return jnp.bitwise_xor(me, k) if outs > 1 else k

    def eights(k):
        return (count_ref[who(k)] + ROW8 - 1) // ROW8

    for k in range(owners):
        o = who(k)

        def start(j, _, k=k, o=o):
            for i in range(ROW8):
                s = j * ROW8 + i
                pltpu.make_async_copy(
                    table_ref.at[lax.shift_right_logical(rows_ref[o, s], 3)], buf.at[k * CAP + s], sems.at[k]
                ).start()
            return 0

        def clear(j, _, k=k):
            buf[pl.ds(k * CAP + j * ROW8, ROW8)] = jnp.zeros((ROW8, 8, D), BF)
            return 0

        lax.fori_loop(0, eights(k), start, 0)
        full = BUNCH // ROW8
        lax.fori_loop(eights(k), (eights(k) + full - 1) // full * full, clear, 0)
    width = BUNCH * 8
    lane = lax.broadcasted_iota(jnp.int32, (BUNCH, width), 1).astype(F32)
    slot = lax.broadcasted_iota(jnp.int32, (BUNCH, 1), 0)
    for k in range(owners):
        eight = buf.at[pl.ds(k * CAP, ROW8)]

        def wait(j, _, k=k, eight=eight):
            pltpu.make_async_copy(eight, eight, sems.at[k]).wait()
            return 0

        lax.fori_loop(0, eights(k), wait, 0)
    low8 = (ids_ref[...] & 7).astype(F32).T
    for k in range(owners):
        o = who(k)
        if outs > 1:
            low = jnp.broadcast_to((ids_ref[pl.ds(o, 1), :] & 7).astype(F32), (8, CAP)).T[:, :1]
        else:
            low = low8[:, k : k + 1]
        for b in range(CAP // BUNCH):
            want = (8 * slot).astype(F32) + low[b * BUNCH : (b + 1) * BUNCH]
            pick = (lane == want).astype(F32).astype(BF)
            at = k * CAP + b * BUNCH
            got = nn(pick, buf[at : at + BUNCH].reshape(width, D))
            got = jnp.where(slot + b * BUNCH < count_ref[o], got, 0.0).astype(BF)
            if outs > 1:
                out_refs[k][b * BUNCH : (b + 1) * BUNCH, :] = got
            else:
                out_refs[0][at : at + BUNCH, :] = got


def gather_call(rows, count, groups, outs):
    owners = rows.shape[0]
    shape = jax.ShapeDtypeStruct((owners // outs * CAP, D), BF)
    return pl.pallas_call(
        functools.partial(gather_kernel, owners, outs),
        out_shape=[shape] * outs,
        in_specs=[SM, SM, VM, HBM],
        out_specs=[VM] * outs,
        scratch_shapes=[pltpu.VMEM((owners * CAP, 8, D), BF), pltpu.SemaphoreType.DMA((owners,))],
        compiler_params=pltpu.CompilerParams(vmem_limit_bytes=56 * 1024 * 1024),
        cost_estimate=cost(7),
    )(rows, count, rows, groups)


def place_kernel(at_ref, length_ref, got_ref, own_ref, kept_ref, buf, sems):
    kept_ref[...] = length_ref[...]
    rows = own_ref.shape[0]
    parts = [pl.ds(2 * CAP * j, 2 * CAP) for j in range(4)]
    copies = [pltpu.make_async_copy(got_ref.at[p], buf.at[p], sems.at[j]) for j, p in enumerate(parts)]
    for c in copies:
        c.start()
    at = jnp.broadcast_to(at_ref[...].astype(F32), (8, rows)).T[:, :1]
    lane = lax.broadcasted_iota(jnp.int32, (rows, 2 * CAP), 1).astype(F32)
    own = None
    for j, c in enumerate(copies):
        pick = (lane + 2.0 * CAP * j == at).astype(F32).astype(BF)
        c.wait()
        part = nn(pick, buf[2 * CAP * j : 2 * CAP * (j + 1), :])
        own = part if own is None else own + part
    own_ref[...] = own.astype(BF)


def place_call(at, length, got):
    return pl.pallas_call(
        place_kernel,
        out_shape=[pltpu.VMEM((at.shape[1], D), BF), pltpu.VMEM(length.shape, jnp.int32)],
        in_specs=[VM, VM, HBM],
        out_specs=[VM, VM],
        scratch_shapes=[pltpu.VMEM(got.shape, BF), pltpu.SemaphoreType.DMA((4,))],
        compiler_params=PARAMS,
        cost_estimate=cost(1.5),
        name="place",
    )(at, length, got)


def scalars(length_ref=None):
    xl, co = lax.axis_index("xl"), lax.axis_index("co")
    length = None if length_ref is None else length_ref[0:1, 0:1]
    return length, PART * (2 * xl + co), co, xl, 1 - xl


def project(first, side, sc_ref, pieces, w_ref, k_ref, v_ref, q_ref, g_ref, x_ref, n_scr, nq_scr):
    co = sc_ref[2]
    base = first + GRP * sc_ref[3 + side]
    qo = pl.multiple_of(sc_ref[1], PART)
    wg, wv, wq, wk = (slice(D * i, D * (i + 1)) for i in range(4))
    for s, ref in enumerate(pieces):
        x = ref[...].astype(F32)
        c = x - jnp.mean(x, axis=1, keepdims=True)
        var = jnp.mean(c * c, axis=1, keepdims=True)
        n_scr[s] = (c * lax.rsqrt(var + 1e-5)).astype(BF)
    for s, ref in enumerate(pieces):
        edge = co if s == 0 else 1 - co
        n = n_scr[s]
        k = twice_silu(0.5 * nn(n, w_ref[:, wk])).astype(BF)
        v = twice_silu(0.5 * tn(w_ref[:, wv], n))
        for j in range(2):
            at = pl.multiple_of((edge + 2 * j) * BLK, BLK)
            k_ref[pl.ds(at, BLK), :] = k[j * BLK : (j + 1) * BLK]
            pos = base + at + lax.broadcasted_iota(jnp.int32, (1, BLK), 1)
            v_ref[:, pl.ds(at, BLK)] = jnp.where(pos < sc_ref[0], v[:, j * BLK : (j + 1) * BLK], 0.0).astype(BF)
            to = pl.multiple_of((edge + 2 * j) * PART, PART)
            nq_scr[pl.ds(to, PART), :] = n_scr[s, pl.ds(j * BLK + qo, PART), :]
            x_ref[pl.ds(to, PART), :] = ref[pl.ds(j * BLK + qo, PART), :]
    nq = nq_scr[...]
    q_ref[...] = twice_silu(0.5 * tn(w_ref[:, wq], nq)).astype(BF) * BF(1 / 16)
    g_ref[...] = twice_silu(0.5 * tn(w_ref[:, wg], nq)).astype(BF)


def attend(sc_ref, tiles, together):
    rid = lax.broadcasted_iota(jnp.int32, (128, 256), 0)
    col = lax.broadcasted_iota(jnp.int32, (1, 512), 1) & 255
    last_key = (col // PART) * BLK + (col % PART) + sc_ref[1]
    key = lax.broadcasted_iota(jnp.int32, (BLK, 512), 0)

    def heads(pp, _):
        steps = [
            (u, t, m, i)
            for u in range(together)
            for t in range(len(tiles))
            for m in range(len(tiles[t][2]))
            for i in range(GRP // BLK)
        ]
        queries = {}
        sums = {}

        def lanes(u):
            return pl.multiple_of((pp * together + u) * 128, 128)

        def scores(step):
            u, t, m, i = step
            if (u, t) not in queries:
                q = tiles[t][0][pl.ds(lanes(u), 128), :]
                zero = jnp.zeros_like(q)
                queries[u, t] = jnp.concatenate([jnp.where(rid < 64, q, zero), jnp.where(rid < 64, zero, q)], axis=1)
            return nn(tiles[t][2][m][0][i * BLK : (i + 1) * BLK, pl.ds(lanes(u), 128)], queries[u, t])

        def weights(step, s):
            _, t, m, i = step
            w = s + s * jnp.tanh(s)
            if tiles[t][2][m][2]:
                w = jnp.where(key + i * BLK <= last_key, w, 0.0)
            return w.astype(BF)

        def add_values(step, w):
            u, t, m, i = step
            o = [
                nn(
                    tiles[t][2][m][1][pl.ds(pl.multiple_of(lanes(u) + 64 * hh, 64), 64), i * BLK : (i + 1) * BLK],
                    w[:, 256 * hh : 256 * (hh + 1)],
                )
                for hh in range(2)
            ]
            old = sums.get((u, t))
            sums[u, t] = o if old is None else (old[0] + o[0], old[1] + o[1])

        s = scores(steps[0])
        before = None
        for n, step in enumerate(steps):
            ahead = scores(steps[n + 1]) if n + 1 < len(steps) else None
            w = weights(step, s)
            if before is not None:
                add_values(steps[n - 1], before)
            before, s = w, ahead
        add_values(steps[-1], before)
        for (u, t), pair in sums.items():
            for hh in range(2):
                tiles[t][1][pl.ds(pl.multiple_of(lanes(u) + 64 * hh, 64), 64), :] = pair[hh]
        return 0

    lax.fori_loop(0, 4 // together, heads, 0)


def near0_kernel(length_ref, p1, p2, w_ref, *refs):
    sc_ref = scalars(length_ref)
    outs, held, (n_scr, nq_scr, sems) = refs[:6], refs[6:12], refs[12:]
    k, v, q, g, x, o = held
    copies = [pltpu.make_async_copy(src, dst, sems.at[i]) for i, (src, dst) in enumerate(zip(held, outs))]
    project(0, 0, sc_ref, (p1, p2), w_ref, k, v, q, g, x, n_scr, nq_scr)
    for c in copies[:5]:
        c.start()
    attend(sc_ref, [(q, o, [(k, v, True)])], 2)
    copies[5].start()
    for c in copies:
        c.wait()


def near1_kernel(length_ref, p1, p2, w_ref, k_ref, v_ref, q_ref, g_ref, x_ref, o_ref, n_scr, nq_scr):
    sc_ref = scalars(length_ref)
    project(2 * GRP, 0, sc_ref, (p1, p2), w_ref, k_ref, v_ref, q_ref, g_ref, x_ref, n_scr, nq_scr)
    attend(sc_ref, [(q_ref, o_ref, [(k_ref, v_ref, True)])], 2)


def past_kernel(k0, v0, k1, v1, q_ref, before_ref, o_ref):
    sc_ref = scalars()
    attend(sc_ref, [(q_ref, o_ref, [(k0, v0, False), (k1, v1, False)])], 2)
    o_ref[...] = o_ref[...] + before_ref[...]


def finish(chunk, sc_ref, wo_ref, ox, sides, out_ref):
    for side, (o_ref, g_ref, x_ref) in enumerate(sides):
        o = o_ref[...] + jnp.where(sc_ref[3 + side] == 1, ox[...], 0.0)
        c = o - jnp.mean(o, axis=0, keepdims=True)
        var = jnp.mean(c * c, axis=0, keepdims=True)
        gated = ((c * lax.rsqrt(var + 1e-5)) * g_ref[...].astype(F32)).astype(BF)
        mixed = lax.dot_general(gated, wo_ref[...], (((0,), (0,)), ((), ())), preferred_element_type=F32)
        out = (x_ref[...].astype(F32) + mixed).astype(BF)
        for j in range(2):
            at = pl.multiple_of(512 * chunk + 256 * j + 128 * sc_ref[3 + side], 128)
            out_ref[pl.ds(at, 128), :] = out[128 * j : 128 * (j + 1)]


def far_core(chunk, sc_ref, past, p1, p2, w_ref, wo_ref, kept, arrive, out_ref, kf, vf, scratch):
    n_scr, nq_scr, qf, gf, xf, of, qx, kx, vx, ox = scratch
    kn, vn, qn, gn, xn, on = kept
    project(2 * GRP * chunk, 1, sc_ref, (p1, p2), w_ref, kf, vf, qf, gf, xf, n_scr, nq_scr)
    for c in arrive:
        c.wait()
    low = sc_ref[3] == 0

    @pl.when(low)
    def _():
        qx[...], kx[...], vx[...] = qf[...], kn[...], vn[...]

    @pl.when(jnp.logical_not(low))
    def _():
        qx[...], kx[...], vx[...] = qn[...], kf[...], vf[...]

    seen = [(past[2 * i], past[2 * i + 1], False) for i in range(2 * chunk)]
    attend(sc_ref, [(qf, of, seen + [(kf, vf, True)]), (qx, ox, [(kx, vx, False)])], 2)
    finish(chunk, sc_ref, wo_ref, ox, ((on, gn, xn), (of, gf, xf)), out_ref)


def far0_kernel(length_ref, p1, p2, w_ref, wo_ref, *refs):
    sc_ref = scalars(length_ref)
    sent, (out_ref, kn, vn, kf, vf), rest = refs[:6], refs[6:11], refs[11:]
    kept = (kn, vn, *rest[:4])
    sems = rest[-1]
    arrive = [pltpu.make_async_copy(src, dst, sems.at[i]) for i, (src, dst) in enumerate(zip(sent, kept))]
    for c in arrive:
        c.start()
    far_core(0, sc_ref, (), p1, p2, w_ref, wo_ref, kept, arrive, out_ref, kf, vf, rest[4:-1])


def far1_kernel(length_ref, *refs):
    sc_ref = scalars(length_ref)
    past, (p1, p2, w_ref, wo_ref), kept = refs[:4], refs[4:8], refs[8:14]
    first_ref, out_ref = refs[14:16]
    scratch, (kf, vf) = refs[16:26], refs[26:]
    far_core(1, sc_ref, past, p1, p2, w_ref, wo_ref, kept, (), out_ref, kf, vf, scratch)
    out_ref[:512, :] = first_ref[...]


SIZES = [(GRP, D), (D, GRP), (D, 256), (D, 256), (256, D)]
SUMS = pltpu.VMEM((D, 256), F32)
PROJECT = [pltpu.VMEM((2, D, D), BF), pltpu.VMEM((256, D), BF)]


def held(some=slice(None)):
    return [pltpu.VMEM(s, BF) for s in SIZES[some]]


def call(kernel, us, inputs, in_specs, out_shape, out_specs, scratch):
    return pl.pallas_call(
        kernel,
        out_shape=out_shape,
        in_specs=in_specs,
        out_specs=out_specs,
        scratch_shapes=scratch,
        compiler_params=PARAMS,
        cost_estimate=cost(us),
    )(*inputs)


def near0_call(length, own, near, w_in):
    shapes = [pltpu.HBM(s, BF) for s in SIZES] + [pltpu.HBM((D, 256), F32)]
    scratch = held() + [SUMS] + PROJECT + [pltpu.SemaphoreType.DMA((6,))]
    return call(near0_kernel, 6, (length, own, near, w_in), [VM] * 4, shapes, [HBM] * 6, scratch)


def near1_call(length, own, near, w_in):
    return call(near1_kernel, 5, (length, own, near, w_in), [VM] * 4, held() + [SUMS], [VM] * 6, PROJECT)


def past_call(past, q, before):
    return call(past_kernel, 5, (*past, q, before), [VM] * 6, SUMS, VM, [])


FAR = PROJECT + held(slice(2, 5)) + [SUMS, pltpu.VMEM((D, 256), BF)] + held(slice(0, 2)) + [SUMS]


def far0_call(length, far, diag, w_in, w_out, sent):
    shapes = [pltpu.VMEM((512, D), BF)] + held(slice(0, 2)) * 2
    scratch = held(slice(2, 5)) + [SUMS] + FAR + [pltpu.SemaphoreType.DMA((6,))]
    inputs = (length, far, diag, w_in, w_out, *sent)
    return call(far0_kernel, 9, inputs, [VM] * 5 + [HBM] * 6, shapes, [VM] * 5, scratch)


def far1_call(length, past, far, diag, w_in, w_out, kept, first):
    inputs = (length, *past, far, diag, w_in, w_out, *kept, first)
    shape = jax.ShapeDtypeStruct((1024, D), BF)
    return call(far1_kernel, 11, inputs, [VM] * 16, shape, VM, FAR + held(slice(0, 2)))


from jax.sharding import Mesh
from jax.sharding import PartitionSpec as P

CTX = ("xh", "xl", "yh", "co")
FLIP = [(0, 1), (1, 0)]


def layer(item_ids, lengths, table, w_in, w_out):
    owned = table.shape[0]
    me = lax.axis_index("dp")
    xh, _, yh, _ = (lax.axis_index(a) for a in CTX)
    owners = lax.axis_size("dp")
    w_in, w_out = in_vmem(w_in), in_vmem(w_out)
    groups = table.reshape(-1, 8, D)

    send = jnp.broadcast_to(item_ids[None, :, None], (owners, 4, 1, BLK)).reshape(owners * 4, 1, BLK)
    wanted = lax.all_to_all(send, ("dp", "xh", "yh"), 0, 0, tiled=True).reshape(owners, 4, BLK)
    mine = lax.dynamic_index_in_dim(wanted, me, 0, keepdims=False)
    user = 2 * xh + yh
    length = jnp.sum(jnp.where(lax.iota(jnp.int32, 4) == user, lengths, 0))
    upto = jnp.triu(jnp.ones((2 * BLK, 2 * BLK), BF))
    length = jnp.broadcast_to(length, (8, 128))

    def ranks(member):
        return nn(member.astype(BF), upto).astype(jnp.int32) - 1

    def fetch(c):
        ids = wanted[:, 2 * c : 2 * c + 2].reshape(owners, 2 * BLK)
        local = ids - me * owned
        here = (local >= 0) & (local < owned)
        rank = jnp.where(here, ranks(here), -1)
        slot = lax.broadcasted_iota(jnp.int32, (owners, CAP, 2 * BLK), 1)
        rows = jnp.sum(jnp.where(rank[:, None, :] == slot, local[:, None, :], 0), axis=2)
        count = jnp.sum(here.astype(jnp.int32), axis=1)
        picked = gather_call(rows, count, groups, 1)[0].reshape(owners, CAP, D)
        return lax.all_to_all(picked, "dp", 0, 0, tiled=True).reshape(owners * CAP, D)

    def place(c, got):
        own_ids = mine[2 * c : 2 * c + 2].reshape(2 * BLK)
        owner = own_ids // owned
        member = owner[None, :] == lax.broadcasted_iota(jnp.int32, (owners, 2 * BLK), 0)
        at = jnp.sum(jnp.where(member, ranks(member), 0), axis=0) + owner * CAP
        return place_call(at[None], length, pltpu.with_memory_space_constraint(got, pltpu.HBM))

    def vmem_all(arrays):
        return [in_vmem(a) for a in arrays]

    for c in range(2):
        got = fetch(c)
        own, kept_length = place(c, got)
        far = lax.ppermute(own, "xl", FLIP)
        near = lax.ppermute(own, "co", FLIP)
        diag = lax.ppermute(far, "co", FLIP)
        own, near, far, diag, kept_length = vmem_all((own, near, far, diag, kept_length))
        if c == 0:
            sent = near0_call(kept_length, own, near, w_in)
            sent = [pltpu.with_memory_space_constraint(a, pltpu.HBM) for a in sent]
            far0, diag0 = far, diag
        else:
            done = far0_call(kept_length, far0, diag0, w_in, w_out, sent)
            first, *past = vmem_all(done)
            kept = near1_call(kept_length, own, near, w_in)
            kept = vmem_all(kept)
            total = past_call(past, kept[2], kept[5])
            kept[5] = in_vmem(total)
            out = far1_call(kept_length, past, far, diag, w_in, w_out, kept, first)
    back = lax.all_to_all(out.reshape(16, PART, D), ("xh", "yh", "xl", "co"), 0, 0, tiled=True)
    return back.reshape(4, BLK, D)


def solution(mesh):
    finer = Mesh(mesh.devices.reshape(mesh.shape["dp"], 2, 2, 2, 2), ("dp",) + CTX)
    return jax.shard_map(
        layer,
        mesh=finer,
        in_specs=(P("dp", CTX), P("dp"), P("dp", None), P(), P()),
        out_specs=P("dp", CTX, None),
        check_vma=False,
    )
```

```python
import functools

import jax
import jax.numpy as jnp
from jax import lax
from jax.experimental import pallas as pl
from jax.experimental.pallas import tpu as pltpu

BF = jnp.bfloat16
F32 = jnp.float32
BLK = 256
D = 512
GRP = 1024
PART = 64
CAP = 128
ROW8 = 8
BUNCH = 32
VM = pl.BlockSpec(memory_space=pltpu.VMEM)
SM = pl.BlockSpec(memory_space=pltpu.SMEM)
HBM = pl.BlockSpec(memory_space=pltpu.HBM)
PARAMS = pltpu.CompilerParams(vmem_limit_bytes=16 * 1024 * 1024)


def cost(us):
    return pl.CostEstimate(flops=int(us * 4_000_000), bytes_accessed=0, transcendentals=0)


def in_vmem(x):
    return pltpu.with_memory_space_constraint(x, pltpu.VMEM)


def twice_silu(h):
    return h + h * jnp.tanh(h)


def tn(a, b):
    return lax.dot_general(a, b, (((0,), (1,)), ((), ())), preferred_element_type=F32)


def nn(a, b):
    return jnp.dot(a, b, preferred_element_type=F32)


def gather_kernel(owners, outs, rows_ref, count_ref, ids_ref, table_ref, *refs):
    out_refs, (buf, sems) = refs[:outs], refs[outs:]
    me = lax.axis_index("dp") if outs > 1 else 0

    def who(k):
        return jnp.bitwise_xor(me, k) if outs > 1 else k

    def eights(k):
        return (count_ref[who(k)] + ROW8 - 1) // ROW8

    for k in range(owners):
        o = who(k)

        def start(j, _, k=k, o=o):
            for i in range(ROW8):
                s = j * ROW8 + i
                pltpu.make_async_copy(
                    table_ref.at[lax.shift_right_logical(rows_ref[o, s], 3)], buf.at[k * CAP + s], sems.at[k]
                ).start()
            return 0

        def clear(j, _, k=k):
            buf[pl.ds(k * CAP + j * ROW8, ROW8)] = jnp.zeros((ROW8, 8, D), BF)
            return 0

        lax.fori_loop(0, eights(k), start, 0)
        full = BUNCH // ROW8
        lax.fori_loop(eights(k), (eights(k) + full - 1) // full * full, clear, 0)
    width = BUNCH * 8
    lane = lax.broadcasted_iota(jnp.int32, (BUNCH, width), 1).astype(F32)
    slot = lax.broadcasted_iota(jnp.int32, (BUNCH, 1), 0)
    for k in range(owners):
        eight = buf.at[pl.ds(k * CAP, ROW8)]

        def wait(j, _, k=k, eight=eight):
            pltpu.make_async_copy(eight, eight, sems.at[k]).wait()
            return 0

        lax.fori_loop(0, eights(k), wait, 0)
    low8 = (ids_ref[...] & 7).astype(F32).T
    for k in range(owners):
        o = who(k)
        if outs > 1:
            low = jnp.broadcast_to((ids_ref[pl.ds(o, 1), :] & 7).astype(F32), (8, CAP)).T[:, :1]
        else:
            low = low8[:, k : k + 1]
        for b in range(CAP // BUNCH):
            want = (8 * slot).astype(F32) + low[b * BUNCH : (b + 1) * BUNCH]
            pick = (lane == want).astype(F32).astype(BF)
            at = k * CAP + b * BUNCH
            got = nn(pick, buf[at : at + BUNCH].reshape(width, D))
            got = jnp.where(slot + b * BUNCH < count_ref[o], got, 0.0).astype(BF)
            if outs > 1:
                out_refs[k][b * BUNCH : (b + 1) * BUNCH, :] = got
            else:
                out_refs[0][at : at + BUNCH, :] = got


def gather_call(rows, count, groups, outs):
    owners = rows.shape[0]
    shape = jax.ShapeDtypeStruct((owners // outs * CAP, D), BF)
    return pl.pallas_call(
        functools.partial(gather_kernel, owners, outs),
        out_shape=[shape] * outs,
        in_specs=[SM, SM, VM, HBM],
        out_specs=[VM] * outs,
        scratch_shapes=[pltpu.VMEM((owners * CAP, 8, D), BF), pltpu.SemaphoreType.DMA((owners,))],
        compiler_params=pltpu.CompilerParams(vmem_limit_bytes=56 * 1024 * 1024),
        cost_estimate=cost(7),
    )(rows, count, rows, groups)


def place_kernel(at_ref, length_ref, got_ref, own_ref, kept_ref):
    kept_ref[...] = length_ref[...]
    rows = own_ref.shape[0]
    at = jnp.broadcast_to(at_ref[...].astype(F32), (8, rows)).T[:, :1]
    lane = lax.broadcasted_iota(jnp.int32, (rows, got_ref.shape[0]), 1).astype(F32)
    own_ref[...] = nn((lane == at).astype(F32).astype(BF), got_ref[...]).astype(BF)


def place_call(at, length, got):
    return pl.pallas_call(
        place_kernel,
        out_shape=[pltpu.VMEM((at.shape[1], D), BF), pltpu.VMEM(length.shape, jnp.int32)],
        in_specs=[VM] * 3,
        out_specs=[VM, VM],
        compiler_params=PARAMS,
        cost_estimate=cost(1.5),
        name="place",
    )(at, length, got)


def scalars(length_ref=None):
    xl, co = lax.axis_index("xl"), lax.axis_index("co")
    length = None if length_ref is None else length_ref[0:1, 0:1]
    return length, PART * (2 * xl + co), co, xl, 1 - xl


def project(first, side, sc_ref, pieces, w_ref, k_ref, v_ref, q_ref, g_ref, x_ref, n_scr, nq_scr):
    co = sc_ref[2]
    base = first + GRP * sc_ref[3 + side]
    qo = pl.multiple_of(sc_ref[1], PART)
    wg, wv, wq, wk = (slice(D * i, D * (i + 1)) for i in range(4))
    for s, ref in enumerate(pieces):
        x = ref[...].astype(F32)
        c = x - jnp.mean(x, axis=1, keepdims=True)
        var = jnp.mean(c * c, axis=1, keepdims=True)
        n_scr[s] = (c * lax.rsqrt(var + 1e-5)).astype(BF)
    for s, ref in enumerate(pieces):
        edge = co if s == 0 else 1 - co
        n = n_scr[s]
        k = twice_silu(0.5 * nn(n, w_ref[:, wk])).astype(BF)
        v = twice_silu(0.5 * tn(w_ref[:, wv], n))
        for j in range(2):
            at = pl.multiple_of((edge + 2 * j) * BLK, BLK)
            k_ref[pl.ds(at, BLK), :] = k[j * BLK : (j + 1) * BLK]
            pos = base + at + lax.broadcasted_iota(jnp.int32, (1, BLK), 1)
            v_ref[:, pl.ds(at, BLK)] = jnp.where(pos < sc_ref[0], v[:, j * BLK : (j + 1) * BLK], 0.0).astype(BF)
            to = pl.multiple_of((edge + 2 * j) * PART, PART)
            nq_scr[pl.ds(to, PART), :] = n_scr[s, pl.ds(j * BLK + qo, PART), :]
            x_ref[pl.ds(to, PART), :] = ref[pl.ds(j * BLK + qo, PART), :]
    nq = nq_scr[...]
    q_ref[...] = twice_silu(0.5 * tn(w_ref[:, wq], nq)).astype(BF) * BF(1 / 16)
    g_ref[...] = twice_silu(0.5 * tn(w_ref[:, wg], nq)).astype(BF)


def attend(sc_ref, tiles, together):
    rid = lax.broadcasted_iota(jnp.int32, (128, 256), 0)
    col = lax.broadcasted_iota(jnp.int32, (1, 512), 1) & 255
    last_key = (col // PART) * BLK + (col % PART) + sc_ref[1]
    key = lax.broadcasted_iota(jnp.int32, (BLK, 512), 0)

    def heads(pp, _):
        steps = [
            (u, t, m, i)
            for u in range(together)
            for t in range(len(tiles))
            for m in range(len(tiles[t][2]))
            for i in range(GRP // BLK)
        ]
        queries = {}
        sums = {}

        def lanes(u):
            return pl.multiple_of((pp * together + u) * 128, 128)

        def scores(step):
            u, t, m, i = step
            if (u, t) not in queries:
                q = tiles[t][0][pl.ds(lanes(u), 128), :]
                zero = jnp.zeros_like(q)
                queries[u, t] = jnp.concatenate([jnp.where(rid < 64, q, zero), jnp.where(rid < 64, zero, q)], axis=1)
            return nn(tiles[t][2][m][0][i * BLK : (i + 1) * BLK, pl.ds(lanes(u), 128)], queries[u, t])

        def weights(step, s):
            _, t, m, i = step
            w = s + s * jnp.tanh(s)
            if tiles[t][2][m][2]:
                w = jnp.where(key + i * BLK <= last_key, w, 0.0)
            return w.astype(BF)

        def add_values(step, w):
            u, t, m, i = step
            o = [
                nn(
                    tiles[t][2][m][1][pl.ds(pl.multiple_of(lanes(u) + 64 * hh, 64), 64), i * BLK : (i + 1) * BLK],
                    w[:, 256 * hh : 256 * (hh + 1)],
                )
                for hh in range(2)
            ]
            old = sums.get((u, t))
            sums[u, t] = o if old is None else (old[0] + o[0], old[1] + o[1])

        s = scores(steps[0])
        before = None
        for n, step in enumerate(steps):
            ahead = scores(steps[n + 1]) if n + 1 < len(steps) else None
            w = weights(step, s)
            if before is not None:
                add_values(steps[n - 1], before)
            before, s = w, ahead
        add_values(steps[-1], before)
        for (u, t), pair in sums.items():
            for hh in range(2):
                tiles[t][1][pl.ds(pl.multiple_of(lanes(u) + 64 * hh, 64), 64), :] = pair[hh]
        return 0

    lax.fori_loop(0, 4 // together, heads, 0)


def near0_kernel(length_ref, p1, p2, w_ref, *refs):
    sc_ref = scalars(length_ref)
    outs, held, (n_scr, nq_scr, sems) = refs[:6], refs[6:12], refs[12:]
    k, v, q, g, x, o = held
    copies = [pltpu.make_async_copy(src, dst, sems.at[i]) for i, (src, dst) in enumerate(zip(held, outs))]
    project(0, 0, sc_ref, (p1, p2), w_ref, k, v, q, g, x, n_scr, nq_scr)
    for c in copies[:5]:
        c.start()
    attend(sc_ref, [(q, o, [(k, v, True)])], 2)
    copies[5].start()
    for c in copies:
        c.wait()


def near1_kernel(length_ref, p1, p2, w_ref, k_ref, v_ref, q_ref, g_ref, x_ref, o_ref, n_scr, nq_scr):
    sc_ref = scalars(length_ref)
    project(2 * GRP, 0, sc_ref, (p1, p2), w_ref, k_ref, v_ref, q_ref, g_ref, x_ref, n_scr, nq_scr)
    attend(sc_ref, [(q_ref, o_ref, [(k_ref, v_ref, True)])], 2)


def past_kernel(k0, v0, k1, v1, q_ref, before_ref, o_ref):
    sc_ref = scalars()
    attend(sc_ref, [(q_ref, o_ref, [(k0, v0, False), (k1, v1, False)])], 2)
    o_ref[...] = o_ref[...] + before_ref[...]


def finish(chunk, sc_ref, wo_ref, ox, sides, out_ref):
    for side, (o_ref, g_ref, x_ref) in enumerate(sides):
        o = o_ref[...] + jnp.where(sc_ref[3 + side] == 1, ox[...], 0.0)
        c = o - jnp.mean(o, axis=0, keepdims=True)
        var = jnp.mean(c * c, axis=0, keepdims=True)
        gated = ((c * lax.rsqrt(var + 1e-5)) * g_ref[...].astype(F32)).astype(BF)
        mixed = lax.dot_general(gated, wo_ref[...], (((0,), (0,)), ((), ())), preferred_element_type=F32)
        out = (x_ref[...].astype(F32) + mixed).astype(BF)
        for j in range(2):
            at = pl.multiple_of(512 * chunk + 256 * j + 128 * sc_ref[3 + side], 128)
            out_ref[pl.ds(at, 128), :] = out[128 * j : 128 * (j + 1)]


def far_core(chunk, sc_ref, past, p1, p2, w_ref, wo_ref, kept, arrive, out_ref, kf, vf, scratch):
    n_scr, nq_scr, qf, gf, xf, of, qx, kx, vx, ox = scratch
    kn, vn, qn, gn, xn, on = kept
    project(2 * GRP * chunk, 1, sc_ref, (p1, p2), w_ref, kf, vf, qf, gf, xf, n_scr, nq_scr)
    for c in arrive:
        c.wait()
    low = sc_ref[3] == 0

    @pl.when(low)
    def _():
        qx[...], kx[...], vx[...] = qf[...], kn[...], vn[...]

    @pl.when(jnp.logical_not(low))
    def _():
        qx[...], kx[...], vx[...] = qn[...], kf[...], vf[...]

    seen = [(past[2 * i], past[2 * i + 1], False) for i in range(2 * chunk)]
    attend(sc_ref, [(qf, of, seen + [(kf, vf, True)]), (qx, ox, [(kx, vx, False)])], 2)
    finish(chunk, sc_ref, wo_ref, ox, ((on, gn, xn), (of, gf, xf)), out_ref)


def far0_kernel(length_ref, p1, p2, w_ref, wo_ref, *refs):
    sc_ref = scalars(length_ref)
    sent, (out_ref, kn, vn, kf, vf), rest = refs[:6], refs[6:11], refs[11:]
    kept = (kn, vn, *rest[:4])
    sems = rest[-1]
    arrive = [pltpu.make_async_copy(src, dst, sems.at[i]) for i, (src, dst) in enumerate(zip(sent, kept))]
    for c in arrive:
        c.start()
    far_core(0, sc_ref, (), p1, p2, w_ref, wo_ref, kept, arrive, out_ref, kf, vf, rest[4:-1])


def far1_kernel(length_ref, *refs):
    sc_ref = scalars(length_ref)
    past, (p1, p2, w_ref, wo_ref), kept = refs[:4], refs[4:8], refs[8:14]
    first_ref, out_ref = refs[14:16]
    scratch, (kf, vf) = refs[16:26], refs[26:]
    far_core(1, sc_ref, past, p1, p2, w_ref, wo_ref, kept, (), out_ref, kf, vf, scratch)
    out_ref[:512, :] = first_ref[...]


SIZES = [(GRP, D), (D, GRP), (D, 256), (D, 256), (256, D)]
SUMS = pltpu.VMEM((D, 256), F32)
PROJECT = [pltpu.VMEM((2, D, D), BF), pltpu.VMEM((256, D), BF)]


def held(some=slice(None)):
    return [pltpu.VMEM(s, BF) for s in SIZES[some]]


def call(kernel, us, inputs, in_specs, out_shape, out_specs, scratch):
    return pl.pallas_call(
        kernel,
        out_shape=out_shape,
        in_specs=in_specs,
        out_specs=out_specs,
        scratch_shapes=scratch,
        compiler_params=PARAMS,
        cost_estimate=cost(us),
    )(*inputs)


def near0_call(length, own, near, w_in):
    shapes = [pltpu.HBM(s, BF) for s in SIZES] + [pltpu.HBM((D, 256), F32)]
    scratch = held() + [SUMS] + PROJECT + [pltpu.SemaphoreType.DMA((6,))]
    return call(near0_kernel, 6, (length, own, near, w_in), [VM] * 4, shapes, [HBM] * 6, scratch)


def near1_call(length, own, near, w_in):
    return call(near1_kernel, 5, (length, own, near, w_in), [VM] * 4, held() + [SUMS], [VM] * 6, PROJECT)


def past_call(past, q, before):
    return call(past_kernel, 5, (*past, q, before), [VM] * 6, SUMS, VM, [])


FAR = PROJECT + held(slice(2, 5)) + [SUMS, pltpu.VMEM((D, 256), BF)] + held(slice(0, 2)) + [SUMS]


def far0_call(length, far, diag, w_in, w_out, sent):
    shapes = [pltpu.VMEM((512, D), BF)] + held(slice(0, 2)) * 2
    scratch = held(slice(2, 5)) + [SUMS] + FAR + [pltpu.SemaphoreType.DMA((6,))]
    inputs = (length, far, diag, w_in, w_out, *sent)
    return call(far0_kernel, 9, inputs, [VM] * 5 + [HBM] * 6, shapes, [VM] * 5, scratch)


def far1_call(length, past, far, diag, w_in, w_out, kept, first):
    inputs = (length, *past, far, diag, w_in, w_out, *kept, first)
    shape = jax.ShapeDtypeStruct((1024, D), BF)
    return call(far1_kernel, 11, inputs, [VM] * 16, shape, VM, FAR + held(slice(0, 2)))


from jax.sharding import Mesh
from jax.sharding import PartitionSpec as P

CTX = ("xh", "xl", "yh", "co")
FLIP = [(0, 1), (1, 0)]


def layer(item_ids, lengths, table, w_in, w_out):
    owned = table.shape[0]
    me = lax.axis_index("dp")
    xh, _, yh, _ = (lax.axis_index(a) for a in CTX)
    owners = lax.axis_size("dp")
    w_in, w_out = in_vmem(w_in), in_vmem(w_out)
    groups = table.reshape(-1, 8, D)

    send = jnp.broadcast_to(item_ids[None, :, None], (owners, 4, 1, BLK)).reshape(owners * 4, 1, BLK)
    wanted = lax.all_to_all(send, ("dp", "xh", "yh"), 0, 0, tiled=True)
    wanted = wanted.reshape(owners, 4, BLK)
    mine = lax.dynamic_index_in_dim(wanted, me, 0, keepdims=False)
    upto = jnp.triu(jnp.ones((2 * BLK, 2 * BLK), BF))
    users = lax.broadcasted_iota(jnp.int32, (4, 8, 128), 0)
    length = jnp.sum(jnp.where(users == 2 * xh + yh, lengths[:, None, None], 0), axis=0)

    def ranks(member):
        return nn(member.astype(BF), upto).astype(jnp.int32) - 1

    def fetch(c):
        ids = wanted[:, 2 * c : 2 * c + 2].reshape(owners, 2 * BLK)
        local = ids - me * owned
        here = (local >= 0) & (local < owned)
        rank = jnp.where(here, ranks(here), -1)
        slot = lax.broadcasted_iota(jnp.int32, (owners, CAP, 2 * BLK), 1)
        rows = jnp.sum(jnp.where(rank[:, None, :] == slot, local[:, None, :], 0), axis=2)
        count = jnp.sum(here.astype(jnp.int32), axis=1)
        picked = gather_call(rows, count, groups, 1)[0].reshape(owners, CAP, D)
        return lax.all_to_all(picked, "dp", 0, 0, tiled=True).reshape(owners * CAP, D)

    def place(c, got):
        own_ids = mine[2 * c : 2 * c + 2].reshape(2 * BLK)
        owner = own_ids // owned
        member = owner[None, :] == lax.broadcasted_iota(jnp.int32, (owners, 2 * BLK), 0)
        at = jnp.sum(jnp.where(member, ranks(member), 0), axis=0) + owner * CAP
        return place_call(at[None], length, in_vmem(got))

    def vmem_all(arrays):
        return [in_vmem(a) for a in arrays]

    for c in range(2):
        got = fetch(c)
        own, kept_length = place(c, got)
        far = lax.ppermute(own, "xl", FLIP)
        near = lax.ppermute(own, "co", FLIP)
        diag = lax.ppermute(far, "co", FLIP)
        own, near, far, diag, kept_length = vmem_all((own, near, far, diag, kept_length))
        if c == 0:
            sent = near0_call(kept_length, own, near, w_in)
            sent = [pltpu.with_memory_space_constraint(a, pltpu.HBM) for a in sent]
            far0, diag0 = far, diag
        else:
            done = far0_call(kept_length, far0, diag0, w_in, w_out, sent)
            first, *past = vmem_all(done)
            kept = near1_call(kept_length, own, near, w_in)
            kept = vmem_all(kept)
            total = past_call(past, kept[2], kept[5])
            kept[5] = in_vmem(total)
            out = far1_call(kept_length, past, far, diag, w_in, w_out, kept, first)
    back = lax.all_to_all(out.reshape(16, PART, D), ("xh", "yh", "xl", "co"), 0, 0, tiled=True)
    return back.reshape(4, BLK, D)


def solution(mesh):
    finer = Mesh(mesh.devices.reshape(mesh.shape["dp"], 2, 2, 2, 2), ("dp",) + CTX)
    return jax.shard_map(
        layer,
        mesh=finer,
        in_specs=(P("dp", CTX), P("dp"), P("dp", None), P(), P()),
        out_specs=P("dp", CTX, None),
        check_vma=False,
    )
```

```python
import functools

import jax
import jax.numpy as jnp
from jax import lax
from jax.experimental import pallas as pl
from jax.experimental.pallas import tpu as pltpu

BF = jnp.bfloat16
F32 = jnp.float32
BLK = 256
D = 512
GRP = 1024
PART = 64
CAP = 128
ROW8 = 8
BUNCH = 32
VM = pl.BlockSpec(memory_space=pltpu.VMEM)
SM = pl.BlockSpec(memory_space=pltpu.SMEM)
HBM = pl.BlockSpec(memory_space=pltpu.HBM)
PARAMS = pltpu.CompilerParams(vmem_limit_bytes=16 * 1024 * 1024)


def cost(us):
    return pl.CostEstimate(flops=int(us * 4_000_000), bytes_accessed=0, transcendentals=0)


def in_vmem(x):
    return pltpu.with_memory_space_constraint(x, pltpu.VMEM)


def twice_silu(h):
    return h + h * jnp.tanh(h)


def tn(a, b):
    return lax.dot_general(a, b, (((0,), (1,)), ((), ())), preferred_element_type=F32)


def nn(a, b):
    return jnp.dot(a, b, preferred_element_type=F32)


def gather_kernel(owners, outs, rows_ref, count_ref, ids_ref, table_ref, *refs):
    out_refs, (buf, sems) = refs[:outs], refs[outs:]
    me = lax.axis_index("dp") if outs > 1 else 0

    def who(k):
        return jnp.bitwise_xor(me, k) if outs > 1 else k

    def eights(k):
        return (count_ref[who(k)] + ROW8 - 1) // ROW8

    for k in range(owners):
        o = who(k)

        def start(j, _, k=k, o=o):
            for i in range(ROW8):
                s = j * ROW8 + i
                pltpu.make_async_copy(
                    table_ref.at[lax.shift_right_logical(rows_ref[o, s], 3)], buf.at[k * CAP + s], sems.at[k]
                ).start()
            return 0

        def clear(j, _, k=k):
            buf[pl.ds(k * CAP + j * ROW8, ROW8)] = jnp.zeros((ROW8, 8, D), BF)
            return 0

        lax.fori_loop(0, eights(k), start, 0)
        full = BUNCH // ROW8
        lax.fori_loop(eights(k), (eights(k) + full - 1) // full * full, clear, 0)
    width = BUNCH * 8
    lane = lax.broadcasted_iota(jnp.int32, (BUNCH, width), 1).astype(F32)
    slot = lax.broadcasted_iota(jnp.int32, (BUNCH, 1), 0)
    for k in range(owners):
        eight = buf.at[pl.ds(k * CAP, ROW8)]

        def wait(j, _, k=k, eight=eight):
            pltpu.make_async_copy(eight, eight, sems.at[k]).wait()
            return 0

        lax.fori_loop(0, eights(k), wait, 0)
    low8 = (ids_ref[...] & 7).astype(F32).T
    for k in range(owners):
        o = who(k)
        if outs > 1:
            low = jnp.broadcast_to((ids_ref[pl.ds(o, 1), :] & 7).astype(F32), (8, CAP)).T[:, :1]
        else:
            low = low8[:, k : k + 1]
        for b in range(CAP // BUNCH):
            want = (8 * slot).astype(F32) + low[b * BUNCH : (b + 1) * BUNCH]
            pick = (lane == want).astype(F32).astype(BF)
            at = k * CAP + b * BUNCH
            got = nn(pick, buf[at : at + BUNCH].reshape(width, D))
            got = jnp.where(slot + b * BUNCH < count_ref[o], got, 0.0).astype(BF)
            if outs > 1:
                out_refs[k][b * BUNCH : (b + 1) * BUNCH, :] = got
            else:
                out_refs[0][at : at + BUNCH, :] = got


def gather_call(rows, count, groups, outs):
    owners = rows.shape[0]
    shape = jax.ShapeDtypeStruct((owners // outs * CAP, D), BF)
    return pl.pallas_call(
        functools.partial(gather_kernel, owners, outs),
        out_shape=[shape] * outs,
        in_specs=[SM, SM, VM, HBM],
        out_specs=[VM] * outs,
        scratch_shapes=[pltpu.VMEM((owners * CAP, 8, D), BF), pltpu.SemaphoreType.DMA((owners,))],
        compiler_params=pltpu.CompilerParams(vmem_limit_bytes=56 * 1024 * 1024),
        cost_estimate=cost(7),
    )(rows, count, rows, groups)


def place_kernel(at_ref, length_ref, got_ref, own_ref, kept_ref):
    kept_ref[...] = length_ref[...]
    rows = own_ref.shape[0]
    at = jnp.broadcast_to(at_ref[...].astype(F32), (8, rows)).T[:, :1]
    lane = lax.broadcasted_iota(jnp.int32, (rows, got_ref.shape[0]), 1).astype(F32)
    own_ref[...] = nn((lane == at).astype(F32).astype(BF), got_ref[...]).astype(BF)


def place_call(at, length, got):
    return pl.pallas_call(
        place_kernel,
        out_shape=[pltpu.VMEM((at.shape[1], D), BF), pltpu.VMEM(length.shape, jnp.int32)],
        in_specs=[VM] * 3,
        out_specs=[VM, VM],
        compiler_params=PARAMS,
        cost_estimate=cost(1.5),
        name="place",
    )(at, length, got)


def scalars(length_ref=None):
    xl, co = lax.axis_index("xl"), lax.axis_index("co")
    length = None if length_ref is None else length_ref[0:1, 0:1]
    return length, PART * (2 * xl + co), co, xl, 1 - xl


def project(first, side, sc_ref, pieces, w_ref, k_ref, v_ref, q_ref, g_ref, x_ref, n_scr, nq_scr):
    co = sc_ref[2]
    base = first + GRP * sc_ref[3 + side]
    qo = pl.multiple_of(sc_ref[1], PART)
    wg, wv, wq, wk = (slice(D * i, D * (i + 1)) for i in range(4))
    for s, ref in enumerate(pieces):
        x = ref[...].astype(F32)
        c = x - jnp.mean(x, axis=1, keepdims=True)
        var = jnp.mean(c * c, axis=1, keepdims=True)
        n_scr[s] = (c * lax.rsqrt(var + 1e-5)).astype(BF)
    for s, ref in enumerate(pieces):
        edge = co if s == 0 else 1 - co
        n = n_scr[s]
        k = twice_silu(0.5 * nn(n, w_ref[:, wk])).astype(BF)
        v = twice_silu(0.5 * tn(w_ref[:, wv], n))
        for j in range(2):
            at = pl.multiple_of((edge + 2 * j) * BLK, BLK)
            k_ref[pl.ds(at, BLK), :] = k[j * BLK : (j + 1) * BLK]
            pos = base + at + lax.broadcasted_iota(jnp.int32, (1, BLK), 1)
            v_ref[:, pl.ds(at, BLK)] = jnp.where(pos < sc_ref[0], v[:, j * BLK : (j + 1) * BLK], 0.0).astype(BF)
            to = pl.multiple_of((edge + 2 * j) * PART, PART)
            nq_scr[pl.ds(to, PART), :] = n_scr[s, pl.ds(j * BLK + qo, PART), :]
            x_ref[pl.ds(to, PART), :] = ref[pl.ds(j * BLK + qo, PART), :]
    nq = nq_scr[...]
    q_ref[...] = twice_silu(0.5 * tn(w_ref[:, wq], nq)).astype(BF) * BF(1 / 16)
    g_ref[...] = twice_silu(0.5 * tn(w_ref[:, wg], nq)).astype(BF)


def attend(sc_ref, tiles, together):
    rid = lax.broadcasted_iota(jnp.int32, (128, 256), 0)
    col = lax.broadcasted_iota(jnp.int32, (1, 512), 1) & 255
    last_key = (col // PART) * BLK + (col % PART) + sc_ref[1]
    key = lax.broadcasted_iota(jnp.int32, (BLK, 512), 0)

    def heads(pp, _):
        steps = [
            (u, t, m, i)
            for u in range(together)
            for t in range(len(tiles))
            for m in range(len(tiles[t][2]))
            for i in range(GRP // BLK)
        ]
        queries = {}
        sums = {}

        def lanes(u):
            return pl.multiple_of((pp * together + u) * 128, 128)

        def scores(step):
            u, t, m, i = step
            if (u, t) not in queries:
                q = tiles[t][0][pl.ds(lanes(u), 128), :]
                zero = jnp.zeros_like(q)
                queries[u, t] = jnp.concatenate([jnp.where(rid < 64, q, zero), jnp.where(rid < 64, zero, q)], axis=1)
            return nn(tiles[t][2][m][0][i * BLK : (i + 1) * BLK, pl.ds(lanes(u), 128)], queries[u, t])

        def weights(step, s):
            _, t, m, i = step
            w = s + s * jnp.tanh(s)
            if tiles[t][2][m][2]:
                w = jnp.where(key + i * BLK <= last_key, w, 0.0)
            return w.astype(BF)

        def add_values(step, w):
            u, t, m, i = step
            o = [
                nn(
                    tiles[t][2][m][1][pl.ds(pl.multiple_of(lanes(u) + 64 * hh, 64), 64), i * BLK : (i + 1) * BLK],
                    w[:, 256 * hh : 256 * (hh + 1)],
                )
                for hh in range(2)
            ]
            old = sums.get((u, t))
            sums[u, t] = o if old is None else (old[0] + o[0], old[1] + o[1])

        s = scores(steps[0])
        before = None
        for n, step in enumerate(steps):
            ahead = scores(steps[n + 1]) if n + 1 < len(steps) else None
            w = weights(step, s)
            if before is not None:
                add_values(steps[n - 1], before)
            before, s = w, ahead
        add_values(steps[-1], before)
        for (u, t), pair in sums.items():
            for hh in range(2):
                tiles[t][1][pl.ds(pl.multiple_of(lanes(u) + 64 * hh, 64), 64), :] = pair[hh]
        return 0

    lax.fori_loop(0, 4 // together, heads, 0)


def early_kernel(side, length_ref, p1, p2, w_ref, *refs):
    sc_ref = scalars(length_ref)
    outs, held, (n_scr, nq_scr, sems) = refs[:6], refs[6:12], refs[12:]
    k, v, q, g, x, o = held
    copies = [pltpu.make_async_copy(src, dst, sems.at[i]) for i, (src, dst) in enumerate(zip(held, outs))]
    project(0, side, sc_ref, (p1, p2), w_ref, k, v, q, g, x, n_scr, nq_scr)
    for c in copies[:5]:
        c.start()
    attend(sc_ref, [(q, o, [(k, v, True)])], 2)
    copies[5].start()
    for c in copies:
        c.wait()


def middle_kernel(length_ref, p1, p2, w_ref, wo_hbm, *refs):
    sc_ref = scalars(length_ref)
    sent, (k1, v1, q1, g1, x1, o1), refs = refs[:12], refs[12:18], refs[18:]
    (out_ref, kn, vn, kf, vf), refs = refs[:5], refs[5:]
    qn, gn, xn, on, qf, gf, xf, of, wo_ref, qx, kx, vx, ox, n_scr, nq_scr, sems = refs
    landed = (kn, vn, qn, gn, xn, on, kf, vf, qf, gf, xf, of, wo_ref)
    copies = [pltpu.make_async_copy(src, dst, sems.at[i]) for i, (src, dst) in enumerate(zip((*sent, wo_hbm), landed))]
    for c in copies:
        c.start()
    project(2 * GRP, 0, sc_ref, (p1, p2), w_ref, k1, v1, q1, g1, x1, n_scr, nq_scr)
    for c in copies:
        c.wait()
    cross(sc_ref, (qn, kn, vn), (qf, kf, vf), (qx, kx, vx))
    attend(sc_ref, [(q1, o1, [(k1, v1, True)]), (qx, ox, [(kx, vx, False)])], 2)
    finish(0, sc_ref, wo_ref, ox, ((on, gn, xn), (of, gf, xf)), out_ref)


def cross(sc_ref, near, far, to):
    low = sc_ref[3] == 0

    @pl.when(low)
    def _():
        to[0][...], to[1][...], to[2][...] = far[0][...], near[1][...], near[2][...]

    @pl.when(jnp.logical_not(low))
    def _():
        to[0][...], to[1][...], to[2][...] = near[0][...], far[1][...], far[2][...]


def past_kernel(k0, v0, k1, v1, q_ref, before_ref, o_ref):
    sc_ref = scalars()
    attend(sc_ref, [(q_ref, o_ref, [(k0, v0, False), (k1, v1, False)])], 2)
    o_ref[...] = o_ref[...] + before_ref[...]


def finish(chunk, sc_ref, wo_ref, ox, sides, out_ref):
    for side, (o_ref, g_ref, x_ref) in enumerate(sides):
        o = o_ref[...] + jnp.where(sc_ref[3 + side] == 1, ox[...], 0.0)
        c = o - jnp.mean(o, axis=0, keepdims=True)
        var = jnp.mean(c * c, axis=0, keepdims=True)
        gated = ((c * lax.rsqrt(var + 1e-5)) * g_ref[...].astype(F32)).astype(BF)
        mixed = lax.dot_general(gated, wo_ref[...], (((0,), (0,)), ((), ())), preferred_element_type=F32)
        out = (x_ref[...].astype(F32) + mixed).astype(BF)
        for j in range(2):
            at = pl.multiple_of(512 * chunk + 256 * j + 128 * sc_ref[3 + side], 128)
            out_ref[pl.ds(at, 128), :] = out[128 * j : 128 * (j + 1)]


def far1_kernel(length_ref, *refs):
    sc_ref = scalars(length_ref)
    past, (p1, p2, w_ref, wo_hbm), kept = refs[:4], refs[4:8], refs[8:14]
    first_ref, out_ref = refs[14:16]
    n_scr, nq_scr, qf, gf, xf, of, qx, kx, vx, ox, kf, vf, wo_ref, sem = refs[16:]
    kn, vn, qn, gn, xn, on = kept
    copy = pltpu.make_async_copy(wo_hbm, wo_ref, sem)
    copy.start()
    project(2 * GRP, 1, sc_ref, (p1, p2), w_ref, kf, vf, qf, gf, xf, n_scr, nq_scr)
    copy.wait()
    cross(sc_ref, (qn, kn, vn), (qf, kf, vf), (qx, kx, vx))
    seen = [(past[0], past[1], False), (past[2], past[3], False)]
    attend(sc_ref, [(qf, of, seen + [(kf, vf, True)]), (qx, ox, [(kx, vx, False)])], 2)
    finish(1, sc_ref, wo_ref, ox, ((on, gn, xn), (of, gf, xf)), out_ref)
    out_ref[:512, :] = first_ref[...]


SIZES = [(GRP, D), (D, GRP), (D, 256), (D, 256), (256, D)]
SUMS = pltpu.VMEM((D, 256), F32)
PROJECT = [pltpu.VMEM((2, D, D), BF), pltpu.VMEM((256, D), BF)]


def held(some=slice(None)):
    return [pltpu.VMEM(s, BF) for s in SIZES[some]]


def call(kernel, us, inputs, in_specs, out_shape, out_specs, scratch):
    return pl.pallas_call(
        kernel,
        out_shape=out_shape,
        in_specs=in_specs,
        out_specs=out_specs,
        scratch_shapes=scratch,
        compiler_params=PARAMS,
        cost_estimate=cost(us),
    )(*inputs)


def early_call(side, length, p1, p2, w_in):
    shapes = [pltpu.HBM(s, BF) for s in SIZES] + [pltpu.HBM((D, 256), F32)]
    scratch = held() + [SUMS] + PROJECT + [pltpu.SemaphoreType.DMA((6,))]
    kernel = functools.partial(early_kernel, side)
    return call(kernel, 6, (length, p1, p2, w_in), [VM] * 4, shapes, [HBM] * 6, scratch)


SQUARE = pltpu.VMEM((D, D), BF)
CROSS = [pltpu.VMEM((D, 256), BF)] + held(slice(0, 2)) + [SUMS]


def middle_call(length, own, near, w_in, w_out, sent):
    shapes = held() + [SUMS, SQUARE] + held(slice(0, 2)) * 2
    scratch = (held(slice(2, 5)) + [SUMS]) * 2 + [SQUARE] + CROSS + PROJECT + [pltpu.SemaphoreType.DMA((13,))]
    inputs = (length, own, near, w_in, w_out, *sent)
    return call(middle_kernel, 9, inputs, [VM] * 4 + [HBM] * 13, shapes, [VM] * 11, scratch)


def past_call(past, q, before):
    return call(past_kernel, 5, (*past, q, before), [VM] * 6, SUMS, VM, [])


def far1_call(length, past, far, diag, w_in, w_out, kept, first):
    inputs = (length, *past, far, diag, w_in, w_out, *kept, first)
    specs = [VM] * 8 + [HBM] + [VM] * 7
    scratch = PROJECT + held(slice(2, 5)) + [SUMS] + CROSS + held(slice(0, 2)) + [SQUARE, pltpu.SemaphoreType.DMA]
    return call(far1_kernel, 11, inputs, specs, jax.ShapeDtypeStruct((1024, D), BF), VM, scratch)


from jax.sharding import Mesh
from jax.sharding import PartitionSpec as P

CTX = ("xh", "xl", "yh", "co")
FLIP = [(0, 1), (1, 0)]


def layer(item_ids, lengths, table, w_in, w_out):
    owned = table.shape[0]
    me = lax.axis_index("dp")
    xh, _, yh, _ = (lax.axis_index(a) for a in CTX)
    owners = lax.axis_size("dp")
    w_in = in_vmem(w_in)
    w_out = pltpu.with_memory_space_constraint(w_out, pltpu.HBM)
    groups = table.reshape(-1, 8, D)

    send = jnp.broadcast_to(item_ids[None, :, None], (owners, 4, 1, BLK)).reshape(owners * 4, 1, BLK)
    wanted = lax.all_to_all(send, ("dp", "xh", "yh"), 0, 0, tiled=True)
    wanted = wanted.reshape(owners, 4, BLK)
    mine = lax.dynamic_index_in_dim(wanted, me, 0, keepdims=False)
    upto = jnp.triu(jnp.ones((2 * BLK, 2 * BLK), BF))
    users = lax.broadcasted_iota(jnp.int32, (4, 8, 128), 0)
    length = jnp.sum(jnp.where(users == 2 * xh + yh, lengths[:, None, None], 0), axis=0)

    def ranks(member):
        return nn(member.astype(BF), upto).astype(jnp.int32) - 1

    def fetch(c):
        ids = wanted[:, 2 * c : 2 * c + 2].reshape(owners, 2 * BLK)
        local = ids - me * owned
        here = (local >= 0) & (local < owned)
        rank = jnp.where(here, ranks(here), -1)
        slot = lax.broadcasted_iota(jnp.int32, (owners, CAP, 2 * BLK), 1)
        rows = jnp.sum(jnp.where(rank[:, None, :] == slot, local[:, None, :], 0), axis=2)
        count = jnp.sum(here.astype(jnp.int32), axis=1)
        picked = gather_call(rows, count, groups, 1)[0].reshape(owners, CAP, D)
        return lax.all_to_all(picked, "dp", 0, 0, tiled=True).reshape(owners * CAP, D)

    def place(c, got):
        own_ids = mine[2 * c : 2 * c + 2].reshape(2 * BLK)
        owner = own_ids // owned
        member = owner[None, :] == lax.broadcasted_iota(jnp.int32, (owners, 2 * BLK), 0)
        at = jnp.sum(jnp.where(member, ranks(member), 0), axis=0) + owner * CAP
        return place_call(at[None], length, in_vmem(got))

    def vmem_all(arrays):
        return [in_vmem(a) for a in arrays]

    for c in range(2):
        got = fetch(c)
        own, kept_length = place(c, got)
        far = lax.ppermute(own, "xl", FLIP)
        near = lax.ppermute(own, "co", FLIP)
        diag = lax.ppermute(far, "co", FLIP)
        own, near, far, diag, kept_length = vmem_all((own, near, far, diag, kept_length))
        if c == 0:
            sent = early_call(0, kept_length, own, near, w_in)
            sent += early_call(1, kept_length, far, diag, w_in)
            sent = [pltpu.with_memory_space_constraint(a, pltpu.HBM) for a in sent]
        else:
            done = middle_call(kept_length, own, near, w_in, w_out, sent)
            done = vmem_all(done)
            kept, first, past = done[:6], done[6], done[7:]
            total = past_call(past, kept[2], kept[5])
            kept[5] = in_vmem(total)
            out = far1_call(kept_length, past, far, diag, w_in, w_out, kept, first)
    back = lax.all_to_all(out.reshape(16, PART, D), ("xh", "yh", "xl", "co"), 0, 0, tiled=True)
    return back.reshape(4, BLK, D)


def solution(mesh):
    finer = Mesh(mesh.devices.reshape(mesh.shape["dp"], 2, 2, 2, 2), ("dp",) + CTX)
    return jax.shard_map(
        layer,
        mesh=finer,
        in_specs=(P("dp", CTX), P("dp"), P("dp", None), P(), P()),
        out_specs=P("dp", CTX, None),
        check_vma=False,
    )
```

```python
import functools

import jax
import jax.numpy as jnp
from jax import lax
from jax.experimental import pallas as pl
from jax.experimental.pallas import tpu as pltpu

BF = jnp.bfloat16
F32 = jnp.float32
BLK = 256
D = 512
GRP = 1024
PART = 64
CAP = 128
ROW8 = 8
BUNCH = 32
VM = pl.BlockSpec(memory_space=pltpu.VMEM)
SM = pl.BlockSpec(memory_space=pltpu.SMEM)
HBM = pl.BlockSpec(memory_space=pltpu.HBM)
PARAMS = pltpu.CompilerParams(vmem_limit_bytes=16 * 1024 * 1024)


def cost(us):
    return pl.CostEstimate(flops=int(us * 4_000_000), bytes_accessed=0, transcendentals=0)


def in_vmem(x):
    return pltpu.with_memory_space_constraint(x, pltpu.VMEM)


def twice_silu(h):
    return h + h * jnp.tanh(h)


def tn(a, b):
    return lax.dot_general(a, b, (((0,), (1,)), ((), ())), preferred_element_type=F32)


def nn(a, b):
    return jnp.dot(a, b, preferred_element_type=F32)


def gather_kernel(owners, outs, rows_ref, count_ref, ids_ref, table_ref, *refs):
    out_refs, (buf, sems) = refs[:outs], refs[outs:]
    me = lax.axis_index("dp") if outs > 1 else 0

    def who(k):
        return jnp.bitwise_xor(me, k) if outs > 1 else k

    def eights(k):
        return (count_ref[who(k)] + ROW8 - 1) // ROW8

    for k in range(owners):
        o = who(k)

        def start(j, _, k=k, o=o):
            for i in range(ROW8):
                s = j * ROW8 + i
                pltpu.make_async_copy(
                    table_ref.at[lax.shift_right_logical(rows_ref[o, s], 3)], buf.at[k * CAP + s], sems.at[k]
                ).start()
            return 0

        def clear(j, _, k=k):
            buf[pl.ds(k * CAP + j * ROW8, ROW8)] = jnp.zeros((ROW8, 8, D), BF)
            return 0

        lax.fori_loop(0, eights(k), start, 0)
        full = BUNCH // ROW8
        lax.fori_loop(eights(k), (eights(k) + full - 1) // full * full, clear, 0)
    width = BUNCH * 8
    lane = lax.broadcasted_iota(jnp.int32, (BUNCH, width), 1).astype(F32)
    slot = lax.broadcasted_iota(jnp.int32, (BUNCH, 1), 0)
    for k in range(owners):
        eight = buf.at[pl.ds(k * CAP, ROW8)]

        def wait(j, _, k=k, eight=eight):
            pltpu.make_async_copy(eight, eight, sems.at[k]).wait()
            return 0

        lax.fori_loop(0, eights(k), wait, 0)
    low8 = (ids_ref[...] & 7).astype(F32).T
    for k in range(owners):
        o = who(k)
        if outs > 1:
            low = jnp.broadcast_to((ids_ref[pl.ds(o, 1), :] & 7).astype(F32), (8, CAP)).T[:, :1]
        else:
            low = low8[:, k : k + 1]
        for b in range(CAP // BUNCH):
            want = (8 * slot).astype(F32) + low[b * BUNCH : (b + 1) * BUNCH]
            pick = (lane == want).astype(F32).astype(BF)
            at = k * CAP + b * BUNCH
            got = nn(pick, buf[at : at + BUNCH].reshape(width, D))
            got = jnp.where(slot + b * BUNCH < count_ref[o], got, 0.0).astype(BF)
            if outs > 1:
                out_refs[k][b * BUNCH : (b + 1) * BUNCH, :] = got
            else:
                out_refs[0][at : at + BUNCH, :] = got


def gather_call(rows, count, groups, outs):
    owners = rows.shape[0]
    shape = jax.ShapeDtypeStruct((owners // outs * CAP, D), BF)
    return pl.pallas_call(
        functools.partial(gather_kernel, owners, outs),
        out_shape=[shape] * outs,
        in_specs=[SM, SM, VM, HBM],
        out_specs=[VM] * outs,
        scratch_shapes=[pltpu.VMEM((owners * CAP, 8, D), BF), pltpu.SemaphoreType.DMA((owners,))],
        compiler_params=pltpu.CompilerParams(vmem_limit_bytes=56 * 1024 * 1024),
        cost_estimate=cost(7),
    )(rows, count, rows, groups)


def place_kernel(at_ref, length_ref, got_ref, own_ref, kept_ref):
    kept_ref[...] = length_ref[...]
    rows = own_ref.shape[0]
    at = jnp.broadcast_to(at_ref[...].astype(F32), (8, rows)).T[:, :1]
    lane = lax.broadcasted_iota(jnp.int32, (rows, got_ref.shape[0]), 1).astype(F32)
    own_ref[...] = nn((lane == at).astype(F32).astype(BF), got_ref[...]).astype(BF)


def place_call(at, length, got):
    return pl.pallas_call(
        place_kernel,
        out_shape=[pltpu.VMEM((at.shape[1], D), BF), pltpu.VMEM(length.shape, jnp.int32)],
        in_specs=[VM] * 3,
        out_specs=[VM, VM],
        compiler_params=PARAMS,
        cost_estimate=cost(1.5),
        name="place",
    )(at, length, got)


def scalars(length_ref=None):
    xl, co = lax.axis_index("xl"), lax.axis_index("co")
    length = None if length_ref is None else length_ref[0:1, 0:1]
    return length, PART * (2 * xl + co), co, xl, 1 - xl


def project(first, side, sc_ref, pieces, w_ref, k_ref, v_ref, q_ref, g_ref, x_ref, n_scr, nq_scr):
    co = sc_ref[2]
    base = first + GRP * sc_ref[3 + side]
    qo = pl.multiple_of(sc_ref[1], PART)
    wg, wv, wq, wk = (slice(D * i, D * (i + 1)) for i in range(4))
    for s, ref in enumerate(pieces):
        x = ref[...].astype(F32)
        c = x - jnp.mean(x, axis=1, keepdims=True)
        var = jnp.mean(c * c, axis=1, keepdims=True)
        n_scr[s] = (c * lax.rsqrt(var + 1e-5)).astype(BF)
    for s, ref in enumerate(pieces):
        edge = co if s == 0 else 1 - co
        n = n_scr[s]
        k = twice_silu(0.5 * nn(n, w_ref[:, wk])).astype(BF)
        v = twice_silu(0.5 * tn(w_ref[:, wv], n))
        for j in range(2):
            at = pl.multiple_of((edge + 2 * j) * BLK, BLK)
            k_ref[pl.ds(at, BLK), :] = k[j * BLK : (j + 1) * BLK]
            pos = base + at + lax.broadcasted_iota(jnp.int32, (1, BLK), 1)
            v_ref[:, pl.ds(at, BLK)] = jnp.where(pos < sc_ref[0], v[:, j * BLK : (j + 1) * BLK], 0.0).astype(BF)
            to = pl.multiple_of((edge + 2 * j) * PART, PART)
            nq_scr[pl.ds(to, PART), :] = n_scr[s, pl.ds(j * BLK + qo, PART), :]
            x_ref[pl.ds(to, PART), :] = ref[pl.ds(j * BLK + qo, PART), :]
    nq = nq_scr[...]
    q_ref[...] = twice_silu(0.5 * tn(w_ref[:, wq], nq)).astype(BF) * BF(1 / 16)
    g_ref[...] = twice_silu(0.5 * tn(w_ref[:, wg], nq)).astype(BF)


def attend(sc_ref, tiles, together):
    rid = lax.broadcasted_iota(jnp.int32, (128, 256), 0)
    col = lax.broadcasted_iota(jnp.int32, (1, 512), 1) & 255
    last_key = (col // PART) * BLK + (col % PART) + sc_ref[1]
    key = lax.broadcasted_iota(jnp.int32, (BLK, 512), 0)

    def heads(pp, _):
        steps = [
            (u, t, m, i)
            for u in range(together)
            for t in range(len(tiles))
            for m in range(len(tiles[t][2]))
            for i in range(GRP // BLK)
        ]
        queries = {}
        sums = {}

        def lanes(u):
            return pl.multiple_of((pp * together + u) * 128, 128)

        def scores(step):
            u, t, m, i = step
            if (u, t) not in queries:
                q = tiles[t][0][pl.ds(lanes(u), 128), :]
                zero = jnp.zeros_like(q)
                queries[u, t] = jnp.concatenate([jnp.where(rid < 64, q, zero), jnp.where(rid < 64, zero, q)], axis=1)
            return nn(tiles[t][2][m][0][i * BLK : (i + 1) * BLK, pl.ds(lanes(u), 128)], queries[u, t])

        def weights(step, s):
            _, t, m, i = step
            w = s + s * jnp.tanh(s)
            if tiles[t][2][m][2]:
                w = jnp.where(key + i * BLK <= last_key, w, 0.0)
            return w.astype(BF)

        def add_values(step, w):
            u, t, m, i = step
            o = [
                nn(
                    tiles[t][2][m][1][pl.ds(pl.multiple_of(lanes(u) + 64 * hh, 64), 64), i * BLK : (i + 1) * BLK],
                    w[:, 256 * hh : 256 * (hh + 1)],
                )
                for hh in range(2)
            ]
            old = sums.get((u, t))
            sums[u, t] = o if old is None else (old[0] + o[0], old[1] + o[1])

        s = scores(steps[0])
        before = None
        for n, step in enumerate(steps):
            ahead = scores(steps[n + 1]) if n + 1 < len(steps) else None
            w = weights(step, s)
            if before is not None:
                add_values(steps[n - 1], before)
            before, s = w, ahead
        add_values(steps[-1], before)
        for (u, t), pair in sums.items():
            for hh in range(2):
                tiles[t][1][pl.ds(pl.multiple_of(lanes(u) + 64 * hh, 64), 64), :] = pair[hh]
        return 0

    lax.fori_loop(0, 4 // together, heads, 0)


def early_kernel(side, length_ref, p1, p2, w_ref, *refs):
    sc_ref = scalars(length_ref)
    outs, held, (n_scr, nq_scr, sems) = refs[:6], refs[6:12], refs[12:]
    k, v, q, g, x, o = held
    copies = [pltpu.make_async_copy(src, dst, sems.at[i]) for i, (src, dst) in enumerate(zip(held, outs))]
    project(0, side, sc_ref, (p1, p2), w_ref, k, v, q, g, x, n_scr, nq_scr)
    for c in copies[:5]:
        c.start()
    attend(sc_ref, [(q, o, [(k, v, True)])], 2)
    copies[5].start()
    for c in copies:
        c.wait()


def middle_kernel(length_ref, p1, p2, w_ref, wo_hbm, *refs):
    sc_ref = scalars(length_ref)
    sent, (k1, v1, q1, g1, x1, o1), refs = refs[:12], refs[12:18], refs[18:]
    (out_ref, kn, vn, kf, vf), refs = refs[:5], refs[5:]
    qn, gn, xn, on, qf, gf, xf, of, wo_ref, qx, kx, vx, ox, n_scr, nq_scr, sems = refs
    landed = (kn, vn, qn, gn, xn, on, kf, vf, qf, gf, xf, of, wo_ref)
    copies = [pltpu.make_async_copy(src, dst, sems.at[i]) for i, (src, dst) in enumerate(zip((*sent, wo_hbm), landed))]
    for c in copies:
        c.start()
    project(2 * GRP, 0, sc_ref, (p1, p2), w_ref, k1, v1, q1, g1, x1, n_scr, nq_scr)
    for c in copies:
        c.wait()
    cross(sc_ref, (qn, kn, vn), (qf, kf, vf), (qx, kx, vx))
    attend(sc_ref, [(q1, o1, [(k1, v1, True)]), (qx, ox, [(kx, vx, False)])], 2)
    finish(0, sc_ref, wo_ref, ox, ((on, gn, xn), (of, gf, xf)), out_ref)


def cross(sc_ref, near, far, to):
    low = sc_ref[3] == 0

    @pl.when(low)
    def _():
        to[0][...], to[1][...], to[2][...] = far[0][...], near[1][...], near[2][...]

    @pl.when(jnp.logical_not(low))
    def _():
        to[0][...], to[1][...], to[2][...] = near[0][...], far[1][...], far[2][...]


def past_kernel(k0, v0, k1, v1, q_ref, before_ref, o_ref):
    sc_ref = scalars()
    attend(sc_ref, [(q_ref, o_ref, [(k0, v0, False), (k1, v1, False)])], 2)
    o_ref[...] = o_ref[...] + before_ref[...]


def finish(chunk, sc_ref, wo_ref, ox, sides, out_ref):
    for side, (o_ref, g_ref, x_ref) in enumerate(sides):
        o = o_ref[...] + jnp.where(sc_ref[3 + side] == 1, ox[...], 0.0)
        c = o - jnp.mean(o, axis=0, keepdims=True)
        var = jnp.mean(c * c, axis=0, keepdims=True)
        gated = ((c * lax.rsqrt(var + 1e-5)) * g_ref[...].astype(F32)).astype(BF)
        mixed = lax.dot_general(gated, wo_ref[...], (((0,), (0,)), ((), ())), preferred_element_type=F32)
        out = (x_ref[...].astype(F32) + mixed).astype(BF)
        for j in range(2):
            at = pl.multiple_of(512 * chunk + 256 * j + 128 * sc_ref[3 + side], 128)
            out_ref[pl.ds(at, 128), :] = out[128 * j : 128 * (j + 1)]


def far1_kernel(length_ref, *refs):
    sc_ref = scalars(length_ref)
    past, (p1, p2, w_ref, wo_ref), kept = refs[:4], refs[4:8], refs[8:14]
    first_ref, out_ref = refs[14:16]
    n_scr, nq_scr, qf, gf, xf, of, qx, kx, vx, ox, kf, vf = refs[16:]
    kn, vn, qn, gn, xn, on = kept
    project(2 * GRP, 1, sc_ref, (p1, p2), w_ref, kf, vf, qf, gf, xf, n_scr, nq_scr)
    cross(sc_ref, (qn, kn, vn), (qf, kf, vf), (qx, kx, vx))
    seen = [(past[0], past[1], False), (past[2], past[3], False)]
    attend(sc_ref, [(qf, of, seen + [(kf, vf, True)]), (qx, ox, [(kx, vx, False)])], 2)
    finish(1, sc_ref, wo_ref, ox, ((on, gn, xn), (of, gf, xf)), out_ref)
    out_ref[:512, :] = first_ref[...]


SIZES = [(GRP, D), (D, GRP), (D, 256), (D, 256), (256, D)]
SUMS = pltpu.VMEM((D, 256), F32)
PROJECT = [pltpu.VMEM((2, D, D), BF), pltpu.VMEM((256, D), BF)]


def held(some=slice(None)):
    return [pltpu.VMEM(s, BF) for s in SIZES[some]]


def call(kernel, us, inputs, in_specs, out_shape, out_specs, scratch):
    return pl.pallas_call(
        kernel,
        out_shape=out_shape,
        in_specs=in_specs,
        out_specs=out_specs,
        scratch_shapes=scratch,
        compiler_params=PARAMS,
        cost_estimate=cost(us),
    )(*inputs)


def early_call(side, length, p1, p2, w_in):
    shapes = [pltpu.HBM(s, BF) for s in SIZES] + [pltpu.HBM((D, 256), F32)]
    scratch = held() + [SUMS] + PROJECT + [pltpu.SemaphoreType.DMA((6,))]
    kernel = functools.partial(early_kernel, side)
    return call(kernel, 6, (length, p1, p2, w_in), [VM] * 4, shapes, [HBM] * 6, scratch)


SQUARE = pltpu.VMEM((D, D), BF)
CROSS = [pltpu.VMEM((D, 256), BF)] + held(slice(0, 2)) + [SUMS]


def middle_call(length, own, near, w_in, w_out, sent):
    shapes = held() + [SUMS, SQUARE] + held(slice(0, 2)) * 2
    scratch = (held(slice(2, 5)) + [SUMS]) * 2 + [SQUARE] + CROSS + PROJECT + [pltpu.SemaphoreType.DMA((13,))]
    inputs = (length, own, near, w_in, w_out, *sent)
    return call(middle_kernel, 9, inputs, [VM] * 4 + [HBM] * 13, shapes, [VM] * 11, scratch)


def past_call(past, q, before):
    return call(past_kernel, 5, (*past, q, before), [VM] * 6, SUMS, VM, [])


def far1_call(length, past, far, diag, w_in, w_out, kept, first):
    inputs = (length, *past, far, diag, w_in, w_out, *kept, first)
    scratch = PROJECT + held(slice(2, 5)) + [SUMS] + CROSS + held(slice(0, 2))
    return call(far1_kernel, 11, inputs, [VM] * 16, jax.ShapeDtypeStruct((1024, D), BF), VM, scratch)


from jax.sharding import Mesh
from jax.sharding import PartitionSpec as P

CTX = ("xh", "xl", "yh", "co")
FLIP = [(0, 1), (1, 0)]


def layer(item_ids, lengths, table, w_in, w_out):
    owned = table.shape[0]
    me = lax.axis_index("dp")
    xh, _, yh, _ = (lax.axis_index(a) for a in CTX)
    owners = lax.axis_size("dp")
    w_in = in_vmem(w_in)
    w_out, w_far = pltpu.with_memory_space_constraint(w_out, pltpu.HBM), in_vmem(w_out)
    groups = table.reshape(-1, 8, D)

    send = jnp.broadcast_to(item_ids[None, :, None], (owners, 4, 1, BLK)).reshape(owners * 4, 1, BLK)
    wanted = lax.all_to_all(send, ("dp", "xh", "yh"), 0, 0, tiled=True)
    wanted = wanted.reshape(owners, 4, BLK)
    mine = lax.dynamic_index_in_dim(wanted, me, 0, keepdims=False)
    upto = jnp.triu(jnp.ones((2 * BLK, 2 * BLK), BF))
    users = lax.broadcasted_iota(jnp.int32, (4, 8, 128), 0)
    length = jnp.sum(jnp.where(users == 2 * xh + yh, lengths[:, None, None], 0), axis=0)

    def ranks(member):
        return nn(member.astype(BF), upto).astype(jnp.int32) - 1

    def fetch(c):
        ids = wanted[:, 2 * c : 2 * c + 2].reshape(owners, 2 * BLK)
        local = ids - me * owned
        here = (local >= 0) & (local < owned)
        rank = jnp.where(here, ranks(here), -1)
        slot = lax.broadcasted_iota(jnp.int32, (owners, CAP, 2 * BLK), 1)
        rows = jnp.sum(jnp.where(rank[:, None, :] == slot, local[:, None, :], 0), axis=2)
        count = jnp.sum(here.astype(jnp.int32), axis=1)
        picked = gather_call(rows, count, groups, 1)[0].reshape(owners, CAP, D)
        return lax.all_to_all(picked, "dp", 0, 0, tiled=True).reshape(owners * CAP, D)

    def place(c, got):
        own_ids = mine[2 * c : 2 * c + 2].reshape(2 * BLK)
        owner = own_ids // owned
        member = owner[None, :] == lax.broadcasted_iota(jnp.int32, (owners, 2 * BLK), 0)
        at = jnp.sum(jnp.where(member, ranks(member), 0), axis=0) + owner * CAP
        return place_call(at[None], length, in_vmem(got))

    def vmem_all(arrays):
        return [in_vmem(a) for a in arrays]

    for c in range(2):
        got = fetch(c)
        own, kept_length = place(c, got)
        far = lax.ppermute(own, "xl", FLIP)
        near = lax.ppermute(own, "co", FLIP)
        diag = lax.ppermute(far, "co", FLIP)
        own, near, far, diag, kept_length = vmem_all((own, near, far, diag, kept_length))
        if c == 0:
            sent = early_call(0, kept_length, own, near, w_in)
            sent += early_call(1, kept_length, far, diag, w_in)
            sent = [pltpu.with_memory_space_constraint(a, pltpu.HBM) for a in sent]
        else:
            done = middle_call(kept_length, own, near, w_in, w_out, sent)
            done = vmem_all(done)
            kept, first, past = done[:6], done[6], done[7:]
            total = past_call(past, kept[2], kept[5])
            kept[5] = in_vmem(total)
            out = far1_call(kept_length, past, far, diag, w_in, w_far, kept, first)
    back = lax.all_to_all(out.reshape(16, PART, D), ("xh", "yh", "xl", "co"), 0, 0, tiled=True)
    return back.reshape(4, BLK, D)


def solution(mesh):
    finer = Mesh(mesh.devices.reshape(mesh.shape["dp"], 2, 2, 2, 2), ("dp",) + CTX)
    return jax.shard_map(
        layer,
        mesh=finer,
        in_specs=(P("dp", CTX), P("dp"), P("dp", None), P(), P()),
        out_specs=P("dp", CTX, None),
        check_vma=False,
    )
```
